8 devices in a mesh: dp: 2 (over z, y), tp: 4 (over x, core).
Axes of the slice: x: 2, y: 2, z: 1, core: 2. Of those that a mesh axis runs over, the one named last changes fastest.
Arguments:
- resid_in: bfloat16 [256, 1, 3072], P(('dp', 'tp')), parts along dimension 0
- grad_out: bfloat16 [256, 1, 3072], P(('dp', 'tp')), parts along dimension 0
- positions: int32 [256], P('dp'), parts along dimension 0
- ln1_gain: float32 [3072], replicated
- ln1_bias: float32 [3072], replicated
- ln2_gain: float32 [3072], replicated
- ln2_bias: float32 [3072], replicated
- w_query: bfloat16 [3072, 3072], P(None, 'tp')
- w_key: bfloat16 [3072, 1024], P(None, 'tp')
- w_value: bfloat16 [3072, 1024], P(None, 'tp')
- w_out: bfloat16 [3072, 3072], P('tp')
- w_up: bfloat16 [3072, 8192], P(None, 'tp')
- w_down: bfloat16 [8192, 3072], P('tp')
Outputs:
- output 1: bfloat16 [256, 1, 3072], P(('dp', 'tp')), parts along dimension 0
- output 2: bfloat16 [256, 1, 3072], P(('dp', 'tp')), parts along dimension 0
- output 3: float32 [6144], P('dp'), parts along dimension 0
- output 4: float32 [6144], P('dp'), parts along dimension 0
- output 5: float32 [6144], P('dp'), parts along dimension 0
- output 6: float32 [6144], P('dp'), parts along dimension 0
- output 7: float32 [6144, 3072], P('dp', 'tp'), parts along dimension 0
- output 8: float32 [6144, 1024], P('dp', 'tp'), parts along dimension 0
- output 9: float32 [6144, 1024], P('dp', 'tp'), parts along dimension 0
- output 10: float32 [6144, 3072], P(('dp', 'tp')), parts along dimension 0
- output 11: float32 [6144, 8192], P('dp', 'tp'), parts along dimension 0
- output 12: float32 [16384, 3072], P(('dp', 'tp')), parts along dimension 0
There are 2 independent parts. The reference program is written for one: setup_inputs(seed, part) draws one part's arguments, and reference() takes and returns one part's arrays. A program takes and returns all parts, laid end to end along the dimension named above; an argument that names none is the same for every part.
All inputs are finite; a program needn't handle non-finite values.
Results may differ from the reference program's by a relative error of at most 0.018293.
Values are sent between devices in bfloat16 or wider.
A program may use at most 1 GiB of HBM per device.

```python
import jax
import jax.numpy as jnp
from jax import lax

MODEL_DIM = 3072
Q_HEADS = 24
KV_HEADS = 8
HEAD_DIM = 128
FFN_DIM = 8192
SEQ_LEN = 128
BATCH_SIZE = 1
LN_EPS = 1e-5
ROPE_BASE = 10000.0


def setup_inputs(seed: int = 0, part: int = 0) -> dict:
    base_key = jax.random.key(seed)
    part_key = jax.random.fold_in(base_key, part)
    weight_keys = jax.random.split(base_key, 10)
    part_keys = jax.random.split(part_key, 4)
    act_shape = (SEQ_LEN, BATCH_SIZE, MODEL_DIM)
    q_width = Q_HEADS * HEAD_DIM
    kv_width = KV_HEADS * HEAD_DIM
    in_scale = MODEL_DIM ** -0.5
    pos_steps = jax.random.randint(part_keys[2], (SEQ_LEN,), 1, 4)
    pos_start = jax.random.randint(part_keys[3], (), 0, 1024)
    return {
        'resid_in': jax.random.normal(part_keys[0], act_shape, jnp.float32).astype(jnp.bfloat16),
        'grad_out': jax.random.normal(part_keys[1], act_shape, jnp.float32).astype(jnp.bfloat16),
        'positions': (pos_start + jnp.cumsum(pos_steps) - pos_steps[0]).astype(jnp.int32),
        'ln1_gain': 0.3 * jax.random.normal(weight_keys[0], (MODEL_DIM,), jnp.float32),
        'ln1_bias': 0.3 * jax.random.normal(weight_keys[1], (MODEL_DIM,), jnp.float32),
        'ln2_gain': 0.3 * jax.random.normal(weight_keys[2], (MODEL_DIM,), jnp.float32),
        'ln2_bias': 0.3 * jax.random.normal(weight_keys[3], (MODEL_DIM,), jnp.float32),
        'w_query': (jax.random.normal(weight_keys[4], (MODEL_DIM, q_width), jnp.float32) * in_scale).astype(jnp.bfloat16),
        'w_key': (jax.random.normal(weight_keys[5], (MODEL_DIM, kv_width), jnp.float32) * in_scale).astype(jnp.bfloat16),
        'w_value': (jax.random.normal(weight_keys[6], (MODEL_DIM, kv_width), jnp.float32) * in_scale).astype(jnp.bfloat16),
        'w_out': (jax.random.normal(weight_keys[7], (q_width, MODEL_DIM), jnp.float32) * q_width ** -0.5).astype(jnp.bfloat16),
        'w_up': (jax.random.normal(weight_keys[8], (MODEL_DIM, FFN_DIM), jnp.float32) * in_scale).astype(jnp.bfloat16),
        'w_down': (jax.random.normal(weight_keys[9], (FFN_DIM, MODEL_DIM), jnp.float32) * FFN_DIM ** -0.5).astype(jnp.bfloat16),
    }


def layer_norm_1p(resid_f, gain, bias):
    mean_val = jnp.mean(resid_f, axis=-1, keepdims=True)
    centred = resid_f - mean_val
    var_val = jnp.mean(centred * centred, axis=-1, keepdims=True)
    return centred * lax.rsqrt(var_val + LN_EPS) * (1.0 + gain) + bias


def rope_tables(positions, head_dim):
    rot_half = head_dim // 4
    inv_freq = ROPE_BASE ** (-jnp.arange(rot_half, dtype=jnp.float32) / rot_half)
    angles = positions.astype(jnp.float32)[..., None] * inv_freq
    return jnp.cos(angles), jnp.sin(angles)


def apply_rope(values, cos_tab, sin_tab):
    rot_half = cos_tab.shape[-1]
    table_shape = cos_tab.shape[:-1] + (1,) * (values.ndim - cos_tab.ndim) + (rot_half,)
    cos_full = cos_tab.reshape(table_shape)
    sin_full = sin_tab.reshape(table_shape)
    first_half = values[..., :rot_half]
    second_half = values[..., rot_half:2 * rot_half]
    return jnp.concatenate([first_half * cos_full - second_half * sin_full, second_half * cos_full + first_half * sin_full, values[..., 2 * rot_half:]], axis=-1)


def causal_probs(q_head, k_head, causal):
    attn_scale = HEAD_DIM ** -0.5
    scores = jnp.einsum('sbgd,tbd->bgst', q_head.astype(jnp.float32), k_head.astype(jnp.float32)) * attn_scale
    scores = jnp.where(causal, scores, -1e30)
    row_max = jnp.max(scores, axis=-1, keepdims=True)
    exp_scores = jnp.exp(scores - row_max)
    return exp_scores / jnp.sum(exp_scores, axis=-1, keepdims=True)


def reference(resid_in, grad_out, positions, ln1_gain, ln1_bias, ln2_gain, ln2_bias, w_query, w_key, w_value, w_out, w_up, w_down):
    seq_len, n_batch, model_dim = resid_in.shape
    tokens = seq_len * n_batch
    q_per_kv = Q_HEADS // KV_HEADS
    attn_scale = HEAD_DIM ** -0.5
    causal = jnp.arange(seq_len)[:, None] >= jnp.arange(seq_len)[None, :]
    cos_tab, sin_tab = rope_tables(positions, HEAD_DIM)
    resid_f = resid_in.astype(jnp.float32).reshape(tokens, model_dim)
    h_one = layer_norm_1p(resid_f, ln1_gain, ln1_bias).astype(jnp.bfloat16)
    q_proj = jnp.dot(h_one, w_query, preferred_element_type=jnp.float32).astype(jnp.bfloat16)
    k_proj = jnp.dot(h_one, w_key, preferred_element_type=jnp.float32).astype(jnp.bfloat16)
    v_proj = jnp.dot(h_one, w_value, preferred_element_type=jnp.float32).astype(jnp.bfloat16)
    q_rot = apply_rope(q_proj.astype(jnp.float32).reshape(seq_len, n_batch, KV_HEADS, q_per_kv, HEAD_DIM), cos_tab, sin_tab).astype(jnp.bfloat16)
    k_rot = apply_rope(k_proj.astype(jnp.float32).reshape(seq_len, n_batch, KV_HEADS, HEAD_DIM), cos_tab, sin_tab).astype(jnp.bfloat16)
    q_heads = jnp.moveaxis(q_rot, 2, 0)
    k_heads = jnp.moveaxis(k_rot, 2, 0)
    v_heads = jnp.moveaxis(v_proj.reshape(seq_len, n_batch, KV_HEADS, HEAD_DIM), 2, 0)

    def head_forward(operands):
        q_head, k_head, v_head = operands
        attn_prob = causal_probs(q_head, k_head, causal)
        return jnp.einsum('bgst,tbd->sbgd', attn_prob.astype(jnp.bfloat16).astype(jnp.float32), v_head.astype(jnp.float32)).astype(jnp.bfloat16)

    ctx_heads = lax.map(head_forward, (q_heads, k_heads, v_heads))
    context = jnp.moveaxis(ctx_heads, 0, 2).reshape(tokens, Q_HEADS * HEAD_DIM)
    attn_out = jnp.dot(context, w_out, preferred_element_type=jnp.float32).astype(jnp.bfloat16)
    resid_mid = (resid_f + attn_out.astype(jnp.float32)).astype(jnp.bfloat16)
    mid_f = resid_mid.astype(jnp.float32)
    h_two = layer_norm_1p(mid_f, ln2_gain, ln2_bias).astype(jnp.bfloat16)
    up_proj = jnp.dot(h_two, w_up, preferred_element_type=jnp.float32).astype(jnp.bfloat16)
    relu_up = jnp.maximum(up_proj.astype(jnp.float32), 0.0)
    mlp_act = (relu_up * relu_up).astype(jnp.bfloat16)
    mlp_out = jnp.dot(mlp_act, w_down, preferred_element_type=jnp.float32).astype(jnp.bfloat16)
    resid_out = (mid_f + mlp_out.astype(jnp.float32)).astype(jnp.bfloat16)

    grad_flat = grad_out.reshape(tokens, model_dim)
    grad_w_down = jnp.dot(mlp_act.T, grad_flat, preferred_element_type=jnp.float32)
    grad_up = (jnp.dot(grad_flat, w_down.T, preferred_element_type=jnp.float32) * (2.0 * relu_up)).astype(jnp.bfloat16)
    grad_w_up = jnp.dot(h_two.T, grad_up, preferred_element_type=jnp.float32)
    grad_h_two = jnp.dot(grad_up, w_up.T, preferred_element_type=jnp.float32).astype(jnp.bfloat16)
    ln2_back = jax.vjp(layer_norm_1p, mid_f, ln2_gain, ln2_bias)[1]
    grad_mid_ln, grad_ln2_gain, grad_ln2_bias = ln2_back(grad_h_two.astype(jnp.float32))
    grad_mid = (grad_flat.astype(jnp.float32) + grad_mid_ln).astype(jnp.bfloat16)
    grad_w_out = jnp.dot(context.T, grad_mid, preferred_element_type=jnp.float32)
    grad_ctx = jnp.dot(grad_mid, w_out.T, preferred_element_type=jnp.float32).astype(jnp.bfloat16)
    gc_heads = jnp.moveaxis(grad_ctx.reshape(seq_len, n_batch, KV_HEADS, q_per_kv, HEAD_DIM), 2, 0)

    def head_backward(operands):
        q_head, k_head, v_head, gc_head = operands
        attn_prob = causal_probs(q_head, k_head, causal)
        grad_v = jnp.einsum('bgst,sbgd->tbd', attn_prob.astype(jnp.bfloat16).astype(jnp.float32), gc_head.astype(jnp.float32)).astype(jnp.bfloat16)
        grad_prob = jnp.einsum('sbgd,tbd->bgst', gc_head.astype(jnp.float32), v_head.astype(jnp.float32))
        grad_score = (attn_prob * (grad_prob - jnp.sum(grad_prob * attn_prob, axis=-1, keepdims=True)) * attn_scale).astype(jnp.bfloat16)
        grad_q = jnp.einsum('bgst,tbd->sbgd', grad_score.astype(jnp.float32), k_head.astype(jnp.float32))
        grad_k = jnp.einsum('bgst,sbgd->tbd', grad_score.astype(jnp.float32), q_head.astype(jnp.float32))
        return grad_q, grad_k, grad_v

    gq_heads, gk_heads, gv_heads = lax.map(head_backward, (q_heads, k_heads, v_heads, gc_heads))
    grad_q = apply_rope(jnp.moveaxis(gq_heads, 0, 2), cos_tab, -sin_tab).astype(jnp.bfloat16).reshape(tokens, Q_HEADS * HEAD_DIM)
    grad_k = apply_rope(jnp.moveaxis(gk_heads, 0, 2), cos_tab, -sin_tab).astype(jnp.bfloat16).reshape(tokens, KV_HEADS * HEAD_DIM)
    grad_v = jnp.moveaxis(gv_heads, 0, 2).reshape(tokens, KV_HEADS * HEAD_DIM)
    grad_w_query = jnp.dot(h_one.T, grad_q, preferred_element_type=jnp.float32)
    grad_w_key = jnp.dot(h_one.T, grad_k, preferred_element_type=jnp.float32)
    grad_w_value = jnp.dot(h_one.T, grad_v, preferred_element_type=jnp.float32)
    grad_h_one = (jnp.dot(grad_q, w_query.T, preferred_element_type=jnp.float32) + jnp.dot(grad_k, w_key.T, preferred_element_type=jnp.float32) + jnp.dot(grad_v, w_value.T, preferred_element_type=jnp.float32)).astype(jnp.bfloat16)
    ln1_back = jax.vjp(layer_norm_1p, resid_f, ln1_gain, ln1_bias)[1]
    grad_in_ln, grad_ln1_gain, grad_ln1_bias = ln1_back(grad_h_one.astype(jnp.float32))
    grad_in = (grad_mid.astype(jnp.float32) + grad_in_ln).astype(jnp.bfloat16)
    return (resid_out.reshape(resid_in.shape), grad_in.reshape(resid_in.shape), grad_ln1_gain, grad_ln1_bias, grad_ln2_gain, grad_ln2_bias, grad_w_query, grad_w_key, grad_w_value, grad_w_out, grad_w_up, grad_w_down)
```

```python
import functools
import math
import numpy as np
import jax
import jax.numpy as jnp
from jax import lax
from jax.experimental import pallas as pl
from jax.experimental.pallas import tpu as pltpu
from jax.sharding import PartitionSpec as P

KV_HEADS = 8
LN_EPS = 1e-5
ROPE_BASE = 10000.0
F32 = jnp.float32
BF16 = jnp.bfloat16
ANY = pl.BlockSpec(memory_space=pl.ANY)
VMEM = pl.BlockSpec(memory_space=pltpu.VMEM)
VMEM_LIMIT = 67_043_328
CHUNKS = 4


def mm(a, b):
    return jnp.dot(a, b, preferred_element_type=F32)


def mm_bt(a, b):
    return lax.dot_general(a, b, (((1,), (1,)), ((), ())), preferred_element_type=F32)


def mm_at(a, b):
    return lax.dot_general(a, b, (((0,), (0,)), ((), ())), preferred_element_type=F32)


def centre(rows):
    centred = rows - jnp.mean(rows, axis=-1, keepdims=True)
    scale = lax.rsqrt(jnp.mean(centred * centred, axis=-1, keepdims=True) + LN_EPS)
    return centred * scale, scale


def norm_rows(rows, gain, bias):
    normed, _ = centre(rows)
    return normed * (1.0 + gain) + bias


def norm_rows_back(rows, grad, gain):
    normed, scale = centre(rows)
    weighted = grad * (1.0 + gain)
    inner = jnp.mean(weighted * normed, axis=-1, keepdims=True)
    grad_rows = scale * (weighted - jnp.mean(weighted, axis=-1, keepdims=True) - normed * inner)
    return grad_rows, jnp.sum(grad * normed, axis=0, keepdims=True), jnp.sum(grad, axis=0, keepdims=True)


class Sems:
    def __init__(self):
        self.next = 0

    def take(self, count):
        base = self.next
        self.next += count
        return base


def chain_kernel(dims, x_hbm, dy_hbm, pos_ref, freq_ref, g1_ref, b1_ref, g2_ref, b2_ref, wq_hbm, wk_hbm, wv_hbm, wo_hbm, w1_hbm, w2_hbm,
                 h1_out, h2_out, dy_out, dx1_out, act_out, du_out, ctx_out, dqkv_out, mid_out, dmid_out, ysend_out, ykeep_out, hsend_out, hkeep_out, lng_out,
                 wqkv, wo, w1, w2, h1, h2, dyf, dx1, x_own, mid, tmat, act, du, qs, kv, ctx, prob, cosb, sinb, gcs, dqkv, lng,
                 part_a, part_b, part_c, dr_a, dr_b, dr_c, dr_d, snd_a, snd_b, lnk_a, lnk_b, ysend, ykeep, hsend, hkeep,
                 local_sem, out_sem, send_sem, recv_sem):
    seq, d, hd, nq, nk, f, rows = dims
    grp = nq // nk
    half = rows // 2
    cw = d // CHUNKS
    me = lax.axis_index("tp")
    part, peer, diag = me ^ 1, me ^ 2, me ^ 3
    sems = Sems()

    def block(idx, sub=None):
        if sub is None:
            return pl.ds(pl.multiple_of(idx * rows, rows), rows)
        return pl.ds(pl.multiple_of(idx * rows + sub * half, half), half)

    def remote(src, dst, sem, dev):
        return pltpu.make_async_remote_copy(src, dst, send_sem.at[sem], recv_sem.at[sem], device_id={"tp": dev})

    def local(src, dst, idx):
        return pltpu.make_async_copy(src, dst, local_sem.at[idx])

    x_in = local(x_hbm, x_own, 0)
    dy_in = local(dy_hbm, dyf.at[block(me)], 1)
    nqd, nkd = nq * hd, nk * hd
    weight_in = [
        local(wq_hbm, wqkv.at[:, pl.ds(0, nqd)], 2),
        local(wk_hbm, wqkv.at[:, pl.ds(nqd, nkd)], 3),
        local(wv_hbm, wqkv.at[:, pl.ds(nqd + nkd, nkd)], 4),
        local(wo_hbm, wo, 5),
        local(w2_hbm, w2, 6),
        local(w1_hbm, w1, 7),
    ]
    x_in.start()
    dy_in.start()
    barrier = pltpu.get_barrier_semaphore()
    for dev in (part, peer):
        pl.semaphore_signal(barrier, inc=1, device_id={"tp": dev})
    for copy in weight_in:
        copy.start()

    outs = []

    def put(src, dst):
        copy = pltpu.make_async_copy(src, dst, out_sem.at[len(outs)])
        copy.start()
        outs.append(copy)

    class Gather:
        def __init__(self, buf):
            self.buf, self.base = buf, sems.take(6)

        def copy(self, kind, sub):
            owner = (me, me, peer)[kind]
            dev = (peer, part, part)[kind]
            piece = self.buf.at[block(owner, sub)]
            return remote(piece, piece, self.base + 2 * kind + sub, dev)

        def send(self, sub):
            for kind in (0, 1):
                self.copy(kind, sub).start()

        def forward(self, sub):
            self.copy(0, sub).wait_recv()
            self.copy(2, sub).start()

        def finish(self):
            for sub in (0, 1):
                self.copy(1, sub).wait_recv()
                self.copy(2, sub).wait_recv()

    class Scatter:
        def __init__(self, partial, from_part, summed, from_peer=None):
            self.partial, self.from_part, self.summed, self.from_peer = partial, from_part, summed, from_peer
            self.base = sems.take(2 * CHUNKS)
            self.link = sems.take(CHUNKS + 1) if from_peer is not None else None

        def cols(self, i):
            return pl.ds(pl.multiple_of(i * cw, cw), cw)

        def pair(self, i, kind):
            owner = (diag, part)[kind]
            return remote(self.partial.at[block(owner), self.cols(i)], self.from_part.at[kind, :, self.cols(i)], self.base + CHUNKS * kind + i, part)

        def first(self, i):
            top = pl.ds(0, half)
            return remote(self.summed.at[top, self.cols(i)], self.from_peer.at[top, self.cols(i)], self.link + i, peer)

        def second(self):
            low = pl.ds(half, half)
            return remote(self.summed.at[low], self.from_peer.at[low], self.link + CHUNKS, peer)

        def chip_sum(self, i):
            self.pair(i, 0).wait_recv()
            cols = self.cols(i)
            self.summed[:, cols] = self.partial[block(peer), cols] + self.from_part[0, :, cols]
            if self.from_peer is not None:
                self.first(i).start()

        def run(self, chunk, drain=True):
            def step(i, carry):
                self.partial[:, self.cols(i)] = chunk(self.cols(i))
                self.pair(i, 0).start()
                self.pair(i, 1).start()
                if drain:
                    @pl.when(i > 0)
                    def _():
                        self.chip_sum(i - 1)
                return carry

            lax.fori_loop(0, CHUNKS, step, 0)
            if drain:
                self.chip_sum(CHUNKS - 1)
            if self.from_peer is not None:
                self.second().start()

        def drain(self):
            for i in range(CHUNKS):
                self.chip_sum(i)

        def kept(self):
            for i in range(CHUNKS):
                self.pair(i, 1).wait_recv()

        def rows_sum(self, sub):
            if sub == 0:
                self.kept()
                for i in range(CHUNKS):
                    self.first(i).wait_recv()
            else:
                self.second().wait_recv()
            part_rows = pl.ds(sub * half, half)
            return (self.partial[block(me, sub), :] + self.from_part[1, part_rows, :]) + self.from_peer[part_rows, :]

    x_in.wait()
    h1[block(me), :] = norm_rows(x_own[...].astype(F32), g1_ref[...], b1_ref[...]).astype(BF16)
    pl.semaphore_wait(barrier, 2)
    gather_h1, gather_dy = Gather(h1), Gather(dyf)
    for sub in (0, 1):
        gather_h1.send(sub)
    dy_in.wait()
    for sub in (0, 1):
        gather_dy.send(sub)

    pos_rows = jnp.broadcast_to(pos_ref[...].astype(F32), (hd, seq)).T
    angles = pos_rows * freq_ref[...]
    lane = lax.broadcasted_iota(jnp.int32, (seq, hd), 1)
    rot = hd // 4
    cosb[...] = jnp.cos(angles)
    sinb[...] = jnp.where(lane < rot, -1.0, 1.0) * jnp.sin(angles)

    def turn(v, sign):
        other = jnp.where(lane < rot, pltpu.roll(v, hd - rot, 1), pltpu.roll(v, rot, 1))
        other = jnp.where(lane < 2 * rot, other, 0.0)
        return v * cosb[...] + (sign * sinb[...]) * other

    for sub in (0, 1):
        gather_h1.forward(sub)
    for copy in weight_in[:3]:
        copy.wait()
    gather_h1.finish()

    qkv = mm(h1[...], wqkv[...])
    for k in range(nk):
        for g in range(grp):
            lo = (k * grp + g) * hd
            head = qkv[:, lo:lo + hd].astype(BF16).astype(F32)
            qs[k, g * seq:(g + 1) * seq, :] = turn(head, 1.0).astype(BF16)
        lo = nqd + k * hd
        kv[0, k] = turn(qkv[:, lo:lo + hd].astype(BF16).astype(F32), 1.0).astype(BF16)
        lo = nqd + nkd + k * hd
        kv[1, k] = qkv[:, lo:lo + hd].astype(BF16)
    put(h1, h1_out)
    query = lax.rem(lax.broadcasted_iota(jnp.int32, (grp * seq, seq), 0), seq)
    causal = query >= lax.broadcasted_iota(jnp.int32, (grp * seq, seq), 1)
    for k in range(nk):
        scores = jnp.where(causal, mm_bt(qs[k], kv[0, k]) * hd ** -0.5, -1e30)
        exped = jnp.exp(scores - jnp.max(scores, axis=-1, keepdims=True))
        prob[k] = exped / jnp.sum(exped, axis=-1, keepdims=True)
        head_ctx = mm(prob[k].astype(BF16), kv[1, k]).astype(BF16)
        for g in range(grp):
            lo = (k * grp + g) * hd
            ctx[:, lo:lo + hd] = head_ctx[g * seq:(g + 1) * seq, :]
    put(ctx, ctx_out)
    weight_in[3].wait()
    sum_attn = Scatter(part_a, dr_a, snd_a, lnk_a)
    sum_attn.run(lambda cols: mm(ctx[...], wo[:, cols]))

    for sub in (0, 1):
        gather_dy.forward(sub)
    gather_dy.finish()
    weight_in[4].wait()
    put(dyf, dy_out)
    nb = f // 2

    def down_back(j, carry):
        cols = pl.ds(pl.multiple_of(j * nb, nb), nb)
        tmat[:, cols] = mm_bt(dyf[...], w2[cols, :])
        return carry

    lax.fori_loop(0, f // nb, down_back, 0)

    gather_h2 = Gather(h2)
    for sub in (0, 1):
        own = pl.ds(sub * half, half)
        attn_rows = sum_attn.rows_sum(sub).astype(BF16)
        mid_rows = (x_own[own, :].astype(F32) + attn_rows.astype(F32)).astype(BF16)
        mid[own, :] = mid_rows
        h2[block(me, sub), :] = norm_rows(mid_rows.astype(F32), g2_ref[...], b2_ref[...]).astype(BF16)
        gather_h2.send(sub)
    put(mid, mid_out)
    weight_in[5].wait()
    for sub in (0, 1):
        gather_h2.forward(sub)
    gather_h2.finish()

    def up(j, carry):
        cols = pl.ds(pl.multiple_of(j * nb, nb), nb)
        relu_up = jnp.maximum(mm(h2[...], w1[:, cols]).astype(BF16).astype(F32), 0.0)
        act[:, cols] = (relu_up * relu_up).astype(BF16)
        du[:, cols] = (tmat[:, cols] * (2.0 * relu_up)).astype(BF16)
        return carry

    lax.fori_loop(0, f // nb, up, 0)
    put(h2, h2_out)
    put(act, act_out)
    put(du, du_out)
    sum_dh2 = Scatter(part_b, dr_b, snd_b, lnk_b)
    sum_dh2.run(lambda cols: mm_bt(du[...], w1[cols, :]))

    sum_mlp = Scatter(part_c, dr_c, ysend)
    sum_mlp.run(lambda cols: mm(act[...], w2[:, cols]), drain=False)
    sum_mlp.drain()
    sum_mlp.kept()
    ykeep[...] = part_c[block(me), :] + dr_c[1]
    put(ysend, ysend_out)
    put(ykeep, ykeep_out)

    gather_dx1 = Gather(dx1)
    for sub in (0, 1):
        own = pl.ds(sub * half, half)
        dh2_rows = sum_dh2.rows_sum(sub).astype(BF16).astype(F32)
        grad_rows, grad_gain, grad_bias = norm_rows_back(mid[own, :].astype(F32), dh2_rows, g2_ref[...])
        dx1[block(me, sub), :] = (dyf[block(me, sub), :].astype(F32) + grad_rows).astype(BF16)
        gather_dx1.send(sub)
        if sub == 0:
            lng[0:1, :] = grad_gain
            lng[1:2, :] = grad_bias
        else:
            lng[0:1, :] += grad_gain
            lng[1:2, :] += grad_bias
    put(lng, lng_out)
    put(dx1.at[block(me)], dmid_out)
    for sub in (0, 1):
        gather_dx1.forward(sub)
    gather_dx1.finish()
    put(dx1, dx1_out)

    dctx = mm_bt(dx1[...], wo[...]).astype(BF16)
    for k in range(nk):
        for g in range(grp):
            lo = (k * grp + g) * hd
            gcs[k, g * seq:(g + 1) * seq, :] = dctx[:, lo:lo + hd]
    for k in range(nk):
        grad_v = mm_at(prob[k].astype(BF16), gcs[k]).astype(BF16)
        grad_p = mm_bt(gcs[k], kv[1, k])
        grad_s = (prob[k] * (grad_p - jnp.sum(grad_p * prob[k], axis=-1, keepdims=True)) * hd ** -0.5).astype(BF16)
        grad_q = mm(grad_s, kv[0, k])
        for g in range(grp):
            lo = (k * grp + g) * hd
            dqkv[:, lo:lo + hd] = turn(grad_q[g * seq:(g + 1) * seq, :], -1.0).astype(BF16)
        lo = nqd + k * hd
        dqkv[:, lo:lo + hd] = turn(mm_at(grad_s, qs[k]), -1.0).astype(BF16)
        lo = nqd + nkd + k * hd
        dqkv[:, lo:lo + hd] = grad_v
    put(dqkv, dqkv_out)
    sum_dh1 = Scatter(part_a, dr_d, hsend)
    for i in range(CHUNKS):
        sum_attn.pair(i, 0).wait_send()
        sum_attn.pair(i, 1).wait_send()
    sum_dh1.run(lambda cols: mm_bt(dqkv[...], wqkv[cols, :]))
    put(hsend, hsend_out)
    sum_dh1.kept()
    hkeep[...] = part_a[block(me), :] + dr_d[1]
    put(hkeep, hkeep_out)

    for gather in (gather_h1, gather_dy, gather_h2, gather_dx1):
        for kind in (0, 1, 2):
            for sub in (0, 1):
                gather.copy(kind, sub).wait_send()
    for scatter in (sum_attn, sum_dh2, sum_mlp, sum_dh1):
        for i in range(CHUNKS):
            if scatter is not sum_attn:
                scatter.pair(i, 0).wait_send()
                scatter.pair(i, 1).wait_send()
            if scatter.from_peer is not None:
                scatter.first(i).wait_send()
        if scatter.from_peer is not None:
            scatter.second().wait_send()
    for copy in outs:
        copy.wait()


def chain(dims, x, dy, pos, freq, g1, b1, g2, b2, wq, wk, wv, wo, w1, w2):
    seq, d, hd, nq, nk, f, rows = dims
    grp = nq // nk
    nqd, nkd = nq * hd, nk * hd
    n_all = nqd + 2 * nkd

    def arr(shape, dtype):
        return jax.ShapeDtypeStruct(shape, dtype)

    def vm(*shape, dtype=BF16):
        return pltpu.VMEM(shape, dtype)

    def vf(*shape):
        return pltpu.VMEM(shape, F32)

    out_shape = [arr((seq, d), BF16)] * 4 + [arr((seq, f), BF16)] * 2 + [arr((seq, nqd), BF16), arr((seq, n_all), BF16)] + [arr((rows, d), BF16)] * 2 + [arr((rows, d), F32)] * 4 + [arr((2, d), F32)]
    scratch = [
        vm(d, n_all), vm(nqd, d), vm(d, f), vm(f, d),
        vm(seq, d), vm(seq, d), vm(seq, d), vm(seq, d),
        vm(rows, d), vm(rows, d), vf(seq, f), vm(seq, f), vm(seq, f),
        vm(nk, grp * seq, hd), vm(2, nk, seq, hd), vm(seq, nqd), vf(nk, grp * seq, seq),
        vf(seq, hd), vf(seq, hd), vm(nk, grp * seq, hd), vm(seq, n_all), vf(2, d),
        vf(seq, d), vf(seq, d), vf(seq, d),
        vf(2, rows, d), vf(2, rows, d), vf(2, rows, d), vf(2, rows, d),
        vf(rows, d), vf(rows, d), vf(rows, d), vf(rows, d),
        vf(rows, d), vf(rows, d), vf(rows, d), vf(rows, d),
        pltpu.SemaphoreType.DMA((8,)), pltpu.SemaphoreType.DMA((15,)),
        pltpu.SemaphoreType.DMA((4 * 6 + 4 * 2 * CHUNKS + 2 * (CHUNKS + 1),)),
        pltpu.SemaphoreType.DMA((4 * 6 + 4 * 2 * CHUNKS + 2 * (CHUNKS + 1),)),
    ]
    return pl.pallas_call(
        functools.partial(chain_kernel, dims),
        out_shape=out_shape,
        in_specs=[ANY, ANY] + [VMEM] * 6 + [ANY] * 6,
        out_specs=[ANY] * len(out_shape),
        scratch_shapes=scratch,
        compiler_params=pltpu.CompilerParams(collective_id=0, has_side_effects=True, vmem_limit_bytes=VMEM_LIMIT),
        name="chain",
    )(x, dy, pos, freq, g1, b1, g2, b2, wq, wk, wv, wo, w1, w2)


SLOTS = 4
TILE = 256


def stream_grads(jobs, stage, sem):
    base = 0
    for tiles, width, compute, targets in jobs:
        def copies(i, slot):
            return [pltpu.make_async_copy(stage.at[slot, :, pl.ds(lo, n)], dst, sem.at[slot, c]) for c, (dst, lo, n) in enumerate(targets(i))]

        def step(i, carry):
            slot = lax.rem(i, SLOTS)

            @pl.when(i >= SLOTS)
            def _():
                for copy in copies(i - SLOTS, slot):
                    copy.wait()

            stage[slot, :, :width] = compute(i)
            for copy in copies(i, slot):
                copy.start()
            return carry

        lax.fori_loop(0, tiles, step, 0)
        for i in range(max(tiles - SLOTS, 0), tiles):
            for copy in copies(i, i % SLOTS):
                copy.wait()


def grads_first_kernel(act_hbm, dy_hbm, ctx_hbm, dx1_hbm, dw2, dwo, act, dyf, ctx, dx1, stage, in_sem, sem):
    loads = [pltpu.make_async_copy(s, t, in_sem.at[i]) for i, (s, t) in enumerate(((act_hbm, act), (dy_hbm, dyf), (ctx_hbm, ctx), (dx1_hbm, dx1)))]
    for copy in loads:
        copy.start()
    loads[0].wait()
    loads[1].wait()

    def tile(i):
        return pl.ds(pl.multiple_of(i * TILE, TILE), TILE)

    d = dyf.shape[1]
    stream_grads([(act.shape[1] // TILE, d, lambda i: mm_at(act[:, tile(i)], dyf[...]), lambda i: [(dw2.at[tile(i)], 0, d)])], stage, sem)
    loads[2].wait()
    loads[3].wait()
    stream_grads([(ctx.shape[1] // TILE, d, lambda i: mm_at(ctx[:, tile(i)], dx1[...]), lambda i: [(dwo.at[tile(i)], 0, d)])], stage, sem)


def grads_second_kernel(dims, h2_hbm, du_hbm, h1_hbm, dqkv_hbm, dw1, dwq, dwk, dwv, h2, du, h1, dqkv, stage, in_sem, sem):
    seq, d, hd, nq, nk, f, rows = dims
    loads = [pltpu.make_async_copy(s, t, in_sem.at[i]) for i, (s, t) in enumerate(((h2_hbm, h2), (du_hbm, du), (h1_hbm, h1), (dqkv_hbm, dqkv)))]
    for copy in loads:
        copy.start()
    loads[0].wait()
    loads[1].wait()

    def tile(i):
        return pl.ds(pl.multiple_of(i * TILE, TILE), TILE)

    nqd, nkd = nq * hd, nk * hd
    stream_grads([(d // TILE, f, lambda i: mm_at(h2[:, tile(i)], du[...]), lambda i: [(dw1.at[tile(i)], 0, f)])], stage, sem)
    loads[2].wait()
    loads[3].wait()
    stream_grads([(d // TILE, nqd + 2 * nkd, lambda i: mm_at(h1[:, tile(i)], dqkv[...]),
                   lambda i: [(dwq.at[tile(i)], 0, nqd), (dwk.at[tile(i)], nqd, nkd), (dwv.at[tile(i)], nqd + nkd, nkd)])], stage, sem)


def cost(flops, nbytes):
    return pl.CostEstimate(flops=flops, bytes_accessed=nbytes, transcendentals=0)


def grads_first(dims, act, dyf, ctx, dx1):
    seq, d, hd, nq, nk, f, rows = dims
    nqd = nq * hd
    return pl.pallas_call(
        grads_first_kernel,
        out_shape=[jax.ShapeDtypeStruct((f, d), F32), jax.ShapeDtypeStruct((nqd, d), F32)],
        in_specs=[ANY] * 4, out_specs=[ANY] * 2,
        scratch_shapes=[pltpu.VMEM((seq, f), BF16), pltpu.VMEM((seq, d), BF16), pltpu.VMEM((seq, nqd), BF16), pltpu.VMEM((seq, d), BF16),
                        pltpu.VMEM((SLOTS, TILE, d), F32), pltpu.SemaphoreType.DMA((4,)), pltpu.SemaphoreType.DMA((SLOTS, 3))],
        compiler_params=pltpu.CompilerParams(vmem_limit_bytes=40 << 20),
        cost_estimate=cost(2 * seq * d * (f + nqd), 4 * d * (f + nqd)),
        name="grads_first",
    )(act, dyf, ctx, dx1)


def grads_second(dims, h2, du, h1, dqkv):
    seq, d, hd, nq, nk, f, rows = dims
    nqd, nkd = nq * hd, nk * hd
    n_all = nqd + 2 * nkd
    return pl.pallas_call(
        functools.partial(grads_second_kernel, dims),
        out_shape=[jax.ShapeDtypeStruct((d, f), F32), jax.ShapeDtypeStruct((d, nqd), F32), jax.ShapeDtypeStruct((d, nkd), F32), jax.ShapeDtypeStruct((d, nkd), F32)],
        in_specs=[ANY] * 4, out_specs=[ANY] * 4,
        scratch_shapes=[pltpu.VMEM((seq, d), BF16), pltpu.VMEM((seq, f), BF16), pltpu.VMEM((seq, d), BF16), pltpu.VMEM((seq, n_all), BF16),
                        pltpu.VMEM((SLOTS, TILE, f), F32), pltpu.SemaphoreType.DMA((4,)), pltpu.SemaphoreType.DMA((SLOTS, 3))],
        compiler_params=pltpu.CompilerParams(vmem_limit_bytes=40 << 20),
        cost_estimate=cost(2 * seq * d * (f + n_all), 4 * d * (f + n_all)),
        name="grads_second",
    )(h2, du, h1, dqkv)


def last_norm_kernel(hkeep, hrecv, x, dmid, g1, lng2, dx_out, lng_out):
    dh1 = (hkeep[...] + hrecv[...]).astype(BF16).astype(F32)
    grad_rows, grad_gain, grad_bias = norm_rows_back(x[...].astype(F32), dh1, g1[...])
    dx_out[...] = (dmid[...].astype(F32) + grad_rows).astype(BF16)
    lng_out[0:1, :] = grad_gain
    lng_out[1:2, :] = grad_bias
    lng_out[2:4, :] = lng2[...]


def last_norm(hkeep, hrecv, x, dmid, g1, lng2):
    rows, d = x.shape
    return pl.pallas_call(
        last_norm_kernel,
        out_shape=[jax.ShapeDtypeStruct((rows, d), BF16), jax.ShapeDtypeStruct((4, d), F32)],
        in_specs=[VMEM] * 6, out_specs=[VMEM] * 2,
        cost_estimate=cost(rows * d * 20, rows * d * 16),
        name="last_norm",
    )(hkeep, hrecv, x, dmid, g1, lng2)


def layer_step(x, dy, positions, g1, b1, g2, b2, wq, wk, wv, wo, w1, w2, head_dim, n_tp):
    rows, batch, d = x.shape
    seq = positions.shape[0]
    nq, nk, f = wq.shape[1] // head_dim, wk.shape[1] // head_dim, w1.shape[1]
    dims = (seq, d, head_dim, nq, nk, f, rows)
    rot = head_dim // 4
    freq = np.zeros((1, head_dim), np.float32)
    freq[0, :2 * rot] = np.tile(ROPE_BASE ** (-np.arange(rot) / rot), 2)
    x2, dy2 = x.reshape(rows, d), dy.reshape(rows, d)
    g1, b1, g2, b2 = (v.reshape(1, d) for v in (g1, b1, g2, b2))
    (h1, h2, dyf, dx1, act, du, ctx, dqkv, mid, dmid, ysend, ykeep, hsend, hkeep, lng2) = chain(
        dims, x2, dy2, positions.reshape(1, seq), jnp.asarray(freq), g1, b1, g2, b2, wq, wk, wv, wo, w1, w2)
    def swap(v, bit):
        return lax.ppermute(v, 'tp', [(i, i ^ bit) for i in range(n_tp)])

    hrecv = swap(hsend, 2)
    yrecv = swap(ysend, 2)
    dw2, dwo = grads_first(dims, act, dyf, ctx, dx1)
    dx, lng = last_norm(hkeep, hrecv, x2, dmid, g1, lng2)
    others = [swap(lng, bit) for bit in (1, 2, 3)]
    dw1, dwq, dwk, dwv = grads_second(dims, h2, du, h1, dqkv)
    total = (lng + others[0]) + (others[1] + others[2])
    y = (mid.astype(F32) + (ykeep + yrecv).astype(BF16).astype(F32)).astype(BF16)
    return (y.reshape(x.shape), dx.reshape(x.shape), total[0], total[1], total[2], total[3], dwq, dwk, dwv, dwo, dw1, dw2)


def solution(mesh):
    seq_spec = P(('dp', 'tp'))
    col_spec = P(None, 'tp')
    row_spec = P('tp', None)
    grad_col_spec = P('dp', 'tp')
    grad_row_spec = P(('dp', 'tp'), None)
    in_specs = (seq_spec, seq_spec, P('dp'), P(), P(), P(), P(), col_spec, col_spec, col_spec, row_spec, col_spec, row_spec)
    out_specs = (seq_spec, seq_spec, P('dp'), P('dp'), P('dp'), P('dp'), grad_col_spec, grad_col_spec, grad_col_spec, grad_row_spec, grad_col_spec, grad_row_spec)

    def run_layer(resid_in, grad_out, positions, ln1_gain, ln1_bias, ln2_gain, ln2_bias, w_query, w_key, w_value, w_out, w_up, w_down):
        step_fn = functools.partial(layer_step, head_dim=w_key.shape[1] // KV_HEADS, n_tp=mesh.shape['tp'])
        sharded = jax.shard_map(step_fn, mesh=mesh, in_specs=in_specs, out_specs=out_specs, check_vma=False)
        return sharded(resid_in, grad_out, positions, ln1_gain, ln1_bias, ln2_gain, ln2_bias, w_query, w_key, w_value, w_out, w_up, w_down)

    return run_layer
```

```python
import functools
import math
import numpy as np
import jax
import jax.numpy as jnp
from jax import lax
from jax.experimental import pallas as pl
from jax.experimental.pallas import tpu as pltpu
from jax.sharding import PartitionSpec as P

KV_HEADS = 8
LN_EPS = 1e-5
ROPE_BASE = 10000.0
F32 = jnp.float32
BF16 = jnp.bfloat16
ANY = pl.BlockSpec(memory_space=pl.ANY)
VMEM = pl.BlockSpec(memory_space=pltpu.VMEM)
VMEM_LIMIT = 67_043_328
CHUNKS = 4


def mm(a, b):
    return jnp.dot(a, b, preferred_element_type=F32)


def mm_bt(a, b):
    return lax.dot_general(a, b, (((1,), (1,)), ((), ())), preferred_element_type=F32)


def mm_at(a, b):
    return lax.dot_general(a, b, (((0,), (0,)), ((), ())), preferred_element_type=F32)


def centre(rows):
    centred = rows - jnp.mean(rows, axis=-1, keepdims=True)
    scale = lax.rsqrt(jnp.mean(centred * centred, axis=-1, keepdims=True) + LN_EPS)
    return centred * scale, scale


def norm_rows(rows, gain, bias):
    normed, _ = centre(rows)
    return normed * (1.0 + gain) + bias


def norm_rows_back(rows, grad, gain):
    normed, scale = centre(rows)
    weighted = grad * (1.0 + gain)
    inner = jnp.mean(weighted * normed, axis=-1, keepdims=True)
    grad_rows = scale * (weighted - jnp.mean(weighted, axis=-1, keepdims=True) - normed * inner)
    return grad_rows, jnp.sum(grad * normed, axis=0, keepdims=True), jnp.sum(grad, axis=0, keepdims=True)


class Sems:
    def __init__(self):
        self.next = 0

    def take(self, count):
        base = self.next
        self.next += count
        return base


def chain_kernel(dims, x_hbm, dy_hbm, pos_hbm, freq_hbm, g1_hbm, b1_hbm, g2_hbm, b2_hbm, wq_hbm, wk_hbm, wv_hbm, wo_hbm, w1_hbm, w2_hbm,
                 h1_out, h2_out, dy_out, dx1_out, act_out, du_out, ctx_out, dqkv_out, y_out, dmid_out, hsend_out, hkeep_out, lng_out,
                 pos_ref, freq_ref, g1_ref, b1_ref, g2_ref, b2_ref,
                 wqkv, wo, w1, w2, h1, h2, dyf, dx1, x_own, mid, y_own, tmat, act, du, qs, kv, ctx, prob, cosb, sinb, gcs, dqkv, lng,
                 part_a, part_b, part_c, dr_a, dr_b, dr_c, dr_d, snd_a, snd_b, snd_c, lnk_a, lnk_b, lnk_c, hsend, hkeep,
                 local_sem, out_sem, send_sem, recv_sem):
    seq, d, hd, nq, nk, f, rows = dims
    grp = nq // nk
    half = rows // 2
    cw = d // CHUNKS
    me = lax.axis_index("tp")
    part, peer, diag = me ^ 1, me ^ 2, me ^ 3
    sems = Sems()

    def block(idx, sub=None):
        if sub is None:
            return pl.ds(pl.multiple_of(idx * rows, rows), rows)
        return pl.ds(pl.multiple_of(idx * rows + sub * half, half), half)

    def remote(src, dst, sem, dev):
        return pltpu.make_async_remote_copy(src, dst, send_sem.at[sem], recv_sem.at[sem], device_id={"tp": dev})

    def local(src, dst, idx):
        return pltpu.make_async_copy(src, dst, local_sem.at[idx])

    x_in = local(x_hbm, x_own, 0)
    dy_in = local(dy_hbm, dyf.at[block(me)], 1)
    nqd, nkd = nq * hd, nk * hd
    weight_in = [
        local(wq_hbm, wqkv.at[:, pl.ds(0, nqd)], 2),
        local(wk_hbm, wqkv.at[:, pl.ds(nqd, nkd)], 3),
        local(wv_hbm, wqkv.at[:, pl.ds(nqd + nkd, nkd)], 4),
        local(wo_hbm, wo, 5),
        local(w2_hbm, w2, 6),
        local(w1_hbm, w1, 7),
    ]
    small_in = [local(src, dst, 8 + i) for i, (src, dst) in enumerate((
        (g1_hbm, g1_ref), (b1_hbm, b1_ref), (pos_hbm, pos_ref), (freq_hbm, freq_ref), (g2_hbm, g2_ref), (b2_hbm, b2_ref)))]
    x_in.start()
    for copy in small_in:
        copy.start()
    dy_in.start()
    barrier = pltpu.get_barrier_semaphore()
    for dev in (part, peer):
        pl.semaphore_signal(barrier, inc=1, device_id={"tp": dev})
    for copy in weight_in:
        copy.start()

    outs = []

    def put(src, dst):
        copy = pltpu.make_async_copy(src, dst, out_sem.at[len(outs)])
        copy.start()
        outs.append(copy)

    class Gather:
        def __init__(self, buf, pieces):
            self.buf, self.pieces, self.base = buf, pieces, sems.take(3 * len(pieces))

        def copy(self, kind, i):
            owner = (me, me, peer)[kind]
            dev = (peer, part, part)[kind]
            row, n_rows, col, n_cols = self.pieces[i]
            at = self.buf.at[pl.ds(pl.multiple_of(owner * rows + row, half), n_rows), pl.ds(col, n_cols)]
            return remote(at, at, self.base + len(self.pieces) * kind + i, dev)

        def send(self, i):
            self.copy(0, i).start()
            self.copy(1, i).start()

        def forward(self, i):
            self.copy(0, i).wait_recv()
            self.copy(2, i).start()

        def finish(self, i):
            self.copy(1, i).wait_recv()
            self.copy(2, i).wait_recv()

        def feed(self, first, use):
            count = len(self.pieces)
            for i in range(first):
                self.forward(i)
            self.forward(first)
            for i in range(first):
                self.finish(i)
            for i in range(first, count):
                if i + 1 < count:
                    self.forward(i + 1)
                self.finish(i)
                use(i - first, pl.ds(self.pieces[i][2], self.pieces[i][3]))

    class Scatter:
        def __init__(self, partial, from_part, summed, from_peer=None):
            self.partial, self.from_part, self.summed, self.from_peer = partial, from_part, summed, from_peer
            self.base = sems.take(2 * CHUNKS)
            self.link = sems.take(CHUNKS + 1) if from_peer is not None else None

        def cols(self, i):
            return pl.ds(pl.multiple_of(i * cw, cw), cw)

        def pair(self, i, kind):
            owner = (diag, part)[kind]
            return remote(self.partial.at[block(owner), self.cols(i)], self.from_part.at[kind, :, self.cols(i)], self.base + CHUNKS * kind + i, part)

        def first(self, i):
            top = pl.ds(0, half)
            return remote(self.summed.at[top, self.cols(i)], self.from_peer.at[top, self.cols(i)], self.link + i, peer)

        def second(self):
            low = pl.ds(half, half)
            return remote(self.summed.at[low], self.from_peer.at[low], self.link + CHUNKS, peer)

        def chip_sum(self, i):
            self.pair(i, 0).wait_recv()
            cols = self.cols(i)
            self.summed[:, cols] = self.partial[block(peer), cols] + self.from_part[0, :, cols]
            if self.from_peer is not None:
                self.first(i).start()

        def run(self, chunk, drain=True):
            def step(i, carry):
                self.partial[:, self.cols(i)] = chunk(self.cols(i))
                self.pair(i, 0).start()
                self.pair(i, 1).start()
                if drain:
                    @pl.when(i > 0)
                    def _():
                        self.chip_sum(i - 1)
                return carry

            lax.fori_loop(0, CHUNKS, step, 0)
            if drain:
                self.chip_sum(CHUNKS - 1)
                if self.from_peer is not None:
                    self.second().start()

        def drain(self):
            for i in range(CHUNKS):
                self.chip_sum(i)
            self.second().start()

        def kept(self):
            for i in range(CHUNKS):
                self.pair(i, 1).wait_recv()

        def rows_sum(self, sub):
            if sub == 0:
                self.kept()
                for i in range(CHUNKS):
                    self.first(i).wait_recv()
            else:
                self.second().wait_recv()
            part_rows = pl.ds(sub * half, half)
            return (self.partial[block(me, sub), :] + self.from_part[1, part_rows, :]) + self.from_peer[part_rows, :]

    x_in.wait()
    small_in[0].wait()
    small_in[1].wait()
    h1[block(me), :] = norm_rows(x_own[...].astype(F32), g1_ref[...], b1_ref[...]).astype(BF16)
    pl.semaphore_wait(barrier, 2)
    wide = [(0, rows, i * cw, cw) for i in range(CHUNKS)]
    late = [(0, half, 0, d)] + [(half, half, i * cw, cw) for i in range(CHUNKS)]
    gather_h1, gather_dy = Gather(h1, wide), Gather(dyf, [(0, rows, 0, d)])
    for i in range(CHUNKS):
        gather_h1.send(i)
    dy_in.wait()
    gather_dy.send(0)

    small_in[2].wait()
    small_in[3].wait()
    pos_rows = jnp.broadcast_to(pos_ref[...].astype(F32), (hd, seq)).T
    angles = pos_rows * freq_ref[...]
    lane = lax.broadcasted_iota(jnp.int32, (seq, hd), 1)
    rot = hd // 4
    cosb[...] = jnp.cos(angles)
    sinb[...] = jnp.where(lane < rot, -1.0, 1.0) * jnp.sin(angles)

    def turn(v, sign):
        other = jnp.where(lane < rot, pltpu.roll(v, hd - rot, 1), pltpu.roll(v, rot, 1))
        other = jnp.where(lane < 2 * rot, other, 0.0)
        return v * cosb[...] + (sign * sinb[...]) * other

    for copy in weight_in[:3]:
        copy.wait()
    n_all = nqd + 2 * nkd

    def add(total, j, piece):
        total[...] = piece if j == 0 else total[...] + piece

    qkv_sum = part_c.at[:, pl.ds(0, n_all)]
    gather_h1.feed(0, lambda j, cols: add(qkv_sum, j, mm(h1[:, cols], wqkv[cols, :])))

    qkv = qkv_sum
    for k in range(nk):
        for g in range(grp):
            lo = (k * grp + g) * hd
            head = qkv[:, lo:lo + hd].astype(BF16).astype(F32)
            qs[k, g * seq:(g + 1) * seq, :] = turn(head, 1.0).astype(BF16)
        lo = nqd + k * hd
        kv[0, k] = turn(qkv[:, lo:lo + hd].astype(BF16).astype(F32), 1.0).astype(BF16)
        lo = nqd + nkd + k * hd
        kv[1, k] = qkv[:, lo:lo + hd].astype(BF16)
    put(h1, h1_out)
    query = lax.rem(lax.broadcasted_iota(jnp.int32, (grp * seq, seq), 0), seq)
    causal = query >= lax.broadcasted_iota(jnp.int32, (grp * seq, seq), 1)
    for k in range(nk):
        scores = jnp.where(causal, mm_bt(qs[k], kv[0, k]) * hd ** -0.5, -1e30)
        exped = jnp.exp(scores - jnp.max(scores, axis=-1, keepdims=True))
        prob[k] = exped / jnp.sum(exped, axis=-1, keepdims=True)
        head_ctx = mm(prob[k].astype(BF16), kv[1, k]).astype(BF16)
        for g in range(grp):
            lo = (k * grp + g) * hd
            ctx[:, lo:lo + hd] = head_ctx[g * seq:(g + 1) * seq, :]
    put(ctx, ctx_out)
    weight_in[3].wait()
    sum_attn = Scatter(part_a, dr_a, snd_a, lnk_a)
    sum_attn.run(lambda cols: mm(ctx[...], wo[:, cols]))

    gather_dy.forward(0)
    gather_dy.finish(0)
    weight_in[4].wait()
    put(dyf, dy_out)
    nb = f // 2

    def down_back(j, carry):
        cols = pl.ds(pl.multiple_of(j * nb, nb), nb)
        tmat[:, cols] = mm_bt(dyf[...], w2[cols, :])
        return carry

    lax.fori_loop(0, f // nb, down_back, 0)

    gather_h2 = Gather(h2, late)
    small_in[4].wait()
    small_in[5].wait()
    for sub in (0, 1):
        own = pl.ds(sub * half, half)
        attn_rows = sum_attn.rows_sum(sub).astype(BF16)
        mid_rows = (x_own[own, :].astype(F32) + attn_rows.astype(F32)).astype(BF16)
        mid[own, :] = mid_rows
        h2[block(me, sub), :] = norm_rows(mid_rows.astype(F32), g2_ref[...], b2_ref[...]).astype(BF16)
        for i in ((0,) if sub == 0 else range(1, 1 + CHUNKS)):
            gather_h2.send(i)
    weight_in[5].wait()

    def up(j, depth):
        def step(i, carry):
            cols = pl.ds(pl.multiple_of(i * nb, nb), nb)
            piece = mm(h2[:, depth], w1[depth, cols])
            if j == 0:
                part_c[:, cols] = piece
            elif j < CHUNKS - 1:
                part_c[:, cols] += piece
            else:
                relu_up = jnp.maximum((part_c[:, cols] + piece).astype(BF16).astype(F32), 0.0)
                act[:, cols] = (relu_up * relu_up).astype(BF16)
                du[:, cols] = (tmat[:, cols] * (2.0 * relu_up)).astype(BF16)
            return carry

        lax.fori_loop(0, f // nb, step, 0)

    gather_h2.feed(1, up)
    put(h2, h2_out)
    put(act, act_out)
    put(du, du_out)
    sum_dh2 = Scatter(part_b, dr_b, snd_b, lnk_b)
    sum_dh2.run(lambda cols: mm_bt(du[...], w1[cols, :]))

    sum_mlp = Scatter(part_c, dr_c, snd_c, lnk_c)
    sum_mlp.run(lambda cols: mm(act[...], w2[:, cols]), drain=False)

    gather_dx1 = Gather(dx1, late)
    for sub in (0, 1):
        own = pl.ds(sub * half, half)
        dh2_rows = sum_dh2.rows_sum(sub).astype(BF16).astype(F32)
        grad_rows, grad_gain, grad_bias = norm_rows_back(mid[own, :].astype(F32), dh2_rows, g2_ref[...])
        dx1[block(me, sub), :] = (dyf[block(me, sub), :].astype(F32) + grad_rows).astype(BF16)
        for i in ((0,) if sub == 0 else range(1, 1 + CHUNKS)):
            gather_dx1.send(i)
        if sub == 0:
            lng[0:1, :] = grad_gain
            lng[1:2, :] = grad_bias
        else:
            lng[0:1, :] += grad_gain
            lng[1:2, :] += grad_bias
    put(lng, lng_out)
    put(dx1.at[block(me)], dmid_out)
    sum_mlp.drain()
    dctx_sum = tmat.at[:, pl.ds(0, nqd)]
    gather_dx1.feed(1, lambda j, cols: add(dctx_sum, j, mm_bt(dx1[:, cols], wo[:, cols])))
    put(dx1, dx1_out)

    dctx = dctx_sum[...].astype(BF16)
    for k in range(nk):
        for g in range(grp):
            lo = (k * grp + g) * hd
            gcs[k, g * seq:(g + 1) * seq, :] = dctx[:, lo:lo + hd]
    for k in range(nk):
        grad_v = mm_at(prob[k].astype(BF16), gcs[k]).astype(BF16)
        grad_p = mm_bt(gcs[k], kv[1, k])
        grad_s = (prob[k] * (grad_p - jnp.sum(grad_p * prob[k], axis=-1, keepdims=True)) * hd ** -0.5).astype(BF16)
        grad_q = mm(grad_s, kv[0, k])
        for g in range(grp):
            lo = (k * grp + g) * hd
            dqkv[:, lo:lo + hd] = turn(grad_q[g * seq:(g + 1) * seq, :], -1.0).astype(BF16)
        lo = nqd + k * hd
        dqkv[:, lo:lo + hd] = turn(mm_at(grad_s, qs[k]), -1.0).astype(BF16)
        lo = nqd + nkd + k * hd
        dqkv[:, lo:lo + hd] = grad_v
    put(dqkv, dqkv_out)
    sum_dh1 = Scatter(part_a, dr_d, hsend)
    for i in range(CHUNKS):
        sum_attn.pair(i, 0).wait_send()
        sum_attn.pair(i, 1).wait_send()
    sum_dh1.run(lambda cols: mm_bt(dqkv[...], wqkv[cols, :]))
    put(hsend, hsend_out)
    sum_dh1.kept()
    hkeep[...] = part_a[block(me), :] + dr_d[1]
    put(hkeep, hkeep_out)
    for sub in (0, 1):
        own = pl.ds(sub * half, half)
        y_own[own, :] = (mid[own, :].astype(F32) + sum_mlp.rows_sum(sub).astype(BF16).astype(F32)).astype(BF16)
    put(y_own, y_out)

    for gather in (gather_h1, gather_dy, gather_h2, gather_dx1):
        for kind in (0, 1, 2):
            for i in range(len(gather.pieces)):
                gather.copy(kind, i).wait_send()
    for scatter in (sum_attn, sum_dh2, sum_mlp, sum_dh1):
        for i in range(CHUNKS):
            if scatter is not sum_attn:
                scatter.pair(i, 0).wait_send()
                scatter.pair(i, 1).wait_send()
            if scatter.from_peer is not None:
                scatter.first(i).wait_send()
        if scatter.from_peer is not None:
            scatter.second().wait_send()
    for copy in outs:
        copy.wait()


def chain(dims, x, dy, pos, freq, g1, b1, g2, b2, wq, wk, wv, wo, w1, w2):
    seq, d, hd, nq, nk, f, rows = dims
    grp = nq // nk
    nqd, nkd = nq * hd, nk * hd
    n_all = nqd + 2 * nkd

    def arr(shape, dtype):
        return jax.ShapeDtypeStruct(shape, dtype)

    def vm(*shape, dtype=BF16):
        return pltpu.VMEM(shape, dtype)

    def vf(*shape):
        return pltpu.VMEM(shape, F32)

    out_shape = [arr((seq, d), BF16)] * 4 + [arr((seq, f), BF16)] * 2 + [arr((seq, nqd), BF16), arr((seq, n_all), BF16)] + [arr((rows, d), BF16)] * 2 + [arr((rows, d), F32)] * 2 + [arr((2, d), F32)]
    n_sems = CHUNKS + 1 + 2 * (CHUNKS + 1)
    n_sems = 3 * n_sems + 4 * 2 * CHUNKS + 3 * (CHUNKS + 1)
    scratch = [
        pltpu.VMEM((1, seq), jnp.int32), vf(1, hd), vf(1, d), vf(1, d), vf(1, d), vf(1, d),
        vm(d, n_all), vm(nqd, d), vm(d, f), vm(f, d),
        vm(seq, d), vm(seq, d), vm(seq, d), vm(seq, d),
        vm(rows, d), vm(rows, d), vm(rows, d), vf(seq, f), vm(seq, f), vm(seq, f),
        vm(nk, grp * seq, hd), vm(2, nk, seq, hd), vm(seq, nqd), vf(nk, grp * seq, seq),
        vf(seq, hd), vf(seq, hd), vm(nk, grp * seq, hd), vm(seq, n_all), vf(2, d),
        vf(seq, d), vf(seq, d), vf(seq, d),
        vf(2, rows, d), vf(2, rows, d), vf(2, rows, d), vf(2, rows, d),
        vf(rows, d), vf(rows, d), vf(rows, d), vf(rows, d),
        vf(rows, d), vf(rows, d), vf(rows, d), vf(rows, d),
        pltpu.SemaphoreType.DMA((14,)), pltpu.SemaphoreType.DMA((len(out_shape),)),
        pltpu.SemaphoreType.DMA((n_sems,)), pltpu.SemaphoreType.DMA((n_sems,)),
    ]
    return pl.pallas_call(
        functools.partial(chain_kernel, dims),
        out_shape=out_shape,
        in_specs=[ANY] * 14,
        out_specs=[ANY] * len(out_shape),
        scratch_shapes=scratch,
        compiler_params=pltpu.CompilerParams(collective_id=0, has_side_effects=True, vmem_limit_bytes=VMEM_LIMIT),
        name="chain",
    )(x, dy, pos, freq, g1, b1, g2, b2, wq, wk, wv, wo, w1, w2)


SLOTS = 4
TILE = 256


def stream_grads(jobs, stage, sem):
    def copies(targets, i, slot):
        return [pltpu.make_async_copy(stage.at[slot, :, pl.ds(lo, n)], dst, sem.at[slot, c]) for c, (dst, lo, n) in enumerate(targets(i))]

    done, pending = 0, []
    for ready, tiles, width, compute, targets in jobs:
        ready()

        def fill(i, slot):
            stage[slot, :, :width] = compute(i)
            for copy in copies(targets, i, slot):
                copy.start()

        lead = min(SLOTS, tiles)
        for i in range(lead):
            slot = (done + i) % SLOTS
            if len(pending) == SLOTS:
                for copy in pending.pop(0):
                    copy.wait()
            fill(i, slot)
            pending.append(copies(targets, i, slot))

        def step(i, carry, base=done):
            slot = lax.rem(base + i, SLOTS)
            for copy in copies(targets, i - SLOTS, slot):
                copy.wait()
            fill(i, slot)
            return carry

        lax.fori_loop(lead, tiles, step, 0)
        if tiles > SLOTS:
            pending = [copies(targets, i, (done + i) % SLOTS) for i in range(tiles - SLOTS, tiles)]
        done += tiles
    for group in pending:
        for copy in group:
            copy.wait()


def grads_first_kernel(act_hbm, dy_hbm, ctx_hbm, dx1_hbm, dw2, dwo, act, dyf, ctx, dx1, stage, in_sem, sem):
    loads = [pltpu.make_async_copy(s, t, in_sem.at[i]) for i, (s, t) in enumerate(((act_hbm, act), (dy_hbm, dyf), (ctx_hbm, ctx), (dx1_hbm, dx1)))]
    for copy in loads:
        copy.start()

    def ready(*which):
        return lambda: [loads[i].wait() for i in which]

    def tile(i):
        return pl.ds(pl.multiple_of(i * TILE, TILE), TILE)

    d = dyf.shape[1]
    stream_grads([
        (ready(0, 1), act.shape[1] // TILE, d, lambda i: mm_at(act[:, tile(i)], dyf[...]), lambda i: [(dw2.at[tile(i)], 0, d)]),
        (ready(2, 3), ctx.shape[1] // TILE, d, lambda i: mm_at(ctx[:, tile(i)], dx1[...]), lambda i: [(dwo.at[tile(i)], 0, d)]),
    ], stage, sem)


def grads_second_kernel(dims, order, y_hbm, h2_hbm, du_hbm, h1_hbm, dqkv_hbm, y_out, dw1, dwq, dwk, dwv, y, h2, du, h1, dqkv, stage, in_sem, sem):
    seq, d, hd, nq, nk, f, rows = dims
    loads = [pltpu.make_async_copy(s, t, in_sem.at[i]) for i, (s, t) in enumerate(((h2_hbm, h2), (du_hbm, du), (h1_hbm, h1), (dqkv_hbm, dqkv), (y_hbm, y)))]
    for copy in loads:
        copy.start()

    def ready(*which):
        return lambda: [loads[i].wait() for i in which]

    def tile(i):
        return pl.ds(pl.multiple_of(i * TILE, TILE), TILE)

    nqd, nkd = nq * hd, nk * hd
    y_copy = pltpu.make_async_copy(y, y_out, in_sem.at[5])

    def ready_rest():
        for i in (2, 3, 4):
            loads[i].wait()
        y_copy.start()

    stream_grads([
        (ready(0, 1), d // TILE, f, lambda i: mm_at(h2[:, tile(i)], du[...]), lambda i: [(dw1.at[tile(i)], 0, f)]),
        (ready_rest, d // TILE, nqd + 2 * nkd, lambda i: mm_at(h1[:, tile(i)], dqkv[...]),
         lambda i: [(dwq.at[tile(i)], 0, nqd), (dwk.at[tile(i)], nqd, nkd), (dwv.at[tile(i)], nqd + nkd, nkd)]),
    ], stage, sem)
    y_copy.wait()


def cost(flops, nbytes):
    return pl.CostEstimate(flops=flops, bytes_accessed=nbytes, transcendentals=0)


def grads_first(dims, act, dyf, ctx, dx1):
    seq, d, hd, nq, nk, f, rows = dims
    nqd = nq * hd
    return pl.pallas_call(
        grads_first_kernel,
        out_shape=[jax.ShapeDtypeStruct((f, d), F32), jax.ShapeDtypeStruct((nqd, d), F32)],
        in_specs=[ANY] * 4, out_specs=[ANY] * 2,
        scratch_shapes=[pltpu.VMEM((seq, f), BF16), pltpu.VMEM((seq, d), BF16), pltpu.VMEM((seq, nqd), BF16), pltpu.VMEM((seq, d), BF16),
                        pltpu.VMEM((SLOTS, TILE, d), F32), pltpu.SemaphoreType.DMA((4,)), pltpu.SemaphoreType.DMA((SLOTS, 3))],
        compiler_params=pltpu.CompilerParams(vmem_limit_bytes=VMEM_LIMIT),
        cost_estimate=cost(2 * seq * d * (f + nqd), 4 * d * (f + nqd)),
        name="grads_first",
    )(act, dyf, ctx, dx1)


def grads_second(dims, order, y, h2, du, h1, dqkv):
    seq, d, hd, nq, nk, f, rows = dims
    nqd, nkd = nq * hd, nk * hd
    n_all = nqd + 2 * nkd
    return pl.pallas_call(
        functools.partial(grads_second_kernel, dims),
        out_shape=[jax.ShapeDtypeStruct((rows, d), BF16), jax.ShapeDtypeStruct((d, f), F32), jax.ShapeDtypeStruct((d, nqd), F32), jax.ShapeDtypeStruct((d, nkd), F32), jax.ShapeDtypeStruct((d, nkd), F32)],
        in_specs=[ANY] * 6, out_specs=[ANY] * 5,
        scratch_shapes=[pltpu.VMEM((rows, d), BF16), pltpu.VMEM((seq, d), BF16), pltpu.VMEM((seq, f), BF16), pltpu.VMEM((seq, d), BF16), pltpu.VMEM((seq, n_all), BF16),
                        pltpu.VMEM((SLOTS, TILE, f), F32), pltpu.SemaphoreType.DMA((6,)), pltpu.SemaphoreType.DMA((SLOTS, 3))],
        compiler_params=pltpu.CompilerParams(vmem_limit_bytes=VMEM_LIMIT),
        cost_estimate=cost(2 * seq * d * (f + n_all), 4 * d * (f + n_all)),
        name="grads_second",
    )(order, y, h2, du, h1, dqkv)


def last_norm_kernel(order, hkeep, hrecv, x, dmid, g1, lng2, dx_out, lng_out):
    dh1 = (hkeep[...] + hrecv[...]).astype(BF16).astype(F32)
    grad_rows, grad_gain, grad_bias = norm_rows_back(x[...].astype(F32), dh1, g1[...])
    dx_out[...] = (dmid[...].astype(F32) + grad_rows).astype(BF16)
    lng_out[0:1, :] = grad_gain
    lng_out[1:2, :] = grad_bias
    lng_out[2:4, :] = lng2[...]


def last_norm(order, hkeep, hrecv, x, dmid, g1, lng2):
    rows, d = x.shape
    return pl.pallas_call(
        last_norm_kernel,
        out_shape=[jax.ShapeDtypeStruct((rows, d), BF16), jax.ShapeDtypeStruct((4, d), F32)],
        in_specs=[ANY] + [VMEM] * 6, out_specs=[VMEM] * 2,
        cost_estimate=cost(rows * d * 20, rows * d * 16),
        name="last_norm",
    )(order, hkeep, hrecv, x, dmid, g1, lng2)


def layer_step(x, dy, positions, g1, b1, g2, b2, wq, wk, wv, wo, w1, w2, head_dim, n_tp):
    rows, batch, d = x.shape
    seq = positions.shape[0]
    nq, nk, f = wq.shape[1] // head_dim, wk.shape[1] // head_dim, w1.shape[1]
    dims = (seq, d, head_dim, nq, nk, f, rows)
    rot = head_dim // 4
    freq = np.zeros((1, head_dim), np.float32)
    freq[0, :2 * rot] = np.tile(ROPE_BASE ** (-np.arange(rot) / rot), 2)
    x2, dy2 = x.reshape(rows, d), dy.reshape(rows, d)
    g1, b1, g2, b2 = (v.reshape(1, d) for v in (g1, b1, g2, b2))
    (h1, h2, dyf, dx1, act, du, ctx, dqkv, y, dmid, hsend, hkeep, lng2) = chain(
        dims, x2, dy2, positions.reshape(1, seq), jnp.asarray(freq), g1, b1, g2, b2, wq, wk, wv, wo, w1, w2)

    def swap(v, bit):
        return lax.ppermute(v, 'tp', [(i, i ^ bit) for i in range(n_tp)])

    hrecv = swap(hsend, 2)
    dw2, dwo = grads_first(dims, act, dyf, ctx, dx1)
    dx, lng = last_norm(dwo, hkeep, hrecv, x2, dmid, g1, lng2)
    others = [swap(lng, bit) for bit in (1, 2, 3)]
    y, dw1, dwq, dwk, dwv = grads_second(dims, lng, y, h2, du, h1, dqkv)
    total = (lng + others[0]) + (others[1] + others[2])
    return (y.reshape(x.shape), dx.reshape(x.shape), total[0], total[1], total[2], total[3], dwq, dwk, dwv, dwo, dw1, dw2)


def solution(mesh):
    seq_spec = P(('dp', 'tp'))
    col_spec = P(None, 'tp')
    row_spec = P('tp', None)
    grad_col_spec = P('dp', 'tp')
    grad_row_spec = P(('dp', 'tp'), None)
    in_specs = (seq_spec, seq_spec, P('dp'), P(), P(), P(), P(), col_spec, col_spec, col_spec, row_spec, col_spec, row_spec)
    out_specs = (seq_spec, seq_spec, P('dp'), P('dp'), P('dp'), P('dp'), grad_col_spec, grad_col_spec, grad_col_spec, grad_row_spec, grad_col_spec, grad_row_spec)

    def run_layer(resid_in, grad_out, positions, ln1_gain, ln1_bias, ln2_gain, ln2_bias, w_query, w_key, w_value, w_out, w_up, w_down):
        step_fn = functools.partial(layer_step, head_dim=w_key.shape[1] // KV_HEADS, n_tp=mesh.shape['tp'])
        sharded = jax.shard_map(step_fn, mesh=mesh, in_specs=in_specs, out_specs=out_specs, check_vma=False)
        return sharded(resid_in, grad_out, positions, ln1_gain, ln1_bias, ln2_gain, ln2_bias, w_query, w_key, w_value, w_out, w_up, w_down)

    return run_layer
```

```python
import functools
import math
import numpy as np
import jax
import jax.numpy as jnp
from jax import lax
from jax.experimental import pallas as pl
from jax.experimental.pallas import tpu as pltpu
from jax.sharding import PartitionSpec as P

KV_HEADS = 8
LN_EPS = 1e-5
ROPE_BASE = 10000.0
F32 = jnp.float32
BF16 = jnp.bfloat16
ANY = pl.BlockSpec(memory_space=pl.ANY)
VMEM = pl.BlockSpec(memory_space=pltpu.VMEM)
VMEM_LIMIT = 67_043_328


def mm(a, b):
    return jnp.dot(a, b, preferred_element_type=F32)


def mm_bt(a, b):
    return lax.dot_general(a, b, (((1,), (1,)), ((), ())), preferred_element_type=F32)


def mm_at(a, b):
    return lax.dot_general(a, b, (((0,), (0,)), ((), ())), preferred_element_type=F32)


def centre(rows):
    centred = rows - jnp.mean(rows, axis=-1, keepdims=True)
    scale = lax.rsqrt(jnp.mean(centred * centred, axis=-1, keepdims=True) + LN_EPS)
    return centred * scale, scale


def norm_rows(rows, gain, bias):
    normed, _ = centre(rows)
    return normed * (1.0 + gain) + bias


def norm_rows_back(rows, grad, gain):
    normed, scale = centre(rows)
    weighted = grad * (1.0 + gain)
    inner = jnp.mean(weighted * normed, axis=-1, keepdims=True)
    grad_rows = scale * (weighted - jnp.mean(weighted, axis=-1, keepdims=True) - normed * inner)
    return grad_rows, jnp.sum(grad * normed, axis=0, keepdims=True), jnp.sum(grad, axis=0, keepdims=True)


class Sems:
    def __init__(self):
        self.next = 0

    def take(self, count):
        base = self.next
        self.next += count
        return base


def chain_kernel(dims, x_hbm, dy_hbm, pos_hbm, freq_hbm, g1_hbm, b1_hbm, g2_hbm, b2_hbm, wq_hbm, wk_hbm, wv_hbm, wo_hbm, w1_hbm, w2_hbm,
                 h1_out, h2_out, dy_out, dx1_out, act_out, du_out, ctx_out, dqkv_out, y_out, mid_out, dmid_out, send_out, hkeep_out, ykeep_out, lng_out,
                 pos_ref, freq_ref, g1_ref, b1_ref, g2_ref, b2_ref,
                 wqkv, wo, w1, w2, h1, h2, dyf, dx1, x_own, mid, y_own, tmat, act, du, qs, kv, ctx, prob, cosb, sinb, gcs, dqkv, lng,
                 part_a, part_b, part_c, dr_a, dr_b, dr_c, dr_d, snd_a, snd_b, snd_c, lnk_a, lnk_b, lnk_c, send, hkeep, ykeep,
                 local_sem, out_sem, send_sem, recv_sem):
    seq, d, hd, nq, nk, f, rows = dims
    grp = nq // nk
    half = rows // 2
    me = lax.axis_index("tp")
    part, peer, diag = me ^ 1, me ^ 2, me ^ 3
    sems = Sems()

    def block(idx, sub=None):
        if sub is None:
            return pl.ds(pl.multiple_of(idx * rows, rows), rows)
        return pl.ds(pl.multiple_of(idx * rows + sub * half, half), half)

    def remote(src, dst, sem, dev):
        return pltpu.make_async_remote_copy(src, dst, send_sem.at[sem], recv_sem.at[sem], device_id={"tp": dev})

    def local(src, dst, idx):
        return pltpu.make_async_copy(src, dst, local_sem.at[idx])

    x_in = local(x_hbm, x_own, 0)
    dy_in = local(dy_hbm, dyf.at[block(me)], 1)
    nqd, nkd = nq * hd, nk * hd
    weight_in = [
        local(wq_hbm, wqkv.at[:, pl.ds(0, nqd)], 2),
        local(wk_hbm, wqkv.at[:, pl.ds(nqd, nkd)], 3),
        local(wv_hbm, wqkv.at[:, pl.ds(nqd + nkd, nkd)], 4),
        local(wo_hbm, wo, 5),
        local(w2_hbm, w2, 6),
        local(w1_hbm, w1, 7),
    ]
    small_in = [local(src, dst, 8 + i) for i, (src, dst) in enumerate((
        (g1_hbm, g1_ref), (b1_hbm, b1_ref), (pos_hbm, pos_ref), (freq_hbm, freq_ref), (g2_hbm, g2_ref), (b2_hbm, b2_ref)))]
    x_in.start()
    for copy in small_in:
        copy.start()
    dy_in.start()
    barrier = pltpu.get_barrier_semaphore()
    for dev in (part, peer):
        pl.semaphore_signal(barrier, inc=1, device_id={"tp": dev})
    for copy in weight_in:
        copy.start()

    outs = []

    def put(src, dst):
        copy = pltpu.make_async_copy(src, dst, out_sem.at[len(outs)])
        copy.start()
        outs.append(copy)

    class Gather:
        def __init__(self, buf, pieces):
            self.buf, self.pieces, self.base = buf, pieces, sems.take(3 * len(pieces))

        def copy(self, kind, i):
            owner = (me, me, peer)[kind]
            dev = (peer, part, part)[kind]
            row, n_rows, col, n_cols = self.pieces[i]
            at = self.buf.at[pl.ds(pl.multiple_of(owner * rows + row, half), n_rows), pl.ds(col, n_cols)]
            return remote(at, at, self.base + len(self.pieces) * kind + i, dev)

        def send(self, i):
            self.copy(0, i).start()
            self.copy(1, i).start()

        def forward(self, i):
            self.copy(0, i).wait_recv()
            self.copy(2, i).start()

        def finish(self, i):
            self.copy(1, i).wait_recv()
            self.copy(2, i).wait_recv()

        def feed(self, first, use):
            count = len(self.pieces)
            for i in range(first):
                self.forward(i)
            self.forward(first)
            for i in range(first):
                self.finish(i)
            for i in range(first, count):
                if i + 1 < count:
                    self.forward(i + 1)
                self.finish(i)
                use(i - first, pl.ds(self.pieces[i][2], self.pieces[i][3]))

    class Scatter:
        def __init__(self, chunks, partial, from_part, summed, from_peer=None, link_rows=0):
            self.chunks, self.cw, self.link_rows = chunks, d // chunks, link_rows
            self.partial, self.from_part, self.summed, self.from_peer = partial, from_part, summed, from_peer
            self.base = sems.take(2 * chunks)
            self.link = sems.take(chunks + 1) if link_rows else None

        def cols(self, i):
            return pl.ds(pl.multiple_of(i * self.cw, self.cw), self.cw)

        def pair(self, i, kind):
            owner = (diag, part)[kind]
            return remote(self.partial.at[block(owner), self.cols(i)], self.from_part.at[kind, :, self.cols(i)], self.base + self.chunks * kind + i, part)

        def first(self, i):
            top = pl.ds(0, half)
            return remote(self.summed.at[top, self.cols(i)], self.from_peer.at[top, self.cols(i)], self.link + i, peer)

        def second(self):
            low = pl.ds(half, half)
            return remote(self.summed.at[low], self.from_peer.at[low], self.link + self.chunks, peer)

        def chip_sum(self, i):
            self.pair(i, 0).wait_recv()
            cols = self.cols(i)
            self.summed[:, cols] = self.partial[block(peer), cols] + self.from_part[0, :, cols]
            if self.link_rows:
                self.first(i).start()

        def run(self, chunk, drain=True):
            def step(i, carry):
                self.partial[:, self.cols(i)] = chunk(self.cols(i))
                self.pair(i, 0).start()
                self.pair(i, 1).start()
                if drain:
                    @pl.when(i > 0)
                    def _():
                        self.chip_sum(i - 1)
                return carry

            lax.fori_loop(0, self.chunks, step, 0)
            if drain:
                self.drain(self.chunks - 1)

        def drain(self, start=0):
            for i in range(start, self.chunks):
                self.chip_sum(i)
            if self.link_rows == rows:
                self.second().start()

        def kept(self):
            for i in range(self.chunks):
                self.pair(i, 1).wait_recv()

        def kept_rows(self, sub):
            return self.partial[block(me, sub), :] + self.from_part[1, pl.ds(sub * half, half), :]

        def rows_sum(self, sub):
            if sub == 0:
                for i in range(self.chunks):
                    self.first(i).wait_recv()
            else:
                self.second().wait_recv()
            return self.kept_rows(sub) + self.from_peer[pl.ds(sub * half, half), :]

        def pair_sent(self):
            for i in range(self.chunks):
                self.pair(i, 0).wait_send()
                self.pair(i, 1).wait_send()

        def link_sent(self):
            if self.link_rows:
                for i in range(self.chunks):
                    self.first(i).wait_send()
            if self.link_rows == rows:
                self.second().wait_send()

    x_in.wait()
    small_in[0].wait()
    small_in[1].wait()
    h1[block(me), :] = norm_rows(x_own[...].astype(F32), g1_ref[...], b1_ref[...]).astype(BF16)
    pl.semaphore_wait(barrier, 2)
    gather_h1 = Gather(h1, [(0, rows) + cut for cut in cuts(d, (1, 1, 1, 1))])
    gather_dy = Gather(dyf, [(0, rows, 0, d)])
    late = [(0, half, 0, d)] + [(half, half) + cut for cut in cuts(d, (1, 1, 1, 1))]
    for i in range(len(gather_h1.pieces)):
        gather_h1.send(i)
    dy_in.wait()
    gather_dy.send(0)

    small_in[2].wait()
    small_in[3].wait()
    pos_rows = jnp.broadcast_to(pos_ref[...].astype(F32), (hd, seq)).T
    angles = pos_rows * freq_ref[...]
    lane = lax.broadcasted_iota(jnp.int32, (seq, hd), 1)
    rot = hd // 4
    cosb[...] = jnp.cos(angles)
    sinb[...] = jnp.where(lane < rot, -1.0, 1.0) * jnp.sin(angles)

    def turn(v, sign):
        other = jnp.where(lane < rot, pltpu.roll(v, hd - rot, 1), pltpu.roll(v, rot, 1))
        other = jnp.where(lane < 2 * rot, other, 0.0)
        return v * cosb[...] + (sign * sinb[...]) * other

    for copy in weight_in[:3]:
        copy.wait()
    n_all = nqd + 2 * nkd

    def add(total, j, piece):
        total[...] = piece if j == 0 else total[...] + piece

    qkv_sum = part_c.at[:, pl.ds(0, n_all)]
    gather_h1.feed(0, lambda j, cols: add(qkv_sum, j, mm(h1[:, cols], wqkv[cols, :])))

    qkv = qkv_sum
    for k in range(nk):
        for g in range(grp):
            lo = (k * grp + g) * hd
            head = qkv[:, lo:lo + hd].astype(BF16).astype(F32)
            qs[k, g * seq:(g + 1) * seq, :] = turn(head, 1.0).astype(BF16)
        lo = nqd + k * hd
        kv[0, k] = turn(qkv[:, lo:lo + hd].astype(BF16).astype(F32), 1.0).astype(BF16)
        lo = nqd + nkd + k * hd
        kv[1, k] = qkv[:, lo:lo + hd].astype(BF16)
    put(h1, h1_out)
    query = lax.rem(lax.broadcasted_iota(jnp.int32, (grp * seq, seq), 0), seq)
    causal = query >= lax.broadcasted_iota(jnp.int32, (grp * seq, seq), 1)
    for k in range(nk):
        scores = jnp.where(causal, mm_bt(qs[k], kv[0, k]) * hd ** -0.5, -1e30)
        exped = jnp.exp(scores - jnp.max(scores, axis=-1, keepdims=True))
        prob[k] = exped / jnp.sum(exped, axis=-1, keepdims=True)
        head_ctx = mm(prob[k].astype(BF16), kv[1, k]).astype(BF16)
        for g in range(grp):
            lo = (k * grp + g) * hd
            ctx[:, lo:lo + hd] = head_ctx[g * seq:(g + 1) * seq, :]
    put(ctx, ctx_out)
    weight_in[3].wait()
    sum_attn = Scatter(4, part_a, dr_a, snd_a, lnk_a, rows)
    sum_attn.run(lambda cols: mm(ctx[...], wo[:, cols]))

    gather_dy.forward(0)
    gather_dy.finish(0)
    weight_in[4].wait()
    put(dyf, dy_out)
    nb = f // 2

    def down_back(j, carry):
        cols = pl.ds(pl.multiple_of(j * nb, nb), nb)
        tmat[:, cols] = mm_bt(dyf[...], w2[cols, :])
        return carry

    lax.fori_loop(0, f // nb, down_back, 0)

    gather_h2 = Gather(h2, late)
    small_in[4].wait()
    small_in[5].wait()
    for sub in (0, 1):
        if sub == 0:
            sum_attn.kept()
        own = pl.ds(sub * half, half)
        attn_rows = sum_attn.rows_sum(sub).astype(BF16)
        mid_rows = (x_own[own, :].astype(F32) + attn_rows.astype(F32)).astype(BF16)
        mid[own, :] = mid_rows
        h2[block(me, sub), :] = norm_rows(mid_rows.astype(F32), g2_ref[...], b2_ref[...]).astype(BF16)
        for i in ((0,) if sub == 0 else range(1, len(late))):
            gather_h2.send(i)
    weight_in[5].wait()

    def up(j, depth):
        def step(i, carry):
            cols = pl.ds(pl.multiple_of(i * nb, nb), nb)
            piece = mm(h2[:, depth], w1[depth, cols])
            if j == 0:
                part_c[:, cols] = piece
            elif j < len(late) - 2:
                part_c[:, cols] += piece
            else:
                relu_up = jnp.maximum((part_c[:, cols] + piece).astype(BF16).astype(F32), 0.0)
                act[:, cols] = (relu_up * relu_up).astype(BF16)
                du[:, cols] = (tmat[:, cols] * (2.0 * relu_up)).astype(BF16)
            return carry

        lax.fori_loop(0, f // nb, step, 0)

    gather_h2.feed(1, up)
    put(h2, h2_out)
    put(act, act_out)
    put(du, du_out)
    sum_dh2 = Scatter(4, part_b, dr_b, snd_b, lnk_b, rows)
    sum_dh2.run(lambda cols: mm_bt(du[...], w1[cols, :]))

    sum_mlp = Scatter(4, part_c, dr_c, snd_c, lnk_c, half)
    sum_mlp.run(lambda cols: mm(act[...], w2[:, cols]), drain=False)

    gather_dx1 = Gather(dx1, late)
    for sub in (0, 1):
        if sub == 0:
            sum_dh2.kept()
        own = pl.ds(sub * half, half)
        dh2_rows = sum_dh2.rows_sum(sub).astype(BF16).astype(F32)
        grad_rows, grad_gain, grad_bias = norm_rows_back(mid[own, :].astype(F32), dh2_rows, g2_ref[...])
        dx1[block(me, sub), :] = (dyf[block(me, sub), :].astype(F32) + grad_rows).astype(BF16)
        for i in ((0,) if sub == 0 else range(1, len(late))):
            gather_dx1.send(i)
        if sub == 0:
            lng[0:1, :] = grad_gain
            lng[1:2, :] = grad_bias
        else:
            lng[0:1, :] += grad_gain
            lng[1:2, :] += grad_bias
    put(lng, lng_out)
    put(dx1.at[block(me)], dmid_out)
    sum_mlp.drain()
    low = pl.ds(half, half)
    send[pl.ds(rows, half), :] = snd_c[low, :]
    sum_mlp.kept()
    ykeep[...] = sum_mlp.kept_rows(1)
    put(ykeep, ykeep_out)
    put(mid.at[low], mid_out)
    dctx_sum = tmat.at[:, pl.ds(0, nqd)]
    gather_dx1.feed(1, lambda j, cols: add(dctx_sum, j, mm_bt(dx1[:, cols], wo[:, cols])))
    put(dx1, dx1_out)

    dctx = dctx_sum[...].astype(BF16)
    for k in range(nk):
        for g in range(grp):
            lo = (k * grp + g) * hd
            gcs[k, g * seq:(g + 1) * seq, :] = dctx[:, lo:lo + hd]
    for k in range(nk):
        grad_v = mm_at(prob[k].astype(BF16), gcs[k]).astype(BF16)
        grad_p = mm_bt(gcs[k], kv[1, k])
        grad_s = (prob[k] * (grad_p - jnp.sum(grad_p * prob[k], axis=-1, keepdims=True)) * hd ** -0.5).astype(BF16)
        grad_q = mm(grad_s, kv[0, k])
        for g in range(grp):
            lo = (k * grp + g) * hd
            dqkv[:, lo:lo + hd] = turn(grad_q[g * seq:(g + 1) * seq, :], -1.0).astype(BF16)
        lo = nqd + k * hd
        dqkv[:, lo:lo + hd] = turn(mm_at(grad_s, qs[k]), -1.0).astype(BF16)
        lo = nqd + nkd + k * hd
        dqkv[:, lo:lo + hd] = grad_v
    put(dqkv, dqkv_out)
    top = pl.ds(0, half)
    y_own[...] = (mid[top, :].astype(F32) + sum_mlp.rows_sum(0).astype(BF16).astype(F32)).astype(BF16)
    put(y_own, y_out)
    sum_dh1 = Scatter(3, part_a, dr_d, send.at[pl.ds(0, rows)])
    sum_attn.pair_sent()
    sum_dh1.run(lambda cols: mm_bt(dqkv[...], wqkv[cols, :]))
    put(send, send_out)
    sum_dh1.kept()
    for sub in (0, 1):
        hkeep[pl.ds(sub * half, half), :] = sum_dh1.kept_rows(sub)
    put(hkeep, hkeep_out)

    for gather in (gather_h1, gather_dy, gather_h2, gather_dx1):
        for kind in (0, 1, 2):
            for i in range(len(gather.pieces)):
                gather.copy(kind, i).wait_send()
    for scatter in (sum_dh2, sum_mlp, sum_dh1):
        scatter.pair_sent()
    for scatter in (sum_attn, sum_dh2, sum_mlp):
        scatter.link_sent()
    for copy in outs:
        copy.wait()


def cuts(d, parts):
    unit, first, out = d // sum(parts), 0, []
    for n in parts:
        out.append((first, n * unit))
        first += n * unit
    return out


def chain(dims, x, dy, pos, freq, g1, b1, g2, b2, wq, wk, wv, wo, w1, w2):
    seq, d, hd, nq, nk, f, rows = dims
    grp = nq // nk
    nqd, nkd = nq * hd, nk * hd
    n_all = nqd + 2 * nkd
    half = rows // 2

    def arr(shape, dtype):
        return jax.ShapeDtypeStruct(shape, dtype)

    def vm(*shape, dtype=BF16):
        return pltpu.VMEM(shape, dtype)

    def vf(*shape):
        return pltpu.VMEM(shape, F32)

    out_shape = [arr((seq, d), BF16)] * 4 + [arr((seq, f), BF16)] * 2 + [arr((seq, nqd), BF16), arr((seq, n_all), BF16)] + [arr((half, d), BF16)] * 2 + [arr((rows, d), BF16), arr((rows + half, d), F32), arr((rows, d), F32), arr((half, d), F32), arr((2, d), F32)]
    n_sems = 3 * (4 + 1 + 5 + 5) + 2 * (4 + 4 + 4 + 3) + (5 + 5 + 5)
    scratch = [
        pltpu.VMEM((1, seq), jnp.int32), vf(1, hd), vf(1, d), vf(1, d), vf(1, d), vf(1, d),
        vm(d, n_all), vm(nqd, d), vm(d, f), vm(f, d),
        vm(seq, d), vm(seq, d), vm(seq, d), vm(seq, d),
        vm(rows, d), vm(rows, d), vm(half, d), vf(seq, f), vm(seq, f), vm(seq, f),
        vm(nk, grp * seq, hd), vm(2, nk, seq, hd), vm(seq, nqd), vf(nk, grp * seq, seq),
        vf(seq, hd), vf(seq, hd), vm(nk, grp * seq, hd), vm(seq, n_all), vf(2, d),
        vf(seq, d), vf(seq, d), vf(seq, d),
        vf(2, rows, d), vf(2, rows, d), vf(2, rows, d), vf(2, rows, d),
        vf(rows, d), vf(rows, d), vf(rows, d), vf(rows, d), vf(rows, d), vf(half, d),
        vf(rows + half, d), vf(rows, d), vf(half, d),
        pltpu.SemaphoreType.DMA((14,)), pltpu.SemaphoreType.DMA((len(out_shape),)),
        pltpu.SemaphoreType.DMA((n_sems,)), pltpu.SemaphoreType.DMA((n_sems,)),
    ]
    return pl.pallas_call(
        functools.partial(chain_kernel, dims),
        out_shape=out_shape,
        in_specs=[ANY] * 14,
        out_specs=[ANY] * len(out_shape),
        scratch_shapes=scratch,
        compiler_params=pltpu.CompilerParams(collective_id=0, has_side_effects=True, vmem_limit_bytes=VMEM_LIMIT),
        name="chain",
    )(x, dy, pos, freq, g1, b1, g2, b2, wq, wk, wv, wo, w1, w2)


SLOTS = 4
TILE = 256


def stream_grads(jobs, stage, sem):
    def copies(job, i, slot):
        return [pltpu.make_async_copy(stage.at[slot, pl.ds(0, job[1]), pl.ds(lo, n)], dst, sem.at[slot, c]) for c, (dst, lo, n) in enumerate(job[5](i))]

    done, pending = 0, []
    for job in jobs:
        ready, tile, tiles, width, compute, targets = job
        ready()

        def fill(i, slot):
            stage[slot, :tile, :width] = compute(i)
            for copy in copies(job, i, slot):
                copy.start()

        lead = min(SLOTS, tiles)
        for i in range(lead):
            slot = (done + i) % SLOTS
            if len(pending) == SLOTS:
                for copy in pending.pop(0):
                    copy.wait()
            fill(i, slot)
            pending.append(copies(job, i, slot))

        def step(i, carry, base=done):
            slot = lax.rem(base + i, SLOTS)
            for copy in copies(job, i - SLOTS, slot):
                copy.wait()
            fill(i, slot)
            return carry

        lax.fori_loop(lead, tiles, step, 0)
        if tiles > SLOTS:
            pending = [copies(job, i, (done + i) % SLOTS) for i in range(tiles - SLOTS, tiles)]
        done += tiles
    for group in pending:
        for copy in group:
            copy.wait()


def tile_at(i, tile, first=0):
    return pl.ds(pl.multiple_of(first + i * tile, tile), tile)


def outer_jobs(ready, left, right, targets, total, lead=0):
    jobs = []
    width = right.shape[1]
    if lead:
        small = TILE // 2
        jobs.append((ready, small, lead // small, width, lambda i: mm_at(left[:, tile_at(i, small)], right[...]), lambda i: targets(tile_at(i, small))))
        ready = lambda: None
    jobs.append((ready, TILE, (total - lead) // TILE, width, lambda i: mm_at(left[:, tile_at(i, TILE, lead)], right[...]), lambda i: targets(tile_at(i, TILE, lead))))
    return jobs


def start_loads(pairs, sem):
    loads = [pltpu.make_async_copy(src, dst, sem.at[i]) for i, (src, dst) in enumerate(pairs)]
    for copy in loads:
        copy.start()

    def ready(*which):
        return lambda: [loads[i].wait() for i in which] and None

    return ready


def grads_first_kernel(dims, act_hbm, dy_hbm, h1_hbm, dqkv_hbm, dw2, dwq, dwk, dwv, act, dyf, h1, dqkv, stage, in_sem, sem):
    seq, d, hd, nq, nk, f, rows = dims
    nqd, nkd = nq * hd, nk * hd
    ready = start_loads(((act_hbm, act), (dy_hbm, dyf), (h1_hbm, h1), (dqkv_hbm, dqkv)), in_sem)
    stream_grads(
        outer_jobs(ready(0, 1), act, dyf, lambda at: [(dw2.at[at], 0, d)], f, TILE)
        + outer_jobs(ready(2, 3), h1, dqkv, lambda at: [(dwq.at[at], 0, nqd), (dwk.at[at], nqd, nkd), (dwv.at[at], nqd + nkd, nkd)], d),
        stage, sem)


def grads_second_kernel(dims, order, h2_hbm, du_hbm, ctx_hbm, dx1_hbm, hkeep_hbm, recv_hbm, x_hbm, dmid_hbm, g1_hbm, lng2_hbm, ykeep_hbm, mid_hbm, y_hbm,
                        y_out, dx_out, lng_out, dw1, dwo,
                        h2, du, ctx, dx1, hkeep, recv, x, dmid, g1, ykeep, mid, y, lng, stage, in_sem, end_sem, sem):
    seq, d, hd, nq, nk, f, rows = dims
    half = rows // 2
    top, low = pl.ds(0, half), pl.ds(half, half)
    ready = start_loads(((h2_hbm, h2), (du_hbm, du), (hkeep_hbm, hkeep), (recv_hbm, recv), (x_hbm, x), (dmid_hbm, dmid), (g1_hbm, g1),
                         (lng2_hbm, lng.at[pl.ds(2, 2)]), (ykeep_hbm, ykeep), (mid_hbm, mid), (y_hbm, y.at[top]), (ctx_hbm, ctx), (dx1_hbm, dx1)), in_sem)
    ends = [pltpu.make_async_copy(src, dst, end_sem.at[i]) for i, (src, dst) in enumerate(((y, y_out), (dmid, dx_out), (lng, lng_out)))]

    def first_norm_back():
        ready(2, 3, 4, 5, 6, 7, 8, 9, 10)()
        dh1 = (hkeep[...] + recv[pl.ds(0, rows), :]).astype(BF16).astype(F32)
        grad_rows, grad_gain, grad_bias = norm_rows_back(x[...].astype(F32), dh1, g1[...])
        dmid[...] = (dmid[...].astype(F32) + grad_rows).astype(BF16)
        lng[0:1, :] = grad_gain
        lng[1:2, :] = grad_bias
        mlp = (ykeep[...] + recv[pl.ds(rows, half), :]).astype(BF16)
        y[low, :] = (mid[...].astype(F32) + mlp.astype(F32)).astype(BF16)
        for copy in ends:
            copy.start()

    def dw1_jobs(after, first, total):
        at = functools.partial(tile_at, tile=TILE, first=first)
        return [(after, TILE, total // TILE, f, lambda i: mm_at(h2[:, at(i)], du[...]), lambda i: [(dw1.at[at(i)], 0, f)])]

    lead = SLOTS * TILE
    stream_grads(
        dw1_jobs(ready(0, 1), 0, lead) + dw1_jobs(first_norm_back, lead, d - lead)
        + outer_jobs(ready(11, 12), ctx, dx1, lambda at: [(dwo.at[at], 0, d)], ctx.shape[1]),
        stage, sem)
    for copy in ends:
        copy.wait()


def cost(flops, nbytes):
    return pl.CostEstimate(flops=flops, bytes_accessed=nbytes, transcendentals=0)


def arr(shape, dtype=F32):
    return jax.ShapeDtypeStruct(shape, dtype)


def grads_first(dims, act, dyf, h1, dqkv):
    seq, d, hd, nq, nk, f, rows = dims
    nqd, nkd = nq * hd, nk * hd
    n_all = nqd + 2 * nkd
    return pl.pallas_call(
        functools.partial(grads_first_kernel, dims),
        out_shape=[arr((f, d)), arr((d, nqd)), arr((d, nkd)), arr((d, nkd))],
        in_specs=[ANY] * 4, out_specs=[ANY] * 4,
        scratch_shapes=[pltpu.VMEM((seq, f), BF16), pltpu.VMEM((seq, d), BF16), pltpu.VMEM((seq, d), BF16), pltpu.VMEM((seq, n_all), BF16),
                        pltpu.VMEM((SLOTS, TILE, d), F32), pltpu.SemaphoreType.DMA((4,)), pltpu.SemaphoreType.DMA((SLOTS, 3))],
        compiler_params=pltpu.CompilerParams(vmem_limit_bytes=VMEM_LIMIT),
        cost_estimate=cost(2 * seq * d * (f + n_all), 4 * d * (f + n_all)),
        name="grads_first",
    )(act, dyf, h1, dqkv)


def grads_second(dims, order, h2, du, ctx, dx1, hkeep, recv, x, dmid, g1, lng2, ykeep, mid, y):
    seq, d, hd, nq, nk, f, rows = dims
    nqd, half = nq * hd, rows // 2

    def vb(*shape):
        return pltpu.VMEM(shape, BF16)

    def vf(*shape):
        return pltpu.VMEM(shape, F32)

    return pl.pallas_call(
        functools.partial(grads_second_kernel, dims),
        out_shape=[arr((rows, d), BF16), arr((rows, d), BF16), arr((4, d)), arr((d, f)), arr((nqd, d))],
        in_specs=[ANY] * 14, out_specs=[ANY] * 5,
        scratch_shapes=[vb(seq, d), vb(seq, f), vb(seq, nqd), vb(seq, d), vf(rows, d), vf(rows + half, d), vb(rows, d), vb(rows, d), vf(1, d),
                        vf(half, d), vb(half, d), vb(rows, d), vf(4, d),
                        vf(SLOTS, TILE, d), pltpu.SemaphoreType.DMA((13,)), pltpu.SemaphoreType.DMA((3,)), pltpu.SemaphoreType.DMA((SLOTS, 3))],
        compiler_params=pltpu.CompilerParams(vmem_limit_bytes=VMEM_LIMIT),
        cost_estimate=cost(2 * seq * d * (f + nqd), 4 * d * (f + nqd)),
        name="grads_second",
    )(order, h2, du, ctx, dx1, hkeep, recv, x, dmid, g1, lng2, ykeep, mid, y)


def layer_step(x, dy, positions, g1, b1, g2, b2, wq, wk, wv, wo, w1, w2, head_dim, n_tp):
    rows, batch, d = x.shape
    seq = positions.shape[0]
    nq, nk, f = wq.shape[1] // head_dim, wk.shape[1] // head_dim, w1.shape[1]
    dims = (seq, d, head_dim, nq, nk, f, rows)
    rot = head_dim // 4
    freq = np.zeros((1, head_dim), np.float32)
    freq[0, :2 * rot] = np.tile(ROPE_BASE ** (-np.arange(rot) / rot), 2)
    x2, dy2 = x.reshape(rows, d), dy.reshape(rows, d)
    g1, b1, g2, b2 = (v.reshape(1, d) for v in (g1, b1, g2, b2))
    (h1, h2, dyf, dx1, act, du, ctx, dqkv, y, mid, dmid, send, hkeep, ykeep, lng2) = chain(
        dims, x2, dy2, positions.reshape(1, seq), jnp.asarray(freq), g1, b1, g2, b2, wq, wk, wv, wo, w1, w2)

    def swap(v, bit):
        return lax.ppermute(v, 'tp', [(i, i ^ bit) for i in range(n_tp)])

    recv = swap(send, 2)
    dw2, dwq, dwk, dwv = grads_first(dims, act, dyf, h1, dqkv)
    y, dx, lng, dw1, dwo = grads_second(dims, dw2, h2, du, ctx, dx1, hkeep, recv, x2, dmid, g1, lng2, ykeep, mid, y)
    others = [swap(lng, bit) for bit in (1, 2, 3)]
    sums = [(lng[i] + others[0][i]) + (others[1][i] + others[2][i]) for i in range(4)]
    return (y.reshape(x.shape), dx.reshape(x.shape), sums[0], sums[1], sums[2], sums[3], dwq, dwk, dwv, dwo, dw1, dw2)


def solution(mesh):
    seq_spec = P(('dp', 'tp'))
    col_spec = P(None, 'tp')
    row_spec = P('tp', None)
    grad_col_spec = P('dp', 'tp')
    grad_row_spec = P(('dp', 'tp'), None)
    in_specs = (seq_spec, seq_spec, P('dp'), P(), P(), P(), P(), col_spec, col_spec, col_spec, row_spec, col_spec, row_spec)
    out_specs = (seq_spec, seq_spec, P('dp'), P('dp'), P('dp'), P('dp'), grad_col_spec, grad_col_spec, grad_col_spec, grad_row_spec, grad_col_spec, grad_row_spec)

    def run_layer(resid_in, grad_out, positions, ln1_gain, ln1_bias, ln2_gain, ln2_bias, w_query, w_key, w_value, w_out, w_up, w_down):
        step_fn = functools.partial(layer_step, head_dim=w_key.shape[1] // KV_HEADS, n_tp=mesh.shape['tp'])
        sharded = jax.shard_map(step_fn, mesh=mesh, in_specs=in_specs, out_specs=out_specs, check_vma=False)
        return sharded(resid_in, grad_out, positions, ln1_gain, ln1_bias, ln2_gain, ln2_bias, w_query, w_key, w_value, w_out, w_up, w_down)

    return run_layer
```

```python
import functools
import math
import numpy as np
import jax
import jax.numpy as jnp
from jax import lax
from jax.experimental import pallas as pl
from jax.experimental.pallas import tpu as pltpu
from jax.sharding import PartitionSpec as P

KV_HEADS = 8
LN_EPS = 1e-5
ROPE_BASE = 10000.0
F32 = jnp.float32
BF16 = jnp.bfloat16
ANY = pl.BlockSpec(memory_space=pl.ANY)
VMEM = pl.BlockSpec(memory_space=pltpu.VMEM)
VMEM_LIMIT = 67_043_328


def mm(a, b):
    return jnp.dot(a, b, preferred_element_type=F32)


def mm_bt(a, b):
    return lax.dot_general(a, b, (((1,), (1,)), ((), ())), preferred_element_type=F32)


def mm_at(a, b):
    return lax.dot_general(a, b, (((0,), (0,)), ((), ())), preferred_element_type=F32)


def centre(rows):
    centred = rows - jnp.mean(rows, axis=-1, keepdims=True)
    scale = lax.rsqrt(jnp.mean(centred * centred, axis=-1, keepdims=True) + LN_EPS)
    return centred * scale, scale


def norm_rows(rows, gain, bias):
    normed, _ = centre(rows)
    return normed * (1.0 + gain) + bias


def norm_rows_back(rows, grad, gain):
    return norm_back(*centre(rows), grad, gain)


def norm_back(normed, scale, grad, gain):
    weighted = grad * (1.0 + gain)
    inner = jnp.mean(weighted * normed, axis=-1, keepdims=True)
    grad_rows = scale * (weighted - jnp.mean(weighted, axis=-1, keepdims=True) - normed * inner)
    return grad_rows, jnp.sum(grad * normed, axis=0, keepdims=True), jnp.sum(grad, axis=0, keepdims=True)


class Sems:
    def __init__(self):
        self.next = 0

    def take(self, count):
        base = self.next
        self.next += count
        return base


def chain_kernel(dims, x_hbm, dy_hbm, pos_hbm, freq_hbm, g1_hbm, b1_hbm, g2_hbm, b2_hbm, wq_hbm, wk_hbm, wv_hbm, wo_hbm, w1_hbm, w2_hbm,
                 h1_out, h2_out, dy_out, dx1_out, act_out, du_out, ctx_out, dqkv_out, y_out, mid_out, dmid_out, send_out, hkeep_out, ykeep_out, dg2_out, db2_out,
                 pos_ref, freq_ref, g1_ref, b1_ref, g2_ref, b2_ref,
                 wqkv, wo, w1, w2, h1, h2, dyf, dx1, x_own, mid, y_own, tmat, act, du, qs, kv, ctx, prob, cosb, sinb, gcs, dqkv, lng,
                 part_a, part_b, part_c, dr_a, dr_b, dr_c, dr_d, snd_a, snd_b, snd_c, lnk_a, lnk_b, lnk_c, send, hkeep, ykeep, lng_in, lng_chip, dg2, db2,
                 local_sem, out_sem, send_sem, recv_sem):
    seq, d, hd, nq, nk, f, rows = dims
    grp = nq // nk
    half = rows // 2
    me = lax.axis_index("tp")
    part, peer, diag = me ^ 1, me ^ 2, me ^ 3
    sems = Sems()

    def block(idx, sub=None):
        if sub is None:
            return pl.ds(pl.multiple_of(idx * rows, rows), rows)
        return pl.ds(pl.multiple_of(idx * rows + sub * half, half), half)

    def remote(src, dst, sem, dev):
        return pltpu.make_async_remote_copy(src, dst, send_sem.at[sem], recv_sem.at[sem], device_id={"tp": dev})

    def local(src, dst, idx):
        return pltpu.make_async_copy(src, dst, local_sem.at[idx])

    x_in = local(x_hbm, x_own, 0)
    dy_in = local(dy_hbm, dyf.at[block(me)], 1)
    nqd, nkd = nq * hd, nk * hd
    weight_in = [
        local(wq_hbm, wqkv.at[:, pl.ds(0, nqd)], 2),
        local(wk_hbm, wqkv.at[:, pl.ds(nqd, nkd)], 3),
        local(wv_hbm, wqkv.at[:, pl.ds(nqd + nkd, nkd)], 4),
        local(wo_hbm, wo, 5),
        local(w2_hbm, w2, 6),
        local(w1_hbm, w1, 7),
    ]
    small_in = [local(src, dst, 8 + i) for i, (src, dst) in enumerate((
        (g1_hbm, g1_ref), (b1_hbm, b1_ref), (pos_hbm, pos_ref), (freq_hbm, freq_ref), (g2_hbm, g2_ref), (b2_hbm, b2_ref)))]
    x_in.start()
    for copy in small_in:
        copy.start()
    dy_in.start()
    barrier = pltpu.get_barrier_semaphore()
    for dev in (part, peer):
        pl.semaphore_signal(barrier, inc=1, device_id={"tp": dev})
    for copy in weight_in:
        copy.start()

    outs = []

    def put(src, dst):
        copy = pltpu.make_async_copy(src, dst, out_sem.at[len(outs)])
        copy.start()
        outs.append(copy)

    class Gather:
        def __init__(self, buf, pieces):
            self.buf, self.pieces, self.base = buf, pieces, sems.take(3 * len(pieces))

        def copy(self, kind, i):
            owner = (me, me, peer)[kind]
            dev = (peer, part, part)[kind]
            row, n_rows, col, n_cols = self.pieces[i]
            at = self.buf.at[pl.ds(pl.multiple_of(owner * rows + row, half), n_rows), pl.ds(col, n_cols)]
            return remote(at, at, self.base + len(self.pieces) * kind + i, dev)

        def send(self, i):
            self.copy(0, i).start()
            self.copy(1, i).start()

        def forward(self, i):
            self.copy(0, i).wait_recv()
            self.copy(2, i).start()

        def finish(self, i):
            self.copy(1, i).wait_recv()
            self.copy(2, i).wait_recv()

        def feed(self, first, use):
            count = len(self.pieces)
            for i in range(first):
                self.forward(i)
            self.forward(first)
            for i in range(first):
                self.finish(i)
            for i in range(first, count):
                if i + 1 < count:
                    self.forward(i + 1)
                self.finish(i)
                use(i - first, pl.ds(self.pieces[i][2], self.pieces[i][3]))

    class Scatter:
        def __init__(self, chunks, partial, from_part, summed, from_peer=None, link_rows=0, early=0):
            self.chunks, self.cw, self.link_rows, self.early = chunks, d // chunks, link_rows, early
            self.partial, self.from_part, self.summed, self.from_peer = partial, from_part, summed, from_peer
            self.base = sems.take(2 * chunks)
            self.link = sems.take(chunks + 1 + early) if link_rows else None

        def cols(self, i):
            return pl.ds(pl.multiple_of(i * self.cw, self.cw), self.cw)

        def pair(self, i, kind):
            owner = (diag, part)[kind]
            return remote(self.partial.at[block(owner), self.cols(i)], self.from_part.at[kind, :, self.cols(i)], self.base + self.chunks * kind + i, part)

        def first(self, i):
            top = pl.ds(0, half)
            return remote(self.summed.at[top, self.cols(i)], self.from_peer.at[top, self.cols(i)], self.link + i, peer)

        def second(self):
            at = (pl.ds(half, half), pl.ds(self.early * self.cw, d - self.early * self.cw))
            return remote(self.summed.at[at], self.from_peer.at[at], self.link + self.chunks, peer)

        def ahead(self, i):
            at = (pl.ds(half, half), self.cols(i))
            return remote(self.summed.at[at], self.from_peer.at[at], self.link + self.chunks + 1 + i, peer)

        def chip_sum(self, i):
            self.pair(i, 0).wait_recv()
            cols = self.cols(i)
            self.summed[:, cols] = self.partial[block(peer), cols] + self.from_part[0, :, cols]
            if self.link_rows:
                self.first(i).start()
            if self.early:
                @pl.when(i < self.early)
                def _():
                    self.ahead(i).start()

        def run(self, chunk, drain=True):
            def step(i, carry):
                self.partial[:, self.cols(i)] = chunk(self.cols(i))
                self.pair(i, 0).start()
                self.pair(i, 1).start()
                if drain:
                    @pl.when(i > 0)
                    def _():
                        self.chip_sum(i - 1)
                return carry

            lax.fori_loop(0, self.chunks, step, 0)
            if drain:
                self.drain(self.chunks - 1)

        def drain(self, start=0):
            for i in range(start, self.chunks):
                self.chip_sum(i)
            if self.link_rows == rows:
                self.second().start()

        def kept(self):
            for i in range(self.chunks):
                self.pair(i, 1).wait_recv()

        def kept_rows(self, sub):
            return self.partial[block(me, sub), :] + self.from_part[1, pl.ds(sub * half, half), :]

        def rows_sum(self, sub):
            if sub == 0:
                for i in range(self.chunks):
                    self.first(i).wait_recv()
            else:
                for i in range(self.early):
                    self.ahead(i).wait_recv()
                self.second().wait_recv()
            return self.kept_rows(sub) + self.from_peer[pl.ds(sub * half, half), :]

        def pair_sent(self):
            for i in range(self.chunks):
                self.pair(i, 0).wait_send()
                self.pair(i, 1).wait_send()

        def link_sent(self):
            if self.link_rows:
                for i in range(self.chunks):
                    self.first(i).wait_send()
            if self.link_rows == rows:
                self.second().wait_send()
            for i in range(self.early):
                self.ahead(i).wait_send()

    x_in.wait()
    small_in[0].wait()
    small_in[1].wait()
    h1[block(me), :] = norm_rows(x_own[...].astype(F32), g1_ref[...], b1_ref[...]).astype(BF16)
    pl.semaphore_wait(barrier, 2)
    gather_h1 = Gather(h1, [(0, rows) + cut for cut in cuts(d, (4, 3, 3, 2))])
    gather_dy = Gather(dyf, [(0, rows, 0, d)])
    late = [(0, half, 0, d)] + [(half, half) + cut for cut in cuts(d, (4, 3, 3, 2))]
    for i in range(len(gather_h1.pieces)):
        gather_h1.send(i)
    dy_in.wait()
    gather_dy.send(0)

    small_in[2].wait()
    small_in[3].wait()
    pos_rows = jnp.broadcast_to(pos_ref[...].astype(F32), (hd, seq)).T
    angles = pos_rows * freq_ref[...]
    lane = lax.broadcasted_iota(jnp.int32, (seq, hd), 1)
    rot = hd // 4
    cosb[...] = jnp.cos(angles)
    sinb[...] = jnp.where(lane < rot, -1.0, 1.0) * jnp.sin(angles)

    def turn(v, sign):
        other = jnp.where(lane < rot, pltpu.roll(v, hd - rot, 1), pltpu.roll(v, rot, 1))
        other = jnp.where(lane < 2 * rot, other, 0.0)
        return v * cosb[...] + (sign * sinb[...]) * other

    for copy in weight_in[:3]:
        copy.wait()
    n_all = nqd + 2 * nkd

    def add(total, j, piece):
        total[...] = piece if j == 0 else total[...] + piece

    qkv_sum = part_c.at[:, pl.ds(0, n_all)]
    gather_h1.feed(0, lambda j, cols: add(qkv_sum, j, mm(h1[:, cols], wqkv[cols, :])))

    qkv = qkv_sum
    for k in range(nk):
        for g in range(grp):
            lo = (k * grp + g) * hd
            head = qkv[:, lo:lo + hd].astype(BF16).astype(F32)
            qs[k, g * seq:(g + 1) * seq, :] = turn(head, 1.0).astype(BF16)
        lo = nqd + k * hd
        kv[0, k] = turn(qkv[:, lo:lo + hd].astype(BF16).astype(F32), 1.0).astype(BF16)
        lo = nqd + nkd + k * hd
        kv[1, k] = qkv[:, lo:lo + hd].astype(BF16)
    put(h1, h1_out)
    query = lax.rem(lax.broadcasted_iota(jnp.int32, (grp * seq, seq), 0), seq)
    causal = query >= lax.broadcasted_iota(jnp.int32, (grp * seq, seq), 1)
    for k in range(nk):
        scores = jnp.where(causal, mm_bt(qs[k], kv[0, k]) * hd ** -0.5, -1e30)
        exped = jnp.exp(scores - jnp.max(scores, axis=-1, keepdims=True))
        prob[k] = exped / jnp.sum(exped, axis=-1, keepdims=True)
        head_ctx = mm(prob[k].astype(BF16), kv[1, k]).astype(BF16)
        for g in range(grp):
            lo = (k * grp + g) * hd
            ctx[:, lo:lo + hd] = head_ctx[g * seq:(g + 1) * seq, :]
    put(ctx, ctx_out)
    weight_in[3].wait()
    sum_attn = Scatter(4, part_a, dr_a, snd_a, lnk_a, rows)
    sum_attn.run(lambda cols: mm(ctx[...], wo[:, cols]))

    gather_dy.forward(0)
    gather_dy.finish(0)
    weight_in[4].wait()
    put(dyf, dy_out)
    nb = f // 2

    def down_back(j, carry):
        cols = pl.ds(pl.multiple_of(j * nb, nb), nb)
        tmat[:, cols] = mm_bt(dyf[...], w2[cols, :])
        return carry

    lax.fori_loop(0, f // nb, down_back, 0)

    gather_h2 = Gather(h2, late)
    small_in[4].wait()
    small_in[5].wait()
    for sub in (0, 1):
        if sub == 0:
            sum_attn.kept()
        own = pl.ds(sub * half, half)
        attn_rows = sum_attn.rows_sum(sub).astype(BF16)
        mid_rows = (x_own[own, :].astype(F32) + attn_rows.astype(F32)).astype(BF16)
        mid[own, :] = mid_rows
        h2[block(me, sub), :] = norm_rows(mid_rows.astype(F32), g2_ref[...], b2_ref[...]).astype(BF16)
        for i in ((0,) if sub == 0 else range(1, len(late))):
            gather_h2.send(i)
    weight_in[5].wait()

    def up(j, depth):
        for i in range(f // nb):
            cols = pl.ds(i * nb, nb)
            piece = mm(h2[:, depth], w1[depth, cols])
            if j == 0:
                part_c[:, cols] = piece
            elif j < len(late) - 2:
                part_c[:, cols] += piece
            else:
                relu_up = jnp.maximum((part_c[:, cols] + piece).astype(BF16).astype(F32), 0.0)
                act[:, cols] = (relu_up * relu_up).astype(BF16)
                du[:, cols] = (tmat[:, cols] * (2.0 * relu_up)).astype(BF16)

    gather_h2.feed(1, up)
    put(h2, h2_out)
    put(act, act_out)
    put(du, du_out)
    sum_dh2 = Scatter(6, part_b, dr_b, snd_b, lnk_b, rows, 2)
    sum_dh2.run(lambda cols: mm_bt(du[...], w1[cols, :]))

    sum_mlp = Scatter(4, part_c, dr_c, snd_c, lnk_c, half)
    sum_mlp.run(lambda cols: mm(act[...], w2[:, cols]), drain=False)

    gather_dx1 = Gather(dx1, late)
    normed2, scale2 = centre(mid[...].astype(F32))
    for sub in (0, 1):
        if sub == 0:
            sum_dh2.kept()
        dh2_rows = sum_dh2.rows_sum(sub).astype(BF16).astype(F32)
        own = slice(sub * half, (sub + 1) * half)
        grad_rows, grad_gain, grad_bias = norm_back(normed2[own], scale2[own], dh2_rows, g2_ref[...])
        dx1[block(me, sub), :] = (dyf[block(me, sub), :].astype(F32) + grad_rows).astype(BF16)
        for i in ((0,) if sub == 0 else range(1, len(late))):
            gather_dx1.send(i)
        if sub == 0:
            lng[0:1, :] = grad_gain
            lng[1:2, :] = grad_bias
        else:
            lng[0:1, :] += grad_gain
            lng[1:2, :] += grad_bias
    put(dx1.at[block(me)], dmid_out)
    lng_base = sems.take(2)
    lng_pair = remote(lng, lng_in.at[0], lng_base, part)
    lng_pair.start()
    sum_mlp.drain()
    low = pl.ds(half, half)
    send[pl.ds(rows, half), :] = snd_c[low, :]
    sum_mlp.kept()
    ykeep[...] = sum_mlp.kept_rows(1)
    put(ykeep, ykeep_out)
    put(mid.at[low], mid_out)
    lng_pair.wait_recv()
    lng_chip[...] = lng[...] + lng_in[0]
    lng_link = remote(lng_chip, lng_in.at[1], lng_base + 1, peer)
    lng_link.start()
    dctx_sum = tmat.at[:, pl.ds(0, nqd)]
    gather_dx1.feed(1, lambda j, cols: add(dctx_sum, j, mm_bt(dx1[:, cols], wo[:, cols])))
    put(dx1, dx1_out)

    dctx = dctx_sum[...].astype(BF16)
    for k in range(nk):
        for g in range(grp):
            lo = (k * grp + g) * hd
            gcs[k, g * seq:(g + 1) * seq, :] = dctx[:, lo:lo + hd]
    for k in range(nk):
        grad_v = mm_at(prob[k].astype(BF16), gcs[k]).astype(BF16)
        grad_p = mm_bt(gcs[k], kv[1, k])
        grad_s = (prob[k] * (grad_p - jnp.sum(grad_p * prob[k], axis=-1, keepdims=True)) * hd ** -0.5).astype(BF16)
        grad_q = mm(grad_s, kv[0, k])
        for g in range(grp):
            lo = (k * grp + g) * hd
            dqkv[:, lo:lo + hd] = turn(grad_q[g * seq:(g + 1) * seq, :], -1.0).astype(BF16)
        lo = nqd + k * hd
        dqkv[:, lo:lo + hd] = turn(mm_at(grad_s, qs[k]), -1.0).astype(BF16)
        lo = nqd + nkd + k * hd
        dqkv[:, lo:lo + hd] = grad_v
    put(dqkv, dqkv_out)
    top = pl.ds(0, half)
    y_own[...] = (mid[top, :].astype(F32) + sum_mlp.rows_sum(0).astype(BF16).astype(F32)).astype(BF16)
    put(y_own, y_out)
    sum_dh1 = Scatter(4, part_a, dr_d, send.at[pl.ds(0, rows)])
    sum_attn.pair_sent()
    lng_link.wait_recv()
    dg2[...] = lng_chip[0:1, :] + lng_in[1, 0:1, :]
    db2[...] = lng_chip[1:2, :] + lng_in[1, 1:2, :]
    put(dg2, dg2_out)
    put(db2, db2_out)
    sum_dh1.run(lambda cols: mm_bt(dqkv[...], wqkv[cols, :]))
    put(send, send_out)
    sum_dh1.kept()
    for sub in (0, 1):
        hkeep[pl.ds(sub * half, half), :] = sum_dh1.kept_rows(sub)
    put(hkeep, hkeep_out)

    for gather in (gather_h1, gather_dy, gather_h2, gather_dx1):
        for kind in (0, 1, 2):
            for i in range(len(gather.pieces)):
                gather.copy(kind, i).wait_send()
    for scatter in (sum_dh2, sum_mlp, sum_dh1):
        scatter.pair_sent()
    for scatter in (sum_attn, sum_dh2, sum_mlp):
        scatter.link_sent()
    lng_pair.wait_send()
    lng_link.wait_send()
    for copy in outs:
        copy.wait()


def cuts(d, parts):
    unit, first, out = d // sum(parts), 0, []
    for n in parts:
        out.append((first, n * unit))
        first += n * unit
    return out


def chain(dims, x, dy, pos, freq, g1, b1, g2, b2, wq, wk, wv, wo, w1, w2):
    seq, d, hd, nq, nk, f, rows = dims
    grp = nq // nk
    nqd, nkd = nq * hd, nk * hd
    n_all = nqd + 2 * nkd
    half = rows // 2

    def arr(shape, dtype):
        return jax.ShapeDtypeStruct(shape, dtype)

    def vm(*shape, dtype=BF16):
        return pltpu.VMEM(shape, dtype)

    def vf(*shape):
        return pltpu.VMEM(shape, F32)

    out_shape = [arr((seq, d), BF16)] * 4 + [arr((seq, f), BF16)] * 2 + [arr((seq, nqd), BF16), arr((seq, n_all), BF16)] + [arr((half, d), BF16)] * 2 + [arr((rows, d), BF16), arr((rows + half, d), F32), arr((rows, d), F32), arr((half, d), F32)] + [arr((1, d), F32)] * 2
    n_sems = 3 * (4 + 1 + 5 + 5) + 2 * (4 + 6 + 4 + 4) + (5 + 9 + 5) + 2
    scratch = [
        pltpu.VMEM((1, seq), jnp.int32), vf(1, hd), vf(1, d), vf(1, d), vf(1, d), vf(1, d),
        vm(d, n_all), vm(nqd, d), vm(d, f), vm(f, d),
        vm(seq, d), vm(seq, d), vm(seq, d), vm(seq, d),
        vm(rows, d), vm(rows, d), vm(half, d), vf(seq, f), vm(seq, f), vm(seq, f),
        vm(nk, grp * seq, hd), vm(2, nk, seq, hd), vm(seq, nqd), vf(nk, grp * seq, seq),
        vf(seq, hd), vf(seq, hd), vm(nk, grp * seq, hd), vm(seq, n_all), vf(2, d),
        vf(seq, d), vf(seq, d), vf(seq, d),
        vf(2, rows, d), vf(2, rows, d), vf(2, rows, d), vf(2, rows, d),
        vf(rows, d), vf(rows, d), vf(rows, d), vf(rows, d), vf(rows, d), vf(half, d),
        vf(rows + half, d), vf(rows, d), vf(half, d), vf(2, 2, d), vf(2, d), vf(1, d), vf(1, d),
        pltpu.SemaphoreType.DMA((14,)), pltpu.SemaphoreType.DMA((len(out_shape),)),
        pltpu.SemaphoreType.DMA((n_sems,)), pltpu.SemaphoreType.DMA((n_sems,)),
    ]
    return pl.pallas_call(
        functools.partial(chain_kernel, dims),
        out_shape=out_shape,
        in_specs=[ANY] * 14,
        out_specs=[ANY] * len(out_shape),
        scratch_shapes=scratch,
        compiler_params=pltpu.CompilerParams(collective_id=0, has_side_effects=True, vmem_limit_bytes=VMEM_LIMIT),
        name="chain",
    )(x, dy, pos, freq, g1, b1, g2, b2, wq, wk, wv, wo, w1, w2)


SLOTS = 4
TILE = 256


def stream_grads(jobs, stage, sem):
    def copies(job, i, slot):
        return [pltpu.make_async_copy(stage.at[slot, pl.ds(0, job[1]), pl.ds(lo, n)], dst, sem.at[slot, c]) for c, (dst, lo, n) in enumerate(job[5](i))]

    done, pending = 0, []
    for job in jobs:
        ready, tile, tiles, width, compute, targets = job
        ready()

        def fill(i, slot):
            stage[slot, :tile, :width] = compute(i)
            for copy in copies(job, i, slot):
                copy.start()

        lead = min(SLOTS, tiles)
        for i in range(lead):
            slot = (done + i) % SLOTS
            if len(pending) == SLOTS:
                for copy in pending.pop(0):
                    copy.wait()
            fill(i, slot)
            pending.append(copies(job, i, slot))

        def step(i, carry, base=done):
            slot = lax.rem(base + i, SLOTS)
            for copy in copies(job, i - SLOTS, slot):
                copy.wait()
            fill(i, slot)
            return carry

        lax.fori_loop(lead, tiles, step, 0)
        if tiles > SLOTS:
            pending = [copies(job, i, (done + i) % SLOTS) for i in range(tiles - SLOTS, tiles)]
        done += tiles
    for group in pending:
        for copy in group:
            copy.wait()


def tile_at(i, tile, first=0):
    return pl.ds(pl.multiple_of(first + i * tile, tile), tile)


def outer_jobs(ready, left, right, targets, total, lead=0):
    jobs = []
    width = right.shape[1]
    if lead:
        small = TILE // 2
        jobs.append((ready, small, lead // small, width, lambda i: mm_at(left[:, tile_at(i, small)], right[...]), lambda i: targets(tile_at(i, small))))
        ready = lambda: None
    jobs.append((ready, TILE, (total - lead) // TILE, width, lambda i: mm_at(left[:, tile_at(i, TILE, lead)], right[...]), lambda i: targets(tile_at(i, TILE, lead))))
    return jobs


def start_loads(pairs, sem):
    loads = [pltpu.make_async_copy(src, dst, sem.at[i]) for i, (src, dst) in enumerate(pairs)]
    for copy in loads:
        copy.start()

    def ready(*which):
        return lambda: [loads[i].wait() for i in which] and None

    return ready


def grads_first_kernel(dims, act_hbm, dy_hbm, h1_hbm, dqkv_hbm, dw2, dwq, dwk, dwv, act, dyf, h1, dqkv, stage, in_sem, sem):
    seq, d, hd, nq, nk, f, rows = dims
    nqd, nkd = nq * hd, nk * hd
    ready = start_loads(((act_hbm, act), (dy_hbm, dyf), (h1_hbm, h1), (dqkv_hbm, dqkv)), in_sem)
    stream_grads(
        outer_jobs(ready(0, 1), act, dyf, lambda at: [(dw2.at[at], 0, d)], f, TILE)
        + outer_jobs(ready(2, 3), h1, dqkv, lambda at: [(dwq.at[at], 0, nqd), (dwk.at[at], nqd, nkd), (dwv.at[at], nqd + nkd, nkd)], d),
        stage, sem)


def grads_second_kernel(dims, order, h2_hbm, du_hbm, ctx_hbm, dx1_hbm, hkeep_hbm, recv_hbm, x_hbm, dmid_hbm, g1_hbm, dg2_hbm, db2_hbm, ykeep_hbm, mid_hbm, y_hbm,
                        y_out, dx_out, lng_out, dg2_out, db2_out, dw1, dwo,
                        h2, du, ctx, dx1, hkeep, recv, x, dmid, g1, ykeep, mid, y, lng, dg2, db2, stage, in_sem, end_sem, sem):
    seq, d, hd, nq, nk, f, rows = dims
    half = rows // 2
    top, low = pl.ds(0, half), pl.ds(half, half)
    ready = start_loads(((h2_hbm, h2), (du_hbm, du), (hkeep_hbm, hkeep), (recv_hbm, recv), (x_hbm, x), (dmid_hbm, dmid), (g1_hbm, g1),
                         (dg2_hbm, dg2), (db2_hbm, db2), (ykeep_hbm, ykeep), (mid_hbm, mid), (y_hbm, y.at[top]), (ctx_hbm, ctx), (dx1_hbm, dx1)), in_sem)
    ends = [pltpu.make_async_copy(src, dst, end_sem.at[i]) for i, (src, dst) in enumerate(((y, y_out), (dmid, dx_out), (lng, lng_out), (dg2, dg2_out), (db2, db2_out)))]

    def first_norm_back():
        ready(2, 3, 4, 5, 6, 7, 8, 9, 10, 11)()
        dh1 = (hkeep[...] + recv[pl.ds(0, rows), :]).astype(BF16).astype(F32)
        grad_rows, grad_gain, grad_bias = norm_rows_back(x[...].astype(F32), dh1, g1[...])
        dmid[...] = (dmid[...].astype(F32) + grad_rows).astype(BF16)
        lng[0:1, :] = grad_gain
        lng[1:2, :] = grad_bias
        mlp = (ykeep[...] + recv[pl.ds(rows, half), :]).astype(BF16)
        y[low, :] = (mid[...].astype(F32) + mlp.astype(F32)).astype(BF16)
        for copy in ends:
            copy.start()

    def dw1_jobs(after, first, total):
        at = functools.partial(tile_at, tile=TILE, first=first)
        return [(after, TILE, total // TILE, f, lambda i: mm_at(h2[:, at(i)], du[...]), lambda i: [(dw1.at[at(i)], 0, f)])]

    lead = SLOTS * TILE
    stream_grads(
        dw1_jobs(ready(0, 1), 0, lead) + dw1_jobs(first_norm_back, lead, d - lead)
        + outer_jobs(ready(12, 13), ctx, dx1, lambda at: [(dwo.at[at], 0, d)], ctx.shape[1]),
        stage, sem)
    for copy in ends:
        copy.wait()


def cost(flops, nbytes):
    return pl.CostEstimate(flops=flops, bytes_accessed=nbytes, transcendentals=0)


def arr(shape, dtype=F32):
    return jax.ShapeDtypeStruct(shape, dtype)


def grads_first(dims, act, dyf, h1, dqkv):
    seq, d, hd, nq, nk, f, rows = dims
    nqd, nkd = nq * hd, nk * hd
    n_all = nqd + 2 * nkd
    return pl.pallas_call(
        functools.partial(grads_first_kernel, dims),
        out_shape=[arr((f, d)), arr((d, nqd)), arr((d, nkd)), arr((d, nkd))],
        in_specs=[ANY] * 4, out_specs=[ANY] * 4,
        scratch_shapes=[pltpu.VMEM((seq, f), BF16), pltpu.VMEM((seq, d), BF16), pltpu.VMEM((seq, d), BF16), pltpu.VMEM((seq, n_all), BF16),
                        pltpu.VMEM((SLOTS, TILE, d), F32), pltpu.SemaphoreType.DMA((4,)), pltpu.SemaphoreType.DMA((SLOTS, 3))],
        compiler_params=pltpu.CompilerParams(vmem_limit_bytes=VMEM_LIMIT),
        cost_estimate=cost(2 * seq * d * (f + n_all), 4 * d * (f + n_all)),
        name="grads_first",
    )(act, dyf, h1, dqkv)


def grads_second(dims, order, h2, du, ctx, dx1, hkeep, recv, x, dmid, g1, dg2, db2, ykeep, mid, y):
    seq, d, hd, nq, nk, f, rows = dims
    nqd, half = nq * hd, rows // 2

    def vb(*shape):
        return pltpu.VMEM(shape, BF16)

    def vf(*shape):
        return pltpu.VMEM(shape, F32)

    return pl.pallas_call(
        functools.partial(grads_second_kernel, dims),
        out_shape=[arr((rows, d), BF16), arr((rows, d), BF16), arr((2, d)), arr((1, d)), arr((1, d)), arr((d, f)), arr((nqd, d))],
        in_specs=[ANY] * 15, out_specs=[ANY] * 7,
        scratch_shapes=[vb(seq, d), vb(seq, f), vb(seq, nqd), vb(seq, d), vf(rows, d), vf(rows + half, d), vb(rows, d), vb(rows, d), vf(1, d),
                        vf(half, d), vb(half, d), vb(rows, d), vf(2, d), vf(1, d), vf(1, d),
                        vf(SLOTS, TILE, d), pltpu.SemaphoreType.DMA((14,)), pltpu.SemaphoreType.DMA((5,)), pltpu.SemaphoreType.DMA((SLOTS, 3))],
        compiler_params=pltpu.CompilerParams(vmem_limit_bytes=VMEM_LIMIT),
        cost_estimate=cost(2 * seq * d * (f + nqd), 4 * d * (f + nqd)),
        name="grads_second",
    )(order, h2, du, ctx, dx1, hkeep, recv, x, dmid, g1, dg2, db2, ykeep, mid, y)


def layer_step(x, dy, positions, g1, b1, g2, b2, wq, wk, wv, wo, w1, w2, head_dim, n_tp):
    rows, batch, d = x.shape
    seq = positions.shape[0]
    nq, nk, f = wq.shape[1] // head_dim, wk.shape[1] // head_dim, w1.shape[1]
    dims = (seq, d, head_dim, nq, nk, f, rows)
    rot = head_dim // 4
    freq = np.zeros((1, head_dim), np.float32)
    freq[0, :2 * rot] = np.tile(ROPE_BASE ** (-np.arange(rot) / rot), 2)
    x2, dy2 = x.reshape(rows, d), dy.reshape(rows, d)
    g1, b1, g2, b2 = (v.reshape(1, d) for v in (g1, b1, g2, b2))
    (h1, h2, dyf, dx1, act, du, ctx, dqkv, y, mid, dmid, send, hkeep, ykeep, dg2, db2) = chain(
        dims, x2, dy2, positions.reshape(1, seq), jnp.asarray(freq), g1, b1, g2, b2, wq, wk, wv, wo, w1, w2)

    def swap(v, bit):
        return lax.ppermute(v, 'tp', [(i, i ^ bit) for i in range(n_tp)])

    recv = swap(send, 2)
    dw2, dwq, dwk, dwv = grads_first(dims, act, dyf, h1, dqkv)
    y, dx, lng, dg2, db2, dw1, dwo = grads_second(dims, dw2, h2, du, ctx, dx1, hkeep, recv, x2, dmid, g1, dg2, db2, ykeep, mid, y)
    others = [swap(lng, bit) for bit in (1, 2, 3)]
    sums = [(lng[i] + others[0][i]) + (others[1][i] + others[2][i]) for i in range(2)]
    return (y.reshape(x.shape), dx.reshape(x.shape), sums[0], sums[1], dg2.reshape(d), db2.reshape(d), dwq, dwk, dwv, dwo, dw1, dw2)


def solution(mesh):
    seq_spec = P(('dp', 'tp'))
    col_spec = P(None, 'tp')
    row_spec = P('tp', None)
    grad_col_spec = P('dp', 'tp')
    grad_row_spec = P(('dp', 'tp'), None)
    in_specs = (seq_spec, seq_spec, P('dp'), P(), P(), P(), P(), col_spec, col_spec, col_spec, row_spec, col_spec, row_spec)
    out_specs = (seq_spec, seq_spec, P('dp'), P('dp'), P('dp'), P('dp'), grad_col_spec, grad_col_spec, grad_col_spec, grad_row_spec, grad_col_spec, grad_row_spec)

    def run_layer(resid_in, grad_out, positions, ln1_gain, ln1_bias, ln2_gain, ln2_bias, w_query, w_key, w_value, w_out, w_up, w_down):
        step_fn = functools.partial(layer_step, head_dim=w_key.shape[1] // KV_HEADS, n_tp=mesh.shape['tp'])
        sharded = jax.shard_map(step_fn, mesh=mesh, in_specs=in_specs, out_specs=out_specs, check_vma=False)
        return sharded(resid_in, grad_out, positions, ln1_gain, ln1_bias, ln2_gain, ln2_bias, w_query, w_key, w_value, w_out, w_up, w_down)

    return run_layer
```

```python
import functools
import math
import numpy as np
import jax
import jax.numpy as jnp
from jax import lax
from jax.experimental import pallas as pl
from jax.experimental.pallas import tpu as pltpu
from jax.sharding import PartitionSpec as P

KV_HEADS = 8
LN_EPS = 1e-5
ROPE_BASE = 10000.0
F32 = jnp.float32
BF16 = jnp.bfloat16
ANY = pl.BlockSpec(memory_space=pl.ANY)
VMEM = pl.BlockSpec(memory_space=pltpu.VMEM)
VMEM_LIMIT = 67_043_328


def mm(a, b):
    return jnp.dot(a, b, preferred_element_type=F32)


def mm_bt(a, b):
    return lax.dot_general(a, b, (((1,), (1,)), ((), ())), preferred_element_type=F32)


def mm_at(a, b):
    return lax.dot_general(a, b, (((0,), (0,)), ((), ())), preferred_element_type=F32)


def centre(rows):
    centred = rows - jnp.mean(rows, axis=-1, keepdims=True)
    scale = lax.rsqrt(jnp.mean(centred * centred, axis=-1, keepdims=True) + LN_EPS)
    return centred * scale, scale


def norm_rows(rows, gain, bias):
    normed, _ = centre(rows)
    return normed * (1.0 + gain) + bias


def norm_rows_back(rows, grad, gain):
    return norm_back(*centre(rows), grad, gain)


def norm_back(normed, scale, grad, gain):
    weighted = grad * (1.0 + gain)
    inner = jnp.mean(weighted * normed, axis=-1, keepdims=True)
    grad_rows = scale * (weighted - jnp.mean(weighted, axis=-1, keepdims=True) - normed * inner)
    return grad_rows, jnp.sum(grad * normed, axis=0, keepdims=True), jnp.sum(grad, axis=0, keepdims=True)


class Sems:
    def __init__(self):
        self.next = 0

    def take(self, count):
        base = self.next
        self.next += count
        return base


def chain_kernel(dims, x_hbm, dy_hbm, pos_hbm, freq_hbm, g1_hbm, b1_hbm, g2_hbm, b2_hbm, wq_hbm, wk_hbm, wv_hbm, wo_hbm, w1_hbm, w2_hbm,
                 h1_out, h2_out, dy_out, dx1_out, act_out, du_out, ctx_out, dqkv_out, y_out, mid_out, dmid_out, send_out, hkeep_out, ykeep_out, dg2_out, db2_out,
                 pos_ref, freq_ref, g1_ref, b1_ref, g2_ref, b2_ref,
                 wqkv, wo, w1, w2, h1, h2, dyf, dx1, x_own, mid, y_own, tmat, act, du, qs, kv, ctx, prob, cosb, sinb, gcs, dqkv, lng,
                 part_a, part_b, part_c, dr_a, dr_b, dr_c, dr_d, snd_a, snd_b, snd_c, lnk_a, lnk_b, lnk_c, send, hkeep, ykeep, lng_in, lng_chip, dg2, db2,
                 local_sem, out_sem, send_sem, recv_sem):
    seq, d, hd, nq, nk, f, rows = dims
    grp = nq // nk
    half = rows // 2
    me = lax.axis_index("tp")
    part, peer, diag = me ^ 1, me ^ 2, me ^ 3
    sems = Sems()

    def block(idx, sub=None):
        if sub is None:
            return pl.ds(pl.multiple_of(idx * rows, rows), rows)
        return pl.ds(pl.multiple_of(idx * rows + sub * half, half), half)

    def remote(src, dst, sem, dev):
        return pltpu.make_async_remote_copy(src, dst, send_sem.at[sem], recv_sem.at[sem], device_id={"tp": dev})

    def local(src, dst, idx):
        return pltpu.make_async_copy(src, dst, local_sem.at[idx])

    x_in = local(x_hbm, x_own, 0)
    dy_in = local(dy_hbm, dyf.at[block(me)], 1)
    nqd, nkd = nq * hd, nk * hd
    weight_in = [
        local(wq_hbm, wqkv.at[:, pl.ds(0, nqd)], 2),
        local(wk_hbm, wqkv.at[:, pl.ds(nqd, nkd)], 3),
        local(wv_hbm, wqkv.at[:, pl.ds(nqd + nkd, nkd)], 4),
        local(wo_hbm, wo, 5),
        local(w2_hbm, w2, 6),
        local(w1_hbm, w1, 7),
    ]
    small_in = [local(src, dst, 8 + i) for i, (src, dst) in enumerate((
        (g1_hbm, g1_ref), (b1_hbm, b1_ref), (pos_hbm, pos_ref), (freq_hbm, freq_ref), (g2_hbm, g2_ref), (b2_hbm, b2_ref)))]
    x_in.start()
    for copy in small_in:
        copy.start()
    dy_in.start()
    barrier = pltpu.get_barrier_semaphore()
    for dev in (part, peer):
        pl.semaphore_signal(barrier, inc=1, device_id={"tp": dev})
    for copy in weight_in:
        copy.start()

    outs = []

    def put(src, dst):
        copy = pltpu.make_async_copy(src, dst, out_sem.at[len(outs)])
        copy.start()
        outs.append(copy)

    class Gather:
        def __init__(self, buf, pieces):
            self.buf, self.pieces, self.base = buf, pieces, sems.take(3 * len(pieces))

        def copy(self, kind, i):
            owner = (me, me, peer)[kind]
            dev = (peer, part, part)[kind]
            row, n_rows, col, n_cols = self.pieces[i]
            at = self.buf.at[pl.ds(pl.multiple_of(owner * rows + row, half), n_rows), pl.ds(col, n_cols)]
            return remote(at, at, self.base + len(self.pieces) * kind + i, dev)

        def send(self, i):
            self.copy(0, i).start()
            self.copy(1, i).start()

        def forward(self, i):
            self.copy(0, i).wait_recv()
            self.copy(2, i).start()

        def finish(self, i):
            self.copy(1, i).wait_recv()
            self.copy(2, i).wait_recv()

        def feed(self, first, use):
            count = len(self.pieces)
            for i in range(first):
                self.forward(i)
            self.forward(first)
            for i in range(first):
                self.finish(i)
            for i in range(first, count):
                if i + 1 < count:
                    self.forward(i + 1)
                self.finish(i)
                use(i - first, pl.ds(self.pieces[i][2], self.pieces[i][3]))

    class Scatter:
        def __init__(self, chunks, partial, from_part, summed, from_peer=None, link_rows=0, early=0):
            self.chunks, self.cw, self.link_rows, self.early = chunks, d // chunks, link_rows, early
            self.partial, self.from_part, self.summed, self.from_peer = partial, from_part, summed, from_peer
            self.base = sems.take(2 * chunks)
            self.link = sems.take(chunks + 1 + early) if link_rows else None

        def cols(self, i):
            return pl.ds(pl.multiple_of(i * self.cw, self.cw), self.cw)

        def pair(self, i, kind):
            owner = (diag, part)[kind]
            return remote(self.partial.at[block(owner), self.cols(i)], self.from_part.at[kind, :, self.cols(i)], self.base + self.chunks * kind + i, part)

        def first(self, i):
            top = pl.ds(0, half)
            return remote(self.summed.at[top, self.cols(i)], self.from_peer.at[top, self.cols(i)], self.link + i, peer)

        def second(self):
            at = (pl.ds(half, half), pl.ds(self.early * self.cw, d - self.early * self.cw))
            return remote(self.summed.at[at], self.from_peer.at[at], self.link + self.chunks, peer)

        def ahead(self, i):
            at = (pl.ds(half, half), self.cols(i))
            return remote(self.summed.at[at], self.from_peer.at[at], self.link + self.chunks + 1 + i, peer)

        def chip_sum(self, i):
            self.pair(i, 0).wait_recv()
            cols = self.cols(i)
            self.summed[:, cols] = self.partial[block(peer), cols] + self.from_part[0, :, cols]
            if self.link_rows:
                self.first(i).start()
            if self.early:
                @pl.when(i < self.early)
                def _():
                    self.ahead(i).start()

        def run(self, chunk, drain=True):
            def step(i, carry):
                self.partial[:, self.cols(i)] = chunk(self.cols(i))
                self.pair(i, 0).start()
                self.pair(i, 1).start()
                if drain:
                    @pl.when(i > 0)
                    def _():
                        self.chip_sum(i - 1)
                return carry

            lax.fori_loop(0, self.chunks, step, 0)
            if drain:
                self.drain(self.chunks - 1)

        def drain(self, start=0):
            for i in range(start, self.chunks):
                self.chip_sum(i)
            if self.link_rows == rows:
                self.second().start()

        def kept(self):
            for i in range(self.chunks):
                self.pair(i, 1).wait_recv()

        def kept_rows(self, sub):
            return self.partial[block(me, sub), :] + self.from_part[1, pl.ds(sub * half, half), :]

        def rows_sum(self, sub):
            if sub == 0:
                for i in range(self.chunks):
                    self.first(i).wait_recv()
            else:
                for i in range(self.early):
                    self.ahead(i).wait_recv()
                self.second().wait_recv()
            return self.kept_rows(sub) + self.from_peer[pl.ds(sub * half, half), :]

        def pair_sent(self):
            for i in range(self.chunks):
                self.pair(i, 0).wait_send()
                self.pair(i, 1).wait_send()

        def link_sent(self):
            if self.link_rows:
                for i in range(self.chunks):
                    self.first(i).wait_send()
            if self.link_rows == rows:
                self.second().wait_send()
            for i in range(self.early):
                self.ahead(i).wait_send()

    x_in.wait()
    small_in[0].wait()
    small_in[1].wait()
    h1[block(me), :] = norm_rows(x_own[...].astype(F32), g1_ref[...], b1_ref[...]).astype(BF16)
    pl.semaphore_wait(barrier, 2)
    gather_h1 = Gather(h1, [(0, rows) + cut for cut in cuts(d, (4, 3, 3, 2))])
    gather_dy = Gather(dyf, [(0, rows, 0, d)])
    late = [(0, half, 0, d)] + [(half, half) + cut for cut in cuts(d, (2, 1))]
    for i in range(len(gather_h1.pieces)):
        gather_h1.send(i)
    dy_in.wait()
    gather_dy.send(0)

    small_in[2].wait()
    small_in[3].wait()
    pos_rows = jnp.broadcast_to(pos_ref[...].astype(F32), (hd, seq)).T
    angles = pos_rows * freq_ref[...]
    lane = lax.broadcasted_iota(jnp.int32, (seq, hd), 1)
    rot = hd // 4
    cosb[...] = jnp.cos(angles)
    sinb[...] = jnp.where(lane < rot, -1.0, 1.0) * jnp.sin(angles)

    def turn(v, sign):
        other = jnp.where(lane < rot, pltpu.roll(v, hd - rot, 1), pltpu.roll(v, rot, 1))
        other = jnp.where(lane < 2 * rot, other, 0.0)
        return v * cosb[...] + (sign * sinb[...]) * other

    for copy in weight_in[:3]:
        copy.wait()
    n_all = nqd + 2 * nkd

    def add(total, j, piece):
        total[...] = piece if j == 0 else total[...] + piece

    qkv_sum = part_c.at[:, pl.ds(0, n_all)]
    gather_h1.feed(0, lambda j, cols: add(qkv_sum, j, mm(h1[:, cols], wqkv[cols, :])))

    qkv = qkv_sum
    for k in range(nk):
        for g in range(grp):
            lo = (k * grp + g) * hd
            head = qkv[:, lo:lo + hd].astype(BF16).astype(F32)
            qs[k, g * seq:(g + 1) * seq, :] = turn(head, 1.0).astype(BF16)
        lo = nqd + k * hd
        kv[0, k] = turn(qkv[:, lo:lo + hd].astype(BF16).astype(F32), 1.0).astype(BF16)
        lo = nqd + nkd + k * hd
        kv[1, k] = qkv[:, lo:lo + hd].astype(BF16)
    put(h1, h1_out)
    query = lax.rem(lax.broadcasted_iota(jnp.int32, (grp * seq, seq), 0), seq)
    causal = query >= lax.broadcasted_iota(jnp.int32, (grp * seq, seq), 1)
    for k in range(nk):
        scores = jnp.where(causal, mm_bt(qs[k], kv[0, k]) * hd ** -0.5, -1e30)
        exped = jnp.exp(scores - jnp.max(scores, axis=-1, keepdims=True))
        prob[k] = exped / jnp.sum(exped, axis=-1, keepdims=True)
        head_ctx = mm(prob[k].astype(BF16), kv[1, k]).astype(BF16)
        for g in range(grp):
            lo = (k * grp + g) * hd
            ctx[:, lo:lo + hd] = head_ctx[g * seq:(g + 1) * seq, :]
    put(ctx, ctx_out)
    weight_in[3].wait()
    sum_attn = Scatter(4, part_a, dr_a, snd_a, lnk_a, rows)
    sum_attn.run(lambda cols: mm(ctx[...], wo[:, cols]))

    gather_dy.forward(0)
    gather_dy.finish(0)
    weight_in[4].wait()
    put(dyf, dy_out)
    nb = f // 2

    def down_back(j, carry):
        cols = pl.ds(pl.multiple_of(j * nb, nb), nb)
        tmat[:, cols] = mm_bt(dyf[...], w2[cols, :])
        return carry

    lax.fori_loop(0, f // nb, down_back, 0)

    gather_h2 = Gather(h2, late)
    small_in[4].wait()
    small_in[5].wait()
    for sub in (0, 1):
        if sub == 0:
            sum_attn.kept()
        own = pl.ds(sub * half, half)
        attn_rows = sum_attn.rows_sum(sub).astype(BF16)
        mid_rows = (x_own[own, :].astype(F32) + attn_rows.astype(F32)).astype(BF16)
        mid[own, :] = mid_rows
        h2[block(me, sub), :] = norm_rows(mid_rows.astype(F32), g2_ref[...], b2_ref[...]).astype(BF16)
        for i in ((0,) if sub == 0 else range(1, len(late))):
            gather_h2.send(i)
    weight_in[5].wait()

    def up(j, depth):
        for i in range(f // nb):
            cols = pl.ds(i * nb, nb)
            piece = mm(h2[:, depth], w1[depth, cols])
            if j == 0:
                part_c[:, cols] = piece
            elif j < len(late) - 2:
                part_c[:, cols] += piece
            else:
                relu_up = jnp.maximum((part_c[:, cols] + piece).astype(BF16).astype(F32), 0.0)
                act[:, cols] = (relu_up * relu_up).astype(BF16)
                du[:, cols] = (tmat[:, cols] * (2.0 * relu_up)).astype(BF16)

    gather_h2.feed(1, up)
    put(h2, h2_out)
    put(act, act_out)
    put(du, du_out)
    sum_dh2 = Scatter(6, part_b, dr_b, snd_b, lnk_b, rows, 2)
    sum_dh2.run(lambda cols: mm_bt(du[...], w1[cols, :]))

    sum_mlp = Scatter(4, part_c, dr_c, snd_c, lnk_c, half)
    sum_mlp.run(lambda cols: mm(act[...], w2[:, cols]), drain=False)

    gather_dx1 = Gather(dx1, late)
    normed2, scale2 = centre(mid[...].astype(F32))
    for sub in (0, 1):
        if sub == 0:
            sum_dh2.kept()
        dh2_rows = sum_dh2.rows_sum(sub).astype(BF16).astype(F32)
        own = slice(sub * half, (sub + 1) * half)
        grad_rows, grad_gain, grad_bias = norm_back(normed2[own], scale2[own], dh2_rows, g2_ref[...])
        dx1[block(me, sub), :] = (dyf[block(me, sub), :].astype(F32) + grad_rows).astype(BF16)
        for i in ((0,) if sub == 0 else range(1, len(late))):
            gather_dx1.send(i)
        if sub == 0:
            lng[0:1, :] = grad_gain
            lng[1:2, :] = grad_bias
        else:
            lng[0:1, :] += grad_gain
            lng[1:2, :] += grad_bias
    put(dx1.at[block(me)], dmid_out)
    lng_base = sems.take(2)
    lng_pair = remote(lng, lng_in.at[0], lng_base, part)
    lng_pair.start()
    sum_mlp.drain()
    low = pl.ds(half, half)
    send[pl.ds(rows, half), :] = snd_c[low, :]
    sum_mlp.kept()
    ykeep[...] = sum_mlp.kept_rows(1)
    put(ykeep, ykeep_out)
    put(mid.at[low], mid_out)
    lng_pair.wait_recv()
    lng_chip[...] = lng[...] + lng_in[0]
    lng_link = remote(lng_chip, lng_in.at[1], lng_base + 1, peer)
    lng_link.start()
    dctx_sum = tmat.at[:, pl.ds(0, nqd)]
    gather_dx1.feed(1, lambda j, cols: add(dctx_sum, j, mm_bt(dx1[:, cols], wo[:, cols])))
    put(dx1, dx1_out)

    dctx = dctx_sum[...].astype(BF16)
    for k in range(nk):
        for g in range(grp):
            lo = (k * grp + g) * hd
            gcs[k, g * seq:(g + 1) * seq, :] = dctx[:, lo:lo + hd]
    for k in range(nk):
        grad_v = mm_at(prob[k].astype(BF16), gcs[k]).astype(BF16)
        grad_p = mm_bt(gcs[k], kv[1, k])
        grad_s = (prob[k] * (grad_p - jnp.sum(grad_p * prob[k], axis=-1, keepdims=True)) * hd ** -0.5).astype(BF16)
        grad_q = mm(grad_s, kv[0, k])
        for g in range(grp):
            lo = (k * grp + g) * hd
            dqkv[:, lo:lo + hd] = turn(grad_q[g * seq:(g + 1) * seq, :], -1.0).astype(BF16)
        lo = nqd + k * hd
        dqkv[:, lo:lo + hd] = turn(mm_at(grad_s, qs[k]), -1.0).astype(BF16)
        lo = nqd + nkd + k * hd
        dqkv[:, lo:lo + hd] = grad_v
    put(dqkv, dqkv_out)
    sum_dh1 = Scatter(4, part_a, dr_d, send.at[pl.ds(0, rows)])
    sum_attn.pair_sent()
    sum_dh1.run(lambda cols: mm_bt(dqkv[...], wqkv[cols, :]), drain=False)
    sum_dh1.drain()
    put(send, send_out)
    sum_dh1.kept()
    for sub in (0, 1):
        hkeep[pl.ds(sub * half, half), :] = sum_dh1.kept_rows(sub)
    put(hkeep, hkeep_out)
    top = pl.ds(0, half)
    y_own[...] = (mid[top, :].astype(F32) + sum_mlp.rows_sum(0).astype(BF16).astype(F32)).astype(BF16)
    put(y_own, y_out)
    lng_link.wait_recv()
    dg2[...] = lng_chip[0:1, :] + lng_in[1, 0:1, :]
    db2[...] = lng_chip[1:2, :] + lng_in[1, 1:2, :]
    put(dg2, dg2_out)
    put(db2, db2_out)

    for gather in (gather_h1, gather_dy, gather_h2, gather_dx1):
        for kind in (0, 1, 2):
            for i in range(len(gather.pieces)):
                gather.copy(kind, i).wait_send()
    for scatter in (sum_dh2, sum_mlp, sum_dh1):
        scatter.pair_sent()
    for scatter in (sum_attn, sum_dh2, sum_mlp):
        scatter.link_sent()
    lng_pair.wait_send()
    lng_link.wait_send()
    for copy in outs:
        copy.wait()


def cuts(d, parts):
    unit, first, out = d // sum(parts), 0, []
    for n in parts:
        out.append((first, n * unit))
        first += n * unit
    return out


def chain(dims, x, dy, pos, freq, g1, b1, g2, b2, wq, wk, wv, wo, w1, w2):
    seq, d, hd, nq, nk, f, rows = dims
    grp = nq // nk
    nqd, nkd = nq * hd, nk * hd
    n_all = nqd + 2 * nkd
    half = rows // 2

    def arr(shape, dtype):
        return jax.ShapeDtypeStruct(shape, dtype)

    def vm(*shape, dtype=BF16):
        return pltpu.VMEM(shape, dtype)

    def vf(*shape):
        return pltpu.VMEM(shape, F32)

    out_shape = [arr((seq, d), BF16)] * 4 + [arr((seq, f), BF16)] * 2 + [arr((seq, nqd), BF16), arr((seq, n_all), BF16)] + [arr((half, d), BF16)] * 2 + [arr((rows, d), BF16), arr((rows + half, d), F32), arr((rows, d), F32), arr((half, d), F32)] + [arr((1, d), F32)] * 2
    n_sems = 3 * (4 + 1 + 3 + 3) + 2 * (4 + 6 + 4 + 4) + (5 + 9 + 5) + 2
    scratch = [
        pltpu.VMEM((1, seq), jnp.int32), vf(1, hd), vf(1, d), vf(1, d), vf(1, d), vf(1, d),
        vm(d, n_all), vm(nqd, d), vm(d, f), vm(f, d),
        vm(seq, d), vm(seq, d), vm(seq, d), vm(seq, d),
        vm(rows, d), vm(rows, d), vm(half, d), vf(seq, f), vm(seq, f), vm(seq, f),
        vm(nk, grp * seq, hd), vm(2, nk, seq, hd), vm(seq, nqd), vf(nk, grp * seq, seq),
        vf(seq, hd), vf(seq, hd), vm(nk, grp * seq, hd), vm(seq, n_all), vf(2, d),
        vf(seq, d), vf(seq, d), vf(seq, d),
        vf(2, rows, d), vf(2, rows, d), vf(2, rows, d), vf(2, rows, d),
        vf(rows, d), vf(rows, d), vf(rows, d), vf(rows, d), vf(rows, d), vf(half, d),
        vf(rows + half, d), vf(rows, d), vf(half, d), vf(2, 2, d), vf(2, d), vf(1, d), vf(1, d),
        pltpu.SemaphoreType.DMA((14,)), pltpu.SemaphoreType.DMA((len(out_shape),)),
        pltpu.SemaphoreType.DMA((n_sems,)), pltpu.SemaphoreType.DMA((n_sems,)),
    ]
    return pl.pallas_call(
        functools.partial(chain_kernel, dims),
        out_shape=out_shape,
        in_specs=[ANY] * 14,
        out_specs=[ANY] * len(out_shape),
        scratch_shapes=scratch,
        compiler_params=pltpu.CompilerParams(collective_id=0, has_side_effects=True, vmem_limit_bytes=VMEM_LIMIT),
        name="chain",
    )(x, dy, pos, freq, g1, b1, g2, b2, wq, wk, wv, wo, w1, w2)


SLOTS = 4
TILE = 256


def stream_grads(jobs, stage, sem):
    def copies(job, i, slot):
        return [pltpu.make_async_copy(stage.at[slot, pl.ds(0, job[1]), pl.ds(lo, n)], dst, sem.at[slot, c]) for c, (dst, lo, n) in enumerate(job[5](i))]

    done, pending = 0, []
    for job in jobs:
        ready, tile, tiles, width, compute, targets = job
        ready()

        def fill(i, slot):
            stage[slot, :tile, :width] = compute(i)
            for copy in copies(job, i, slot):
                copy.start()

        lead = min(SLOTS, tiles)
        for i in range(lead):
            slot = (done + i) % SLOTS
            if len(pending) == SLOTS:
                for copy in pending.pop(0):
                    copy.wait()
            fill(i, slot)
            pending.append(copies(job, i, slot))

        def step(i, carry, base=done):
            slot = lax.rem(base + i, SLOTS)
            for copy in copies(job, i - SLOTS, slot):
                copy.wait()
            fill(i, slot)
            return carry

        lax.fori_loop(lead, tiles, step, 0)
        if tiles > SLOTS:
            pending = [copies(job, i, (done + i) % SLOTS) for i in range(tiles - SLOTS, tiles)]
        done += tiles
    for group in pending:
        for copy in group:
            copy.wait()


def tile_at(i, tile, first=0):
    return pl.ds(pl.multiple_of(first + i * tile, tile), tile)


def outer_jobs(ready, left, right, targets, total, lead=0):
    jobs = []
    width = right.shape[1]
    if lead:
        small = TILE // 2
        jobs.append((ready, small, lead // small, width, lambda i: mm_at(left[:, tile_at(i, small)], right[...]), lambda i: targets(tile_at(i, small))))
        ready = lambda: None
    jobs.append((ready, TILE, (total - lead) // TILE, width, lambda i: mm_at(left[:, tile_at(i, TILE, lead)], right[...]), lambda i: targets(tile_at(i, TILE, lead))))
    return jobs


def start_loads(pairs, sem):
    loads = [pltpu.make_async_copy(src, dst, sem.at[i]) for i, (src, dst) in enumerate(pairs)]
    for copy in loads:
        copy.start()

    def ready(*which):
        return lambda: [loads[i].wait() for i in which] and None

    return ready


def grads_first_kernel(dims, act_hbm, dy_hbm, h1_hbm, dqkv_hbm, dw2, dwq, dwk, dwv, act, dyf, h1, dqkv, stage, in_sem, sem):
    seq, d, hd, nq, nk, f, rows = dims
    nqd, nkd = nq * hd, nk * hd
    ready = start_loads(((act_hbm, act), (dy_hbm, dyf), (h1_hbm, h1), (dqkv_hbm, dqkv)), in_sem)
    stream_grads(
        outer_jobs(ready(0, 1), act, dyf, lambda at: [(dw2.at[at], 0, d)], f, TILE)
        + outer_jobs(ready(2, 3), h1, dqkv, lambda at: [(dwq.at[at], 0, nqd), (dwk.at[at], nqd, nkd), (dwv.at[at], nqd + nkd, nkd)], d),
        stage, sem)


def grads_second_kernel(dims, order, h2_hbm, du_hbm, ctx_hbm, dx1_hbm, hkeep_hbm, recv_hbm, x_hbm, dmid_hbm, g1_hbm, dg2_hbm, db2_hbm, ykeep_hbm, mid_hbm, y_hbm,
                        y_out, dx_out, lng_out, dg2_out, db2_out, dw1, dwo,
                        h2, du, ctx, dx1, hkeep, recv, x, dmid, g1, ykeep, mid, y, lng, dg2, db2, stage, in_sem, end_sem, sem):
    seq, d, hd, nq, nk, f, rows = dims
    half = rows // 2
    top, low = pl.ds(0, half), pl.ds(half, half)
    ready = start_loads(((h2_hbm, h2), (du_hbm, du), (hkeep_hbm, hkeep), (recv_hbm, recv), (x_hbm, x), (dmid_hbm, dmid), (g1_hbm, g1),
                         (dg2_hbm, dg2), (db2_hbm, db2), (ykeep_hbm, ykeep), (mid_hbm, mid), (y_hbm, y.at[top]), (ctx_hbm, ctx), (dx1_hbm, dx1)), in_sem)
    ends = [pltpu.make_async_copy(src, dst, end_sem.at[i]) for i, (src, dst) in enumerate(((y, y_out), (dmid, dx_out), (lng, lng_out), (dg2, dg2_out), (db2, db2_out)))]

    def first_norm_back():
        ready(2, 3, 4, 5, 6, 7, 8, 9, 10, 11)()
        dh1 = (hkeep[...] + recv[pl.ds(0, rows), :]).astype(BF16).astype(F32)
        grad_rows, grad_gain, grad_bias = norm_rows_back(x[...].astype(F32), dh1, g1[...])
        dmid[...] = (dmid[...].astype(F32) + grad_rows).astype(BF16)
        lanes = lng.shape[1]
        for i, total in enumerate((grad_gain, grad_bias)):
            for j in range(d // lanes):
                at = i * (d // lanes) + j
                lng[at:at + 1, :] = total[:, j * lanes:(j + 1) * lanes]
        mlp = (ykeep[...] + recv[pl.ds(rows, half), :]).astype(BF16)
        y[low, :] = (mid[...].astype(F32) + mlp.astype(F32)).astype(BF16)
        for copy in ends:
            copy.start()

    def dw1_jobs(after, first, total):
        at = functools.partial(tile_at, tile=TILE, first=first)
        return [(after, TILE, total // TILE, f, lambda i: mm_at(h2[:, at(i)], du[...]), lambda i: [(dw1.at[at(i)], 0, f)])]

    lead = SLOTS * TILE
    stream_grads(
        dw1_jobs(ready(0, 1), 0, lead) + dw1_jobs(first_norm_back, lead, d - lead)
        + outer_jobs(ready(12, 13), ctx, dx1, lambda at: [(dwo.at[at], 0, d)], ctx.shape[1]),
        stage, sem)
    for copy in ends:
        copy.wait()


def cost(flops, nbytes):
    return pl.CostEstimate(flops=flops, bytes_accessed=nbytes, transcendentals=0)


def arr(shape, dtype=F32):
    return jax.ShapeDtypeStruct(shape, dtype)


def grads_first(dims, act, dyf, h1, dqkv):
    seq, d, hd, nq, nk, f, rows = dims
    nqd, nkd = nq * hd, nk * hd
    n_all = nqd + 2 * nkd
    return pl.pallas_call(
        functools.partial(grads_first_kernel, dims),
        out_shape=[arr((f, d)), arr((d, nqd)), arr((d, nkd)), arr((d, nkd))],
        in_specs=[ANY] * 4, out_specs=[ANY] * 4,
        scratch_shapes=[pltpu.VMEM((seq, f), BF16), pltpu.VMEM((seq, d), BF16), pltpu.VMEM((seq, d), BF16), pltpu.VMEM((seq, n_all), BF16),
                        pltpu.VMEM((SLOTS, TILE, d), F32), pltpu.SemaphoreType.DMA((4,)), pltpu.SemaphoreType.DMA((SLOTS, 3))],
        compiler_params=pltpu.CompilerParams(vmem_limit_bytes=VMEM_LIMIT),
        cost_estimate=cost(2 * seq * d * (f + n_all), 4 * d * (f + n_all)),
        name="grads_first",
    )(act, dyf, h1, dqkv)


def grads_second(dims, order, h2, du, ctx, dx1, hkeep, recv, x, dmid, g1, dg2, db2, ykeep, mid, y):
    seq, d, hd, nq, nk, f, rows = dims
    nqd, half = nq * hd, rows // 2

    def vb(*shape):
        return pltpu.VMEM(shape, BF16)

    def vf(*shape):
        return pltpu.VMEM(shape, F32)

    return pl.pallas_call(
        functools.partial(grads_second_kernel, dims),
        out_shape=[arr((rows, d), BF16), arr((rows, d), BF16), arr((2 * d // 128, 128)), arr((1, d)), arr((1, d)), arr((d, f)), arr((nqd, d))],
        in_specs=[ANY] * 15, out_specs=[ANY] * 7,
        scratch_shapes=[vb(seq, d), vb(seq, f), vb(seq, nqd), vb(seq, d), vf(rows, d), vf(rows + half, d), vb(rows, d), vb(rows, d), vf(1, d),
                        vf(half, d), vb(half, d), vb(rows, d), vf(2 * d // 128, 128), vf(1, d), vf(1, d),
                        vf(SLOTS, TILE, d), pltpu.SemaphoreType.DMA((14,)), pltpu.SemaphoreType.DMA((5,)), pltpu.SemaphoreType.DMA((SLOTS, 3))],
        compiler_params=pltpu.CompilerParams(vmem_limit_bytes=VMEM_LIMIT),
        cost_estimate=cost(2 * seq * d * (f + nqd), 4 * d * (f + nqd)),
        name="grads_second",
    )(order, h2, du, ctx, dx1, hkeep, recv, x, dmid, g1, dg2, db2, ykeep, mid, y)


def layer_step(x, dy, positions, g1, b1, g2, b2, wq, wk, wv, wo, w1, w2, head_dim, n_tp):
    rows, batch, d = x.shape
    seq = positions.shape[0]
    nq, nk, f = wq.shape[1] // head_dim, wk.shape[1] // head_dim, w1.shape[1]
    dims = (seq, d, head_dim, nq, nk, f, rows)
    rot = head_dim // 4
    freq = np.zeros((1, head_dim), np.float32)
    freq[0, :2 * rot] = np.tile(ROPE_BASE ** (-np.arange(rot) / rot), 2)
    x2, dy2 = x.reshape(rows, d), dy.reshape(rows, d)
    g1, b1, g2, b2 = (v.reshape(1, d) for v in (g1, b1, g2, b2))
    (h1, h2, dyf, dx1, act, du, ctx, dqkv, y, mid, dmid, send, hkeep, ykeep, dg2, db2) = chain(
        dims, x2, dy2, positions.reshape(1, seq), jnp.asarray(freq), g1, b1, g2, b2, wq, wk, wv, wo, w1, w2)

    def swap(v, bit):
        return lax.ppermute(v, 'tp', [(i, i ^ bit) for i in range(n_tp)])

    recv = swap(send, 2)
    dw2, dwq, dwk, dwv = grads_first(dims, act, dyf, h1, dqkv)
    y, dx, lng, dg2, db2, dw1, dwo = grads_second(dims, dw2, h2, du, ctx, dx1, hkeep, recv, x2, dmid, g1, dg2, db2, ykeep, mid, y)
    others = [swap(lng, bit) for bit in (1, 2, 3)]
    sums = ((lng + others[0]) + (others[1] + others[2])).reshape(2, d)
    return (y.reshape(x.shape), dx.reshape(x.shape), sums[0], sums[1], dg2.reshape(d), db2.reshape(d), dwq, dwk, dwv, dwo, dw1, dw2)


def solution(mesh):
    seq_spec = P(('dp', 'tp'))
    col_spec = P(None, 'tp')
    row_spec = P('tp', None)
    grad_col_spec = P('dp', 'tp')
    grad_row_spec = P(('dp', 'tp'), None)
    in_specs = (seq_spec, seq_spec, P('dp'), P(), P(), P(), P(), col_spec, col_spec, col_spec, row_spec, col_spec, row_spec)
    out_specs = (seq_spec, seq_spec, P('dp'), P('dp'), P('dp'), P('dp'), grad_col_spec, grad_col_spec, grad_col_spec, grad_row_spec, grad_col_spec, grad_row_spec)

    def run_layer(resid_in, grad_out, positions, ln1_gain, ln1_bias, ln2_gain, ln2_bias, w_query, w_key, w_value, w_out, w_up, w_down):
        step_fn = functools.partial(layer_step, head_dim=w_key.shape[1] // KV_HEADS, n_tp=mesh.shape['tp'])
        sharded = jax.shard_map(step_fn, mesh=mesh, in_specs=in_specs, out_specs=out_specs, check_vma=False)
        return sharded(resid_in, grad_out, positions, ln1_gain, ln1_bias, ln2_gain, ln2_bias, w_query, w_key, w_value, w_out, w_up, w_down)

    return run_layer
```

```python
import functools
import math
import numpy as np
import jax
import jax.numpy as jnp
from jax import lax
from jax.experimental import pallas as pl
from jax.experimental.pallas import tpu as pltpu
from jax.sharding import PartitionSpec as P

KV_HEADS = 8
LN_EPS = 1e-5
ROPE_BASE = 10000.0
F32 = jnp.float32
BF16 = jnp.bfloat16
ANY = pl.BlockSpec(memory_space=pl.ANY)
VMEM = pl.BlockSpec(memory_space=pltpu.VMEM)
VMEM_LIMIT = 67_043_328


def mm(a, b):
    return jnp.dot(a, b, preferred_element_type=F32)


def mm_bt(a, b):
    return lax.dot_general(a, b, (((1,), (1,)), ((), ())), preferred_element_type=F32)


def mm_at(a, b):
    return lax.dot_general(a, b, (((0,), (0,)), ((), ())), preferred_element_type=F32)


def centre(rows):
    centred = rows - jnp.mean(rows, axis=-1, keepdims=True)
    scale = lax.rsqrt(jnp.mean(centred * centred, axis=-1, keepdims=True) + LN_EPS)
    return centred * scale, scale


def norm_rows(rows, gain, bias):
    normed, _ = centre(rows)
    return normed * (1.0 + gain) + bias


def norm_rows_back(rows, grad, gain):
    return norm_back(*centre(rows), grad, gain)


def norm_back(normed, scale, grad, gain):
    weighted = grad * (1.0 + gain)
    inner = jnp.mean(weighted * normed, axis=-1, keepdims=True)
    grad_rows = scale * (weighted - jnp.mean(weighted, axis=-1, keepdims=True) - normed * inner)
    return grad_rows, jnp.sum(grad * normed, axis=0, keepdims=True), jnp.sum(grad, axis=0, keepdims=True)


class Sems:
    def __init__(self):
        self.next = 0

    def take(self, count):
        base = self.next
        self.next += count
        return base


def chain_kernel(dims, x_hbm, dy_hbm, pos_hbm, freq_hbm, g1_hbm, b1_hbm, g2_hbm, b2_hbm, wq_hbm, wk_hbm, wv_hbm, wo_hbm, w1_hbm, w2_hbm,
                 h1_out, h2_out, dy_out, dx1_out, act_out, du_out, ctx_out, dqkv_out, y_out, mid_out, dmid_out, send_out, hkeep_out, ykeep_out, dg2_out, db2_out,
                 pos_ref, freq_ref, g1_ref, b1_ref, g2_ref, b2_ref,
                 wqkv, wo, w1, w2, h1, h2, dyf, dx1, x_own, mid, y_own, tmat, act, du, qs, kv, ctx, prob, cosb, sinb, gcs, dqkv, lng,
                 part_a, part_b, part_c, dr_a, dr_b, dr_c, dr_d, snd_a, snd_b, snd_c, lnk_a, lnk_b, lnk_c, send, hkeep, ykeep, lng_in, lng_chip, dg2, db2,
                 local_sem, out_sem, send_sem, recv_sem):
    seq, d, hd, nq, nk, f, rows = dims
    grp = nq // nk
    half = rows // 2
    me = lax.axis_index("tp")
    part, peer, diag = me ^ 1, me ^ 3, me ^ 2
    sems = Sems()

    def block(idx, sub=None):
        if sub is None:
            return pl.ds(pl.multiple_of(idx * rows, rows), rows)
        return pl.ds(pl.multiple_of(idx * rows + sub * half, half), half)

    def remote(src, dst, sem, dev):
        return pltpu.make_async_remote_copy(src, dst, send_sem.at[sem], recv_sem.at[sem], device_id={"tp": dev})

    def local(src, dst, idx):
        return pltpu.make_async_copy(src, dst, local_sem.at[idx])

    x_in = local(x_hbm, x_own, 0)
    dy_in = local(dy_hbm, dyf.at[block(me)], 1)
    nqd, nkd = nq * hd, nk * hd
    weight_in = [
        local(wq_hbm, wqkv.at[:, pl.ds(0, nqd)], 2),
        local(wk_hbm, wqkv.at[:, pl.ds(nqd, nkd)], 3),
        local(wv_hbm, wqkv.at[:, pl.ds(nqd + nkd, nkd)], 4),
        local(wo_hbm, wo, 5),
        local(w2_hbm, w2, 6),
        local(w1_hbm, w1, 7),
    ]
    small_in = [local(src, dst, 8 + i) for i, (src, dst) in enumerate((
        (g1_hbm, g1_ref), (b1_hbm, b1_ref), (pos_hbm, pos_ref), (freq_hbm, freq_ref), (g2_hbm, g2_ref), (b2_hbm, b2_ref)))]
    x_in.start()
    for copy in small_in:
        copy.start()
    dy_in.start()
    barrier = pltpu.get_barrier_semaphore()
    for dev in (part, peer):
        pl.semaphore_signal(barrier, inc=1, device_id={"tp": dev})
    for copy in weight_in:
        copy.start()

    outs = []

    def put(src, dst):
        copy = pltpu.make_async_copy(src, dst, out_sem.at[len(outs)])
        copy.start()
        outs.append(copy)

    class Gather:
        def __init__(self, buf, pieces):
            self.buf, self.pieces, self.base = buf, pieces, sems.take(3 * len(pieces))

        def copy(self, kind, i):
            owner = (me, me, peer)[kind]
            dev = (peer, part, part)[kind]
            row, n_rows, col, n_cols = self.pieces[i]
            at = self.buf.at[pl.ds(pl.multiple_of(owner * rows + row, half), n_rows), pl.ds(col, n_cols)]
            return remote(at, at, self.base + len(self.pieces) * kind + i, dev)

        def send(self, i):
            self.copy(0, i).start()
            self.copy(1, i).start()

        def forward(self, i):
            self.copy(0, i).wait_recv()
            self.copy(2, i).start()

        def finish(self, i):
            self.copy(1, i).wait_recv()
            self.copy(2, i).wait_recv()

        def feed(self, first, use):
            count = len(self.pieces)
            for i in range(first):
                self.forward(i)
            self.forward(first)
            for i in range(first):
                self.finish(i)
            for i in range(first, count):
                if i + 1 < count:
                    self.forward(i + 1)
                self.finish(i)
                use(i - first, pl.ds(self.pieces[i][2], self.pieces[i][3]))

    class Scatter:
        def __init__(self, chunks, partial, from_part, summed, from_peer=None, link_rows=0, early=0):
            self.chunks, self.cw, self.link_rows, self.early = chunks, d // chunks, link_rows, early
            self.partial, self.from_part, self.summed, self.from_peer = partial, from_part, summed, from_peer
            self.base = sems.take(2 * chunks)
            self.link = sems.take(chunks + 1 + early) if link_rows else None

        def cols(self, i):
            return pl.ds(pl.multiple_of(i * self.cw, self.cw), self.cw)

        def pair(self, i, kind):
            owner = (diag, part)[kind]
            return remote(self.partial.at[block(owner), self.cols(i)], self.from_part.at[kind, :, self.cols(i)], self.base + self.chunks * kind + i, part)

        def first(self, i):
            top = pl.ds(0, half)
            return remote(self.summed.at[top, self.cols(i)], self.from_peer.at[top, self.cols(i)], self.link + i, peer)

        def second(self):
            at = (pl.ds(half, half), pl.ds(self.early * self.cw, d - self.early * self.cw))
            return remote(self.summed.at[at], self.from_peer.at[at], self.link + self.chunks, peer)

        def ahead(self, i):
            at = (pl.ds(half, half), self.cols(i))
            return remote(self.summed.at[at], self.from_peer.at[at], self.link + self.chunks + 1 + i, peer)

        def chip_sum(self, i):
            self.pair(i, 0).wait_recv()
            cols = self.cols(i)
            self.summed[:, cols] = self.partial[block(peer), cols] + self.from_part[0, :, cols]
            if self.link_rows:
                self.first(i).start()
            if self.early:
                @pl.when(i < self.early)
                def _():
                    self.ahead(i).start()

        def run(self, chunk, lag=0):
            def step(i, carry):
                self.partial[:, self.cols(i)] = chunk(self.cols(i))
                self.pair(i, 0).start()
                self.pair(i, 1).start()
                if lag:
                    @pl.when(i >= lag)
                    def _():
                        self.chip_sum(i - lag)
                return carry

            lax.fori_loop(0, self.chunks, step, 0)
            if lag:
                self.drain(self.chunks - lag)

        def drain(self, start=0):
            for i in range(start, self.chunks):
                self.chip_sum(i)
            if self.link_rows == rows:
                self.second().start()

        def kept(self):
            for i in range(self.chunks):
                self.pair(i, 1).wait_recv()

        def kept_rows(self, sub):
            return self.partial[block(me, sub), :] + self.from_part[1, pl.ds(sub * half, half), :]

        def rows_sum(self, sub):
            if sub == 0:
                for i in range(self.chunks):
                    self.first(i).wait_recv()
            else:
                for i in range(self.early):
                    self.ahead(i).wait_recv()
                self.second().wait_recv()
            return self.kept_rows(sub) + self.from_peer[pl.ds(sub * half, half), :]

        def pair_sent(self):
            for i in range(self.chunks):
                self.pair(i, 0).wait_send()
                self.pair(i, 1).wait_send()

        def link_sent(self):
            if self.link_rows:
                for i in range(self.chunks):
                    self.first(i).wait_send()
            if self.link_rows == rows:
                self.second().wait_send()
            for i in range(self.early):
                self.ahead(i).wait_send()

    x_in.wait()
    small_in[0].wait()
    small_in[1].wait()
    h1[block(me), :] = norm_rows(x_own[...].astype(F32), g1_ref[...], b1_ref[...]).astype(BF16)
    pl.semaphore_wait(barrier, 2)
    gather_h1 = Gather(h1, [(0, rows) + cut for cut in cuts(d, (4, 3, 3, 2))])
    gather_dy = Gather(dyf, [(0, rows, 0, d)])
    late = [(0, half, 0, d)] + [(half, half) + cut for cut in cuts(d, (1, 1))]
    for i in range(len(gather_h1.pieces)):
        gather_h1.send(i)
    dy_in.wait()
    gather_dy.send(0)

    small_in[2].wait()
    small_in[3].wait()
    pos_rows = jnp.broadcast_to(pos_ref[...].astype(F32), (hd, seq)).T
    angles = pos_rows * freq_ref[...]
    lane = lax.broadcasted_iota(jnp.int32, (seq, hd), 1)
    rot = hd // 4
    cosb[...] = jnp.cos(angles)
    sinb[...] = jnp.where(lane < rot, -1.0, 1.0) * jnp.sin(angles)

    def turn(v, sign):
        other = jnp.where(lane < rot, pltpu.roll(v, hd - rot, 1), pltpu.roll(v, rot, 1))
        other = jnp.where(lane < 2 * rot, other, 0.0)
        return v * cosb[...] + (sign * sinb[...]) * other

    for copy in weight_in[:3]:
        copy.wait()
    n_all = nqd + 2 * nkd

    def add(total, j, piece):
        total[...] = piece if j == 0 else total[...] + piece

    qkv_sum = part_c.at[:, pl.ds(0, n_all)]
    gather_h1.feed(0, lambda j, cols: add(qkv_sum, j, mm(h1[:, cols], wqkv[cols, :])))

    qkv = qkv_sum
    for k in range(nk):
        for g in range(grp):
            lo = (k * grp + g) * hd
            head = qkv[:, lo:lo + hd].astype(BF16).astype(F32)
            qs[k, g * seq:(g + 1) * seq, :] = turn(head, 1.0).astype(BF16)
        lo = nqd + k * hd
        kv[0, k] = turn(qkv[:, lo:lo + hd].astype(BF16).astype(F32), 1.0).astype(BF16)
        lo = nqd + nkd + k * hd
        kv[1, k] = qkv[:, lo:lo + hd].astype(BF16)
    put(h1, h1_out)
    query = lax.rem(lax.broadcasted_iota(jnp.int32, (grp * seq, seq), 0), seq)
    causal = query >= lax.broadcasted_iota(jnp.int32, (grp * seq, seq), 1)
    for k in range(nk):
        scores = jnp.where(causal, mm_bt(qs[k], kv[0, k]) * hd ** -0.5, -1e30)
        exped = jnp.exp(scores - jnp.max(scores, axis=-1, keepdims=True))
        prob[k] = exped / jnp.sum(exped, axis=-1, keepdims=True)
        head_ctx = mm(prob[k].astype(BF16), kv[1, k]).astype(BF16)
        for g in range(grp):
            lo = (k * grp + g) * hd
            ctx[:, lo:lo + hd] = head_ctx[g * seq:(g + 1) * seq, :]
    put(ctx, ctx_out)
    weight_in[3].wait()
    sum_attn = Scatter(6, part_a, dr_a, snd_a, lnk_a, rows)
    sum_attn.run(lambda cols: mm(ctx[...], wo[:, cols]), lag=2)

    gather_dy.forward(0)
    gather_dy.finish(0)
    weight_in[4].wait()
    put(dyf, dy_out)
    nb = f // 2

    def down_back(j, carry):
        cols = pl.ds(pl.multiple_of(j * nb, nb), nb)
        tmat[:, cols] = mm_bt(dyf[...], w2[cols, :])
        return carry

    lax.fori_loop(0, f // nb, down_back, 0)

    gather_h2 = Gather(h2, late)
    small_in[4].wait()
    small_in[5].wait()
    for sub in (0, 1):
        if sub == 0:
            sum_attn.kept()
        own = pl.ds(sub * half, half)
        attn_rows = sum_attn.rows_sum(sub).astype(BF16)
        mid_rows = (x_own[own, :].astype(F32) + attn_rows.astype(F32)).astype(BF16)
        mid[own, :] = mid_rows
        h2[block(me, sub), :] = norm_rows(mid_rows.astype(F32), g2_ref[...], b2_ref[...]).astype(BF16)
        for i in ((0,) if sub == 0 else range(1, len(late))):
            gather_h2.send(i)
    weight_in[5].wait()

    def up(j, depth):
        cols = pl.ds(0, f)
        piece = mm(h2[:, depth], w1[depth, :])
        if j == 0:
            part_c[:, cols] = piece
        elif j < len(late) - 2:
            part_c[:, cols] += piece
        else:
            relu_up = jnp.maximum((part_c[:, cols] + piece).astype(BF16).astype(F32), 0.0)
            act[...] = (relu_up * relu_up).astype(BF16)
            du[...] = (tmat[...] * (2.0 * relu_up)).astype(BF16)

    gather_h2.feed(1, up)
    put(h2, h2_out)
    put(act, act_out)
    put(du, du_out)
    sum_dh2 = Scatter(12, part_b, dr_b, snd_b, lnk_b, rows, 4)
    sum_dh2.run(lambda cols: mm_bt(du[...], w1[cols, :]), lag=2)

    sum_mlp = Scatter(4, part_c, dr_c, snd_c, lnk_c, half)
    sum_mlp.run(lambda cols: mm(act[...], w2[:, cols]))

    gather_dx1 = Gather(dx1, late)
    normed2, scale2 = centre(mid[...].astype(F32))
    for sub in (0, 1):
        if sub == 0:
            sum_dh2.kept()
        dh2_rows = sum_dh2.rows_sum(sub).astype(BF16).astype(F32)
        own = slice(sub * half, (sub + 1) * half)
        grad_rows, grad_gain, grad_bias = norm_back(normed2[own], scale2[own], dh2_rows, g2_ref[...])
        dx1[block(me, sub), :] = (dyf[block(me, sub), :].astype(F32) + grad_rows).astype(BF16)
        for i in ((0,) if sub == 0 else range(1, len(late))):
            gather_dx1.send(i)
        if sub == 0:
            lng[0:1, :] = grad_gain
            lng[1:2, :] = grad_bias
        else:
            lng[0:1, :] += grad_gain
            lng[1:2, :] += grad_bias
    put(dx1.at[block(me)], dmid_out)
    lng_base = sems.take(2)
    lng_pair = remote(lng, lng_in.at[0], lng_base, part)
    lng_pair.start()
    sum_mlp.drain()
    low = pl.ds(half, half)
    send[pl.ds(rows, half), :] = snd_c[low, :]
    sum_mlp.kept()
    ykeep[...] = sum_mlp.kept_rows(1)
    put(ykeep, ykeep_out)
    put(mid.at[low], mid_out)
    lng_pair.wait_recv()
    lng_chip[...] = lng[...] + lng_in[0]
    lng_link = remote(lng_chip, lng_in.at[1], lng_base + 1, peer)
    lng_link.start()
    dctx_sum = tmat.at[:, pl.ds(0, nqd)]
    gather_dx1.feed(1, lambda j, cols: add(dctx_sum, j, mm_bt(dx1[:, cols], wo[:, cols])))
    put(dx1, dx1_out)

    dctx = dctx_sum[...].astype(BF16)
    for k in range(nk):
        for g in range(grp):
            lo = (k * grp + g) * hd
            gcs[k, g * seq:(g + 1) * seq, :] = dctx[:, lo:lo + hd]
    for k in range(nk):
        grad_v = mm_at(prob[k].astype(BF16), gcs[k]).astype(BF16)
        grad_p = mm_bt(gcs[k], kv[1, k])
        grad_s = (prob[k] * (grad_p - jnp.sum(grad_p * prob[k], axis=-1, keepdims=True)) * hd ** -0.5).astype(BF16)
        grad_q = mm(grad_s, kv[0, k])
        for g in range(grp):
            lo = (k * grp + g) * hd
            dqkv[:, lo:lo + hd] = turn(grad_q[g * seq:(g + 1) * seq, :], -1.0).astype(BF16)
        lo = nqd + k * hd
        dqkv[:, lo:lo + hd] = turn(mm_at(grad_s, qs[k]), -1.0).astype(BF16)
        lo = nqd + nkd + k * hd
        dqkv[:, lo:lo + hd] = grad_v
    put(dqkv, dqkv_out)
    sum_dh1 = Scatter(2, part_a, dr_d, send.at[pl.ds(0, rows)])
    sum_attn.pair_sent()
    sum_dh1.run(lambda cols: mm_bt(dqkv[...], wqkv[cols, :]))
    sum_dh1.drain()
    put(send, send_out)
    sum_dh1.kept()
    for sub in (0, 1):
        hkeep[pl.ds(sub * half, half), :] = sum_dh1.kept_rows(sub)
    put(hkeep, hkeep_out)
    top = pl.ds(0, half)
    y_own[...] = (mid[top, :].astype(F32) + sum_mlp.rows_sum(0).astype(BF16).astype(F32)).astype(BF16)
    put(y_own, y_out)
    lng_link.wait_recv()
    dg2[...] = lng_chip[0:1, :] + lng_in[1, 0:1, :]
    db2[...] = lng_chip[1:2, :] + lng_in[1, 1:2, :]
    put(dg2, dg2_out)
    put(db2, db2_out)

    for gather in (gather_h1, gather_dy, gather_h2, gather_dx1):
        for kind in (0, 1, 2):
            for i in range(len(gather.pieces)):
                gather.copy(kind, i).wait_send()
    for scatter in (sum_dh2, sum_mlp, sum_dh1):
        scatter.pair_sent()
    for scatter in (sum_attn, sum_dh2, sum_mlp):
        scatter.link_sent()
    lng_pair.wait_send()
    lng_link.wait_send()
    for copy in outs:
        copy.wait()


def cuts(d, parts):
    unit, first, out = d // sum(parts), 0, []
    for n in parts:
        out.append((first, n * unit))
        first += n * unit
    return out


def chain(dims, x, dy, pos, freq, g1, b1, g2, b2, wq, wk, wv, wo, w1, w2):
    seq, d, hd, nq, nk, f, rows = dims
    grp = nq // nk
    nqd, nkd = nq * hd, nk * hd
    n_all = nqd + 2 * nkd
    half = rows // 2

    def arr(shape, dtype):
        return jax.ShapeDtypeStruct(shape, dtype)

    def vm(*shape, dtype=BF16):
        return pltpu.VMEM(shape, dtype)

    def vf(*shape):
        return pltpu.VMEM(shape, F32)

    out_shape = [arr((seq, d), BF16)] * 4 + [arr((seq, f), BF16)] * 2 + [arr((seq, nqd), BF16), arr((seq, n_all), BF16)] + [arr((half, d), BF16)] * 2 + [arr((rows, d), BF16), arr((rows + half, d), F32), arr((rows, d), F32), arr((half, d), F32)] + [arr((1, d), F32)] * 2
    n_sems = 3 * (4 + 1 + 3 + 3) + 2 * (6 + 12 + 4 + 2) + (7 + 17 + 5) + 2
    scratch = [
        pltpu.VMEM((1, seq), jnp.int32), vf(1, hd), vf(1, d), vf(1, d), vf(1, d), vf(1, d),
        vm(d, n_all), vm(nqd, d), vm(d, f), vm(f, d),
        vm(seq, d), vm(seq, d), vm(seq, d), vm(seq, d),
        vm(rows, d), vm(rows, d), vm(half, d), vf(seq, f), vm(seq, f), vm(seq, f),
        vm(nk, grp * seq, hd), vm(2, nk, seq, hd), vm(seq, nqd), vf(nk, grp * seq, seq),
        vf(seq, hd), vf(seq, hd), vm(nk, grp * seq, hd), vm(seq, n_all), vf(2, d),
        vf(seq, d), vf(seq, d), vf(seq, d),
        vf(2, rows, d), vf(2, rows, d), vf(2, rows, d), vf(2, rows, d),
        vf(rows, d), vf(rows, d), vf(rows, d), vf(rows, d), vf(rows, d), vf(half, d),
        vf(rows + half, d), vf(rows, d), vf(half, d), vf(2, 2, d), vf(2, d), vf(1, d), vf(1, d),
        pltpu.SemaphoreType.DMA((14,)), pltpu.SemaphoreType.DMA((len(out_shape),)),
        pltpu.SemaphoreType.DMA((n_sems,)), pltpu.SemaphoreType.DMA((n_sems,)),
    ]
    return pl.pallas_call(
        functools.partial(chain_kernel, dims),
        out_shape=out_shape,
        in_specs=[ANY] * 14,
        out_specs=[ANY] * len(out_shape),
        scratch_shapes=scratch,
        compiler_params=pltpu.CompilerParams(collective_id=0, has_side_effects=True, vmem_limit_bytes=VMEM_LIMIT),
        name="chain",
    )(x, dy, pos, freq, g1, b1, g2, b2, wq, wk, wv, wo, w1, w2)


SLOTS = 4
TILE = 256


def stream_grads(jobs, stage, sem):
    def copies(job, i, slot):
        return [pltpu.make_async_copy(stage.at[slot, pl.ds(0, job[1]), pl.ds(lo, n)], dst, sem.at[slot, c]) for c, (dst, lo, n) in enumerate(job[5](i))]

    done, pending = 0, []
    for job in jobs:
        ready, tile, tiles, width, compute, targets = job
        ready()

        def fill(i, slot):
            stage[slot, :tile, :width] = compute(i)
            for copy in copies(job, i, slot):
                copy.start()

        lead = min(SLOTS, tiles)
        for i in range(lead):
            slot = (done + i) % SLOTS
            if len(pending) == SLOTS:
                for copy in pending.pop(0):
                    copy.wait()
            fill(i, slot)
            pending.append(copies(job, i, slot))

        def step(i, carry, base=done):
            slot = lax.rem(base + i, SLOTS)
            for copy in copies(job, i - SLOTS, slot):
                copy.wait()
            fill(i, slot)
            return carry

        lax.fori_loop(lead, tiles, step, 0)
        if tiles > SLOTS:
            pending = [copies(job, i, (done + i) % SLOTS) for i in range(tiles - SLOTS, tiles)]
        done += tiles
    for group in pending:
        for copy in group:
            copy.wait()


def tile_at(i, tile, first=0):
    return pl.ds(pl.multiple_of(first + i * tile, tile), tile)


def outer_jobs(ready, left, right, targets, total, lead=0):
    jobs = []
    width = right.shape[1]
    if lead:
        small = TILE // 2
        jobs.append((ready, small, lead // small, width, lambda i: mm_at(left[:, tile_at(i, small)], right[...]), lambda i: targets(tile_at(i, small))))
        ready = lambda: None
    jobs.append((ready, TILE, (total - lead) // TILE, width, lambda i: mm_at(left[:, tile_at(i, TILE, lead)], right[...]), lambda i: targets(tile_at(i, TILE, lead))))
    return jobs


def start_loads(pairs, sem):
    loads = [pltpu.make_async_copy(src, dst, sem.at[i]) for i, (src, dst) in enumerate(pairs)]
    for copy in loads:
        copy.start()

    def ready(*which):
        def wait():
            for i in which:
                loads[i].wait()

        return wait

    return ready


def grads_first_kernel(dims, act_hbm, dy_hbm, h1_hbm, dqkv_hbm, dw2, dwq, dwk, dwv, act, dyf, h1, dqkv, stage, in_sem, sem):
    seq, d, hd, nq, nk, f, rows = dims
    nqd, nkd = nq * hd, nk * hd
    ready = start_loads(((act_hbm, act), (dy_hbm, dyf), (h1_hbm, h1), (dqkv_hbm, dqkv)), in_sem)
    stream_grads(
        outer_jobs(ready(0, 1), act, dyf, lambda at: [(dw2.at[at], 0, d)], f, TILE)
        + outer_jobs(ready(2, 3), h1, dqkv, lambda at: [(dwq.at[at], 0, nqd), (dwk.at[at], nqd, nkd), (dwv.at[at], nqd + nkd, nkd)], d),
        stage, sem)


def grads_second_kernel(dims, order, h2_hbm, du_hbm, ctx_hbm, dx1_hbm, hkeep_hbm, recv_hbm, x_hbm, dmid_hbm, g1_hbm, dg2_hbm, db2_hbm, ykeep_hbm, mid_hbm, y_hbm,
                        y_out, dx_out, lng_out, dg2_out, db2_out, dw1, dwo,
                        h2, du, ctx, dx1, hkeep, recv, x, dmid, g1, ykeep, mid, y, lng, dg2, db2, stage, in_sem, end_sem, sem):
    seq, d, hd, nq, nk, f, rows = dims
    half = rows // 2
    top, low = pl.ds(0, half), pl.ds(half, half)
    ready = start_loads(((h2_hbm, h2), (du_hbm, du), (hkeep_hbm, hkeep), (recv_hbm, recv), (x_hbm, x), (dmid_hbm, dmid), (g1_hbm, g1),
                         (dg2_hbm, dg2), (db2_hbm, db2), (ykeep_hbm, ykeep), (mid_hbm, mid), (y_hbm, y.at[top]), (ctx_hbm, ctx), (dx1_hbm, dx1)), in_sem)
    ends = [pltpu.make_async_copy(src, dst, end_sem.at[i]) for i, (src, dst) in enumerate(((y, y_out), (dmid, dx_out), (lng, lng_out), (dg2, dg2_out), (db2, db2_out)))]

    def first_norm_back():
        ready(2, 3, 4, 5, 6, 7, 8, 9, 10, 11)()
        dh1 = (hkeep[...] + recv[pl.ds(0, rows), :]).astype(BF16).astype(F32)
        grad_rows, grad_gain, grad_bias = norm_rows_back(x[...].astype(F32), dh1, g1[...])
        dmid[...] = (dmid[...].astype(F32) + grad_rows).astype(BF16)
        lanes = lng.shape[1]
        for i, total in enumerate((grad_gain, grad_bias)):
            for j in range(d // lanes):
                at = i * (d // lanes) + j
                lng[at:at + 1, :] = total[:, j * lanes:(j + 1) * lanes]
        mlp = (ykeep[...] + recv[pl.ds(rows, half), :]).astype(BF16)
        y[low, :] = (mid[...].astype(F32) + mlp.astype(F32)).astype(BF16)
        for copy in ends:
            copy.start()

    def dw1_jobs(after, first, total):
        at = functools.partial(tile_at, tile=TILE, first=first)
        return [(after, TILE, total // TILE, f, lambda i: mm_at(h2[:, at(i)], du[...]), lambda i: [(dw1.at[at(i)], 0, f)])]

    lead = SLOTS * TILE
    stream_grads(
        dw1_jobs(ready(0, 1), 0, lead) + dw1_jobs(first_norm_back, lead, d - lead)
        + outer_jobs(ready(12, 13), ctx, dx1, lambda at: [(dwo.at[at], 0, d)], ctx.shape[1]),
        stage, sem)
    for copy in ends:
        copy.wait()


def cost(flops, nbytes):
    return pl.CostEstimate(flops=flops, bytes_accessed=nbytes, transcendentals=0)


def arr(shape, dtype=F32):
    return jax.ShapeDtypeStruct(shape, dtype)


def grads_first(dims, act, dyf, h1, dqkv):
    seq, d, hd, nq, nk, f, rows = dims
    nqd, nkd = nq * hd, nk * hd
    n_all = nqd + 2 * nkd
    return pl.pallas_call(
        functools.partial(grads_first_kernel, dims),
        out_shape=[arr((f, d)), arr((d, nqd)), arr((d, nkd)), arr((d, nkd))],
        in_specs=[ANY] * 4, out_specs=[ANY] * 4,
        scratch_shapes=[pltpu.VMEM((seq, f), BF16), pltpu.VMEM((seq, d), BF16), pltpu.VMEM((seq, d), BF16), pltpu.VMEM((seq, n_all), BF16),
                        pltpu.VMEM((SLOTS, TILE, d), F32), pltpu.SemaphoreType.DMA((4,)), pltpu.SemaphoreType.DMA((SLOTS, 3))],
        compiler_params=pltpu.CompilerParams(vmem_limit_bytes=VMEM_LIMIT),
        cost_estimate=cost(2 * seq * d * (f + n_all), 4 * d * (f + n_all)),
        name="grads_first",
    )(act, dyf, h1, dqkv)


def grads_second(dims, order, h2, du, ctx, dx1, hkeep, recv, x, dmid, g1, dg2, db2, ykeep, mid, y):
    seq, d, hd, nq, nk, f, rows = dims
    nqd, half = nq * hd, rows // 2

    def vb(*shape):
        return pltpu.VMEM(shape, BF16)

    def vf(*shape):
        return pltpu.VMEM(shape, F32)

    return pl.pallas_call(
        functools.partial(grads_second_kernel, dims),
        out_shape=[arr((rows, d), BF16), arr((rows, d), BF16), arr((2 * d // 128, 128)), arr((1, d)), arr((1, d)), arr((d, f)), arr((nqd, d))],
        in_specs=[ANY] * 15, out_specs=[ANY] * 7,
        scratch_shapes=[vb(seq, d), vb(seq, f), vb(seq, nqd), vb(seq, d), vf(rows, d), vf(rows + half, d), vb(rows, d), vb(rows, d), vf(1, d),
                        vf(half, d), vb(half, d), vb(rows, d), vf(2 * d // 128, 128), vf(1, d), vf(1, d),
                        vf(SLOTS, TILE, d), pltpu.SemaphoreType.DMA((14,)), pltpu.SemaphoreType.DMA((5,)), pltpu.SemaphoreType.DMA((SLOTS, 3))],
        compiler_params=pltpu.CompilerParams(vmem_limit_bytes=VMEM_LIMIT),
        cost_estimate=cost(2 * seq * d * (f + nqd), 4 * d * (f + nqd)),
        name="grads_second",
    )(order, h2, du, ctx, dx1, hkeep, recv, x, dmid, g1, dg2, db2, ykeep, mid, y)


def layer_step(x, dy, positions, g1, b1, g2, b2, wq, wk, wv, wo, w1, w2, head_dim, n_tp):
    rows, batch, d = x.shape
    seq = positions.shape[0]
    nq, nk, f = wq.shape[1] // head_dim, wk.shape[1] // head_dim, w1.shape[1]
    dims = (seq, d, head_dim, nq, nk, f, rows)
    rot = head_dim // 4
    freq = np.zeros((1, head_dim), np.float32)
    freq[0, :2 * rot] = np.tile(ROPE_BASE ** (-np.arange(rot) / rot), 2)
    x2, dy2 = x.reshape(rows, d), dy.reshape(rows, d)
    g1, b1, g2, b2 = (v.reshape(1, d) for v in (g1, b1, g2, b2))
    (h1, h2, dyf, dx1, act, du, ctx, dqkv, y, mid, dmid, send, hkeep, ykeep, dg2, db2) = chain(
        dims, x2, dy2, positions.reshape(1, seq), jnp.asarray(freq), g1, b1, g2, b2, wq, wk, wv, wo, w1, w2)

    def swap(v, bit):
        return lax.ppermute(v, 'tp', [(i, i ^ bit) for i in range(n_tp)])

    recv = swap(send, 3)
    dw2, dwq, dwk, dwv = grads_first(dims, act, dyf, h1, dqkv)
    y, dx, lng, dg2, db2, dw1, dwo = grads_second(dims, dw2, h2, du, ctx, dx1, hkeep, recv, x2, dmid, g1, dg2, db2, ykeep, mid, y)
    others = [swap(lng, bit) for bit in (1, 2, 3)]
    half = lng.shape[0] // 2
    sums = [((lng[at] + others[0][at]) + (others[1][at] + others[2][at])).reshape(d) for at in (slice(0, half), slice(half, None))]
    return (y.reshape(x.shape), dx.reshape(x.shape), sums[0], sums[1], dg2.reshape(d), db2.reshape(d), dwq, dwk, dwv, dwo, dw1, dw2)


def solution(mesh):
    seq_spec = P(('dp', 'tp'))
    col_spec = P(None, 'tp')
    row_spec = P('tp', None)
    grad_col_spec = P('dp', 'tp')
    grad_row_spec = P(('dp', 'tp'), None)
    in_specs = (seq_spec, seq_spec, P('dp'), P(), P(), P(), P(), col_spec, col_spec, col_spec, row_spec, col_spec, row_spec)
    out_specs = (seq_spec, seq_spec, P('dp'), P('dp'), P('dp'), P('dp'), grad_col_spec, grad_col_spec, grad_col_spec, grad_row_spec, grad_col_spec, grad_row_spec)

    def run_layer(resid_in, grad_out, positions, ln1_gain, ln1_bias, ln2_gain, ln2_bias, w_query, w_key, w_value, w_out, w_up, w_down):
        step_fn = functools.partial(layer_step, head_dim=w_key.shape[1] // KV_HEADS, n_tp=mesh.shape['tp'])
        sharded = jax.shard_map(step_fn, mesh=mesh, in_specs=in_specs, out_specs=out_specs, check_vma=False)
        return sharded(resid_in, grad_out, positions, ln1_gain, ln1_bias, ln2_gain, ln2_bias, w_query, w_key, w_value, w_out, w_up, w_down)

    return run_layer
```

```python
import functools
import math
import numpy as np
import jax
import jax.numpy as jnp
from jax import lax
from jax.experimental import pallas as pl
from jax.experimental.pallas import tpu as pltpu
from jax.sharding import PartitionSpec as P

KV_HEADS = 8
LN_EPS = 1e-5
ROPE_BASE = 10000.0
F32 = jnp.float32
BF16 = jnp.bfloat16
ANY = pl.BlockSpec(memory_space=pl.ANY)
VMEM = pl.BlockSpec(memory_space=pltpu.VMEM)
VMEM_LIMIT = 67_043_328


def mm(a, b):
    return jnp.dot(a, b, preferred_element_type=F32)


def mm_bt(a, b):
    return lax.dot_general(a, b, (((1,), (1,)), ((), ())), preferred_element_type=F32)


def mm_at(a, b):
    return lax.dot_general(a, b, (((0,), (0,)), ((), ())), preferred_element_type=F32)


def centre(rows):
    centred = rows - jnp.mean(rows, axis=-1, keepdims=True)
    scale = lax.rsqrt(jnp.mean(centred * centred, axis=-1, keepdims=True) + LN_EPS)
    return centred * scale, scale


def norm_rows(rows, gain, bias):
    normed, _ = centre(rows)
    return normed * (1.0 + gain) + bias


def norm_rows_back(rows, grad, gain):
    return norm_back(*centre(rows), grad, gain)


def norm_back(normed, scale, grad, gain):
    weighted = grad * (1.0 + gain)
    inner = jnp.mean(weighted * normed, axis=-1, keepdims=True)
    grad_rows = scale * (weighted - jnp.mean(weighted, axis=-1, keepdims=True) - normed * inner)
    return grad_rows, jnp.sum(grad * normed, axis=0, keepdims=True), jnp.sum(grad, axis=0, keepdims=True)


class Sems:
    def __init__(self):
        self.next = 0

    def take(self, count):
        base = self.next
        self.next += count
        return base


def chain_kernel(dims, x_hbm, dy_hbm, pos_hbm, freq_hbm, g1_hbm, b1_hbm, g2_hbm, b2_hbm, wq_hbm, wk_hbm, wv_hbm, wo_hbm, w1_hbm, w2_hbm,
                 h1_out, h2_out, dy_out, dx1_out, act_out, du_out, ctx_out, dqkv_out, y_out, mid_out, dmid_out, send_out, hkeep_out, ykeep_out, dg2_out, db2_out,
                 pos_ref, freq_ref, g1_ref, b1_ref, g2_ref, b2_ref,
                 wqkv, wo, w1, w2, h1, h2, dyf, dx1, x_own, mid, y_own, tmat, act, du, qs, kv, ctx, prob, cosb, sinb, gcs, dqkv, lng,
                 part_a, part_b, part_c, dr_a, dr_b, dr_c, dr_d, snd_a, snd_b, snd_c, lnk_a, lnk_b, lnk_c, send, hkeep, ykeep, lng_in, lng_chip, dg2, db2,
                 local_sem, out_sem, send_sem, recv_sem):
    seq, d, hd, nq, nk, f, rows = dims
    grp = nq // nk
    half = rows // 2
    me = lax.axis_index("tp")
    part, peer, diag = me ^ 1, me ^ 3, me ^ 2
    sems = Sems()

    def block(idx, sub=None):
        if sub is None:
            return pl.ds(pl.multiple_of(idx * rows, rows), rows)
        return pl.ds(pl.multiple_of(idx * rows + sub * half, half), half)

    def remote(src, dst, sem, dev):
        return pltpu.make_async_remote_copy(src, dst, send_sem.at[sem], recv_sem.at[sem], device_id={"tp": dev})

    def local(src, dst, idx):
        return pltpu.make_async_copy(src, dst, local_sem.at[idx])

    x_in = local(x_hbm, x_own, 0)
    dy_in = local(dy_hbm, dyf.at[block(me)], 1)
    nqd, nkd = nq * hd, nk * hd
    weight_in = [
        local(wq_hbm, wqkv.at[:, pl.ds(0, nqd)], 2),
        local(wk_hbm, wqkv.at[:, pl.ds(nqd, nkd)], 3),
        local(wv_hbm, wqkv.at[:, pl.ds(nqd + nkd, nkd)], 4),
        local(wo_hbm, wo, 5),
        local(w2_hbm, w2, 6),
        local(w1_hbm, w1, 7),
    ]
    small_in = [local(src, dst, 8 + i) for i, (src, dst) in enumerate((
        (g1_hbm, g1_ref), (b1_hbm, b1_ref), (pos_hbm, pos_ref), (freq_hbm, freq_ref), (g2_hbm, g2_ref), (b2_hbm, b2_ref)))]
    x_in.start()
    for copy in small_in:
        copy.start()
    dy_in.start()
    barrier = pltpu.get_barrier_semaphore()
    for dev in (part, peer):
        pl.semaphore_signal(barrier, inc=1, device_id={"tp": dev})
    for copy in weight_in:
        copy.start()

    outs = []

    def put(src, dst):
        copy = pltpu.make_async_copy(src, dst, out_sem.at[len(outs)])
        copy.start()
        outs.append(copy)

    class Gather:
        def __init__(self, buf, pieces):
            self.buf, self.pieces, self.base = buf, pieces, sems.take(3 * len(pieces))

        def copy(self, kind, i):
            owner = (me, me, peer)[kind]
            dev = (peer, part, part)[kind]
            row, n_rows, col, n_cols = self.pieces[i]
            at = self.buf.at[pl.ds(pl.multiple_of(owner * rows + row, half), n_rows), pl.ds(col, n_cols)]
            return remote(at, at, self.base + len(self.pieces) * kind + i, dev)

        def send(self, i):
            self.copy(0, i).start()
            self.copy(1, i).start()

        def forward(self, i):
            self.copy(0, i).wait_recv()
            self.copy(2, i).start()

        def finish(self, i):
            self.copy(1, i).wait_recv()
            self.copy(2, i).wait_recv()

        def feed(self, first, use):
            count = len(self.pieces)
            for i in range(first):
                self.forward(i)
            self.forward(first)
            for i in range(first):
                self.finish(i)
            for i in range(first, count):
                if i + 1 < count:
                    self.forward(i + 1)
                self.finish(i)
                use(i - first, pl.ds(self.pieces[i][2], self.pieces[i][3]))

    class Scatter:
        def __init__(self, chunks, partial, from_part, summed, from_peer=None, link_rows=0, early=0):
            self.chunks, self.cw, self.link_rows, self.early = chunks, d // chunks, link_rows, early
            self.partial, self.from_part, self.summed, self.from_peer = partial, from_part, summed, from_peer
            self.base = sems.take(2 * chunks)
            self.link = sems.take(chunks + 1 + early) if link_rows else None

        def cols(self, i):
            return pl.ds(pl.multiple_of(i * self.cw, self.cw), self.cw)

        def pair(self, i, kind):
            owner = (diag, part)[kind]
            return remote(self.partial.at[block(owner), self.cols(i)], self.from_part.at[kind, :, self.cols(i)], self.base + self.chunks * kind + i, part)

        def first(self, i):
            top = pl.ds(0, half)
            return remote(self.summed.at[top, self.cols(i)], self.from_peer.at[top, self.cols(i)], self.link + i, peer)

        def second(self):
            at = (pl.ds(half, half), pl.ds(self.early * self.cw, d - self.early * self.cw))
            return remote(self.summed.at[at], self.from_peer.at[at], self.link + self.chunks, peer)

        def ahead(self, i):
            at = (pl.ds(half, half), self.cols(i))
            return remote(self.summed.at[at], self.from_peer.at[at], self.link + self.chunks + 1 + i, peer)

        def chip_sum(self, i):
            self.pair(i, 0).wait_recv()
            cols = self.cols(i)
            self.summed[:, cols] = self.partial[block(peer), cols] + self.from_part[0, :, cols]
            if self.link_rows:
                self.first(i).start()
            if self.early:
                @pl.when(i < self.early)
                def _():
                    self.ahead(i).start()

        def run(self, chunk, lag=0):
            def step(i, carry):
                self.partial[:, self.cols(i)] = chunk(self.cols(i))
                self.pair(i, 0).start()
                self.pair(i, 1).start()
                if lag:
                    @pl.when(i >= lag)
                    def _():
                        self.chip_sum(i - lag)
                return carry

            lax.fori_loop(0, self.chunks, step, 0)
            if lag:
                self.drain(self.chunks - lag)

        def drain(self, start=0):
            for i in range(start, self.chunks):
                self.chip_sum(i)
            if self.link_rows == rows:
                self.second().start()

        def kept(self):
            for i in range(self.chunks):
                self.pair(i, 1).wait_recv()

        def kept_rows(self, sub):
            return self.partial[block(me, sub), :] + self.from_part[1, pl.ds(sub * half, half), :]

        def rows_sum(self, sub):
            if sub == 0:
                for i in range(self.chunks):
                    self.first(i).wait_recv()
            else:
                for i in range(self.early):
                    self.ahead(i).wait_recv()
                self.second().wait_recv()
            return self.kept_rows(sub) + self.from_peer[pl.ds(sub * half, half), :]

        def pair_sent(self):
            for i in range(self.chunks):
                self.pair(i, 0).wait_send()
                self.pair(i, 1).wait_send()

        def link_sent(self):
            if self.link_rows:
                for i in range(self.chunks):
                    self.first(i).wait_send()
            if self.link_rows == rows:
                self.second().wait_send()
            for i in range(self.early):
                self.ahead(i).wait_send()

    x_in.wait()
    small_in[0].wait()
    small_in[1].wait()
    h1[block(me), :] = norm_rows(x_own[...].astype(F32), g1_ref[...], b1_ref[...]).astype(BF16)
    pl.semaphore_wait(barrier, 2)
    gather_h1 = Gather(h1, [(0, rows) + cut for cut in cuts(d, (4, 3, 3, 2))])
    gather_dy = Gather(dyf, [(0, rows, 0, d)])
    late = [(0, half, 0, d)] + [(half, half) + cut for cut in cuts(d, (1, 1))]
    for i in range(len(gather_h1.pieces)):
        gather_h1.send(i)
    dy_in.wait()
    gather_dy.send(0)

    small_in[2].wait()
    small_in[3].wait()
    pos_rows = jnp.broadcast_to(pos_ref[...].astype(F32), (hd, seq)).T
    angles = pos_rows * freq_ref[...]
    lane = lax.broadcasted_iota(jnp.int32, (seq, hd), 1)
    rot = hd // 4
    cosb[...] = jnp.cos(angles)
    sinb[...] = jnp.where(lane < rot, -1.0, 1.0) * jnp.sin(angles)

    def turn(v, sign):
        other = jnp.where(lane < rot, pltpu.roll(v, hd - rot, 1), pltpu.roll(v, rot, 1))
        other = jnp.where(lane < 2 * rot, other, 0.0)
        return v * cosb[...] + (sign * sinb[...]) * other

    for copy in weight_in[:3]:
        copy.wait()
    n_all = nqd + 2 * nkd

    def add(total, j, piece):
        total[...] = piece if j == 0 else total[...] + piece

    qkv_sum = part_c.at[:, pl.ds(0, n_all)]
    gather_h1.feed(0, lambda j, cols: add(qkv_sum, j, mm(h1[:, cols], wqkv[cols, :])))

    qkv = qkv_sum
    for k in range(nk):
        for g in range(grp):
            lo = (k * grp + g) * hd
            head = qkv[:, lo:lo + hd].astype(BF16).astype(F32)
            qs[k, g * seq:(g + 1) * seq, :] = turn(head, 1.0).astype(BF16)
        lo = nqd + k * hd
        kv[0, k] = turn(qkv[:, lo:lo + hd].astype(BF16).astype(F32), 1.0).astype(BF16)
        lo = nqd + nkd + k * hd
        kv[1, k] = qkv[:, lo:lo + hd].astype(BF16)
    put(h1, h1_out)
    query = lax.rem(lax.broadcasted_iota(jnp.int32, (grp * seq, seq), 0), seq)
    causal = query >= lax.broadcasted_iota(jnp.int32, (grp * seq, seq), 1)
    for k in range(nk):
        scores = jnp.where(causal, mm_bt(qs[k], kv[0, k]) * hd ** -0.5, -1e30)
        exped = jnp.exp(scores - jnp.max(scores, axis=-1, keepdims=True))
        prob[k] = exped / jnp.sum(exped, axis=-1, keepdims=True)
        head_ctx = mm(prob[k].astype(BF16), kv[1, k]).astype(BF16)
        for g in range(grp):
            lo = (k * grp + g) * hd
            ctx[:, lo:lo + hd] = head_ctx[g * seq:(g + 1) * seq, :]
    put(ctx, ctx_out)
    weight_in[3].wait()
    sum_attn = Scatter(6, part_a, dr_a, snd_a, lnk_a, rows)
    sum_attn.run(lambda cols: mm(ctx[...], wo[:, cols]), lag=2)

    gather_dy.forward(0)
    gather_dy.finish(0)
    weight_in[4].wait()
    put(dyf, dy_out)
    nb = f // 2

    def down_back(j, carry):
        cols = pl.ds(pl.multiple_of(j * nb, nb), nb)
        tmat[:, cols] = mm_bt(dyf[...], w2[cols, :])
        return carry

    lax.fori_loop(0, f // nb, down_back, 0)

    gather_h2 = Gather(h2, late)
    small_in[4].wait()
    small_in[5].wait()
    for sub in (0, 1):
        if sub == 0:
            sum_attn.kept()
        own = pl.ds(sub * half, half)
        attn_rows = sum_attn.rows_sum(sub).astype(BF16)
        mid_rows = (x_own[own, :].astype(F32) + attn_rows.astype(F32)).astype(BF16)
        mid[own, :] = mid_rows
        h2[block(me, sub), :] = norm_rows(mid_rows.astype(F32), g2_ref[...], b2_ref[...]).astype(BF16)
        for i in ((0,) if sub == 0 else range(1, len(late))):
            gather_h2.send(i)
    weight_in[5].wait()

    def up(j, depth):
        cols = pl.ds(0, f)
        piece = mm(h2[:, depth], w1[depth, :])
        if j == 0:
            part_c[:, cols] = piece
        elif j < len(late) - 2:
            part_c[:, cols] += piece
        else:
            relu_up = jnp.maximum((part_c[:, cols] + piece).astype(BF16).astype(F32), 0.0)
            act[...] = (relu_up * relu_up).astype(BF16)
            du[...] = (tmat[...] * (2.0 * relu_up)).astype(BF16)

    gather_h2.feed(1, up)
    put(h2, h2_out)
    put(act, act_out)
    put(du, du_out)
    sum_dh2 = Scatter(12, part_b, dr_b, snd_b, lnk_b, rows, 4)
    sum_dh2.run(lambda cols: mm_bt(du[...], w1[cols, :]), lag=2)

    sum_mlp = Scatter(4, part_c, dr_c, snd_c, lnk_c, half)
    sum_mlp.run(lambda cols: mm(act[...], w2[:, cols]))

    gather_dx1 = Gather(dx1, late)
    normed2, scale2 = centre(mid[...].astype(F32))
    for sub in (0, 1):
        if sub == 0:
            sum_dh2.kept()
        dh2_rows = sum_dh2.rows_sum(sub).astype(BF16).astype(F32)
        own = slice(sub * half, (sub + 1) * half)
        grad_rows, grad_gain, grad_bias = norm_back(normed2[own], scale2[own], dh2_rows, g2_ref[...])
        dx1[block(me, sub), :] = (dyf[block(me, sub), :].astype(F32) + grad_rows).astype(BF16)
        for i in ((0,) if sub == 0 else range(1, len(late))):
            gather_dx1.send(i)
        if sub == 0:
            lng[0:1, :] = grad_gain
            lng[1:2, :] = grad_bias
        else:
            lng[0:1, :] += grad_gain
            lng[1:2, :] += grad_bias
    put(dx1.at[block(me)], dmid_out)
    lng_base = sems.take(2)
    lng_pair = remote(lng, lng_in.at[0], lng_base, part)
    lng_pair.start()
    sum_mlp.drain()
    low = pl.ds(half, half)
    send[pl.ds(rows, half), :] = snd_c[low, :]
    sum_mlp.kept()
    ykeep[...] = sum_mlp.kept_rows(1)
    put(ykeep, ykeep_out)
    put(mid.at[low], mid_out)
    lng_pair.wait_recv()
    lng_chip[...] = lng[...] + lng_in[0]
    lng_link = remote(lng_chip, lng_in.at[1], lng_base + 1, peer)
    lng_link.start()
    dctx_sum = tmat.at[:, pl.ds(0, nqd)]
    gather_dx1.feed(1, lambda j, cols: add(dctx_sum, j, mm_bt(dx1[:, cols], wo[:, cols])))
    put(dx1, dx1_out)

    dctx = dctx_sum[...].astype(BF16)
    for k in range(nk):
        for g in range(grp):
            lo = (k * grp + g) * hd
            gcs[k, g * seq:(g + 1) * seq, :] = dctx[:, lo:lo + hd]
    for k in range(nk):
        grad_v = mm_at(prob[k].astype(BF16), gcs[k]).astype(BF16)
        grad_p = mm_bt(gcs[k], kv[1, k])
        grad_s = (prob[k] * (grad_p - jnp.sum(grad_p * prob[k], axis=-1, keepdims=True)) * hd ** -0.5).astype(BF16)
        grad_q = mm(grad_s, kv[0, k])
        for g in range(grp):
            lo = (k * grp + g) * hd
            dqkv[:, lo:lo + hd] = turn(grad_q[g * seq:(g + 1) * seq, :], -1.0).astype(BF16)
        lo = nqd + k * hd
        dqkv[:, lo:lo + hd] = turn(mm_at(grad_s, qs[k]), -1.0).astype(BF16)
        lo = nqd + nkd + k * hd
        dqkv[:, lo:lo + hd] = grad_v
    put(dqkv, dqkv_out)
    sum_dh1 = Scatter(2, part_a, dr_d, send.at[pl.ds(0, rows)])
    sum_attn.pair_sent()
    sum_dh1.run(lambda cols: mm_bt(dqkv[...], wqkv[cols, :]))
    sum_dh1.drain()
    put(send, send_out)
    sum_dh1.kept()
    for sub in (0, 1):
        hkeep[pl.ds(sub * half, half), :] = sum_dh1.kept_rows(sub)
    put(hkeep, hkeep_out)
    top = pl.ds(0, half)
    y_own[...] = (mid[top, :].astype(F32) + sum_mlp.rows_sum(0).astype(BF16).astype(F32)).astype(BF16)
    put(y_own, y_out)
    lng_link.wait_recv()
    dg2[...] = lng_chip[0:1, :] + lng_in[1, 0:1, :]
    db2[...] = lng_chip[1:2, :] + lng_in[1, 1:2, :]
    put(dg2, dg2_out)
    put(db2, db2_out)

    for gather in (gather_h1, gather_dy, gather_h2, gather_dx1):
        for kind in (0, 1, 2):
            for i in range(len(gather.pieces)):
                gather.copy(kind, i).wait_send()
    for scatter in (sum_dh2, sum_mlp, sum_dh1):
        scatter.pair_sent()
    for scatter in (sum_attn, sum_dh2, sum_mlp):
        scatter.link_sent()
    lng_pair.wait_send()
    lng_link.wait_send()
    for copy in outs:
        copy.wait()


def cuts(d, parts):
    unit, first, out = d // sum(parts), 0, []
    for n in parts:
        out.append((first, n * unit))
        first += n * unit
    return out


def chain(dims, x, dy, pos, freq, g1, b1, g2, b2, wq, wk, wv, wo, w1, w2):
    seq, d, hd, nq, nk, f, rows = dims
    grp = nq // nk
    nqd, nkd = nq * hd, nk * hd
    n_all = nqd + 2 * nkd
    half = rows // 2

    def arr(shape, dtype):
        return jax.ShapeDtypeStruct(shape, dtype)

    def vm(*shape, dtype=BF16):
        return pltpu.VMEM(shape, dtype)

    def vf(*shape):
        return pltpu.VMEM(shape, F32)

    out_shape = [arr((seq, d), BF16)] * 4 + [arr((seq, f), BF16)] * 2 + [arr((seq, nqd), BF16), arr((seq, n_all), BF16)] + [arr((half, d), BF16)] * 2 + [arr((rows, d), BF16), arr((rows + half, d), F32), arr((rows, d), F32), arr((half, d), F32)] + [arr((1, d), F32)] * 2
    n_sems = 3 * (4 + 1 + 3 + 3) + 2 * (6 + 12 + 4 + 2) + (7 + 17 + 5) + 2
    scratch = [
        pltpu.VMEM((1, seq), jnp.int32), vf(1, hd), vf(1, d), vf(1, d), vf(1, d), vf(1, d),
        vm(d, n_all), vm(nqd, d), vm(d, f), vm(f, d),
        vm(seq, d), vm(seq, d), vm(seq, d), vm(seq, d),
        vm(rows, d), vm(rows, d), vm(half, d), vf(seq, f), vm(seq, f), vm(seq, f),
        vm(nk, grp * seq, hd), vm(2, nk, seq, hd), vm(seq, nqd), vf(nk, grp * seq, seq),
        vf(seq, hd), vf(seq, hd), vm(nk, grp * seq, hd), vm(seq, n_all), vf(2, d),
        vf(seq, d), vf(seq, d), vf(seq, d),
        vf(2, rows, d), vf(2, rows, d), vf(2, rows, d), vf(2, rows, d),
        vf(rows, d), vf(rows, d), vf(rows, d), vf(rows, d), vf(rows, d), vf(half, d),
        vf(rows + half, d), vf(rows, d), vf(half, d), vf(2, 2, d), vf(2, d), vf(1, d), vf(1, d),
        pltpu.SemaphoreType.DMA((14,)), pltpu.SemaphoreType.DMA((len(out_shape),)),
        pltpu.SemaphoreType.DMA((n_sems,)), pltpu.SemaphoreType.DMA((n_sems,)),
    ]
    return pl.pallas_call(
        functools.partial(chain_kernel, dims),
        out_shape=out_shape,
        in_specs=[ANY] * 14,
        out_specs=[ANY] * len(out_shape),
        scratch_shapes=scratch,
        compiler_params=pltpu.CompilerParams(collective_id=0, has_side_effects=True, vmem_limit_bytes=VMEM_LIMIT),
        name="chain",
    )(x, dy, pos, freq, g1, b1, g2, b2, wq, wk, wv, wo, w1, w2)


SLOTS = 4
TILE = 256


def stream_grads(jobs, stage, sem):
    def copies(job, i, slot):
        return [pltpu.make_async_copy(stage.at[slot, pl.ds(0, job[1]), pl.ds(lo, n)], dst, sem.at[slot, c]) for c, (dst, lo, n) in enumerate(job[5](i))]

    done, pending = 0, []
    for job in jobs:
        ready, tile, tiles, width, compute, targets = job
        ready()

        def fill(i, slot):
            stage[slot, :tile, :width] = compute(i)
            for copy in copies(job, i, slot):
                copy.start()

        lead = min(SLOTS, tiles)
        for i in range(lead):
            slot = (done + i) % SLOTS
            if len(pending) == SLOTS:
                for copy in pending.pop(0):
                    copy.wait()
            fill(i, slot)
            pending.append(copies(job, i, slot))

        def step(i, carry, base=done):
            slot = lax.rem(base + i, SLOTS)
            for copy in copies(job, i - SLOTS, slot):
                copy.wait()
            fill(i, slot)
            return carry

        lax.fori_loop(lead, tiles, step, 0)
        if tiles > SLOTS:
            pending = [copies(job, i, (done + i) % SLOTS) for i in range(tiles - SLOTS, tiles)]
        done += tiles
    for group in pending:
        for copy in group:
            copy.wait()


def tile_at(i, tile, first=0):
    return pl.ds(pl.multiple_of(first + i * tile, tile), tile)


def outer_jobs(ready, left, right, targets, total, lead=0):
    jobs = []
    width = right.shape[1]
    if lead:
        small = TILE // 2
        jobs.append((ready, small, lead // small, width, lambda i: mm_at(left[:, tile_at(i, small)], right[...]), lambda i: targets(tile_at(i, small))))
        ready = lambda: None
    jobs.append((ready, TILE, (total - lead) // TILE, width, lambda i: mm_at(left[:, tile_at(i, TILE, lead)], right[...]), lambda i: targets(tile_at(i, TILE, lead))))
    return jobs


def start_loads(pairs, sem):
    loads = [pltpu.make_async_copy(src, dst, sem.at[i]) for i, (src, dst) in enumerate(pairs)]
    for copy in loads:
        copy.start()

    def ready(*which):
        def wait():
            for i in which:
                loads[i].wait()

        return wait

    return ready


def grads_first_kernel(dims, act_hbm, dy_hbm, h1_hbm, dqkv_hbm, dw2, dwq, dwk, dwv, act, dyf, h1, dqkv, stage, in_sem, sem):
    seq, d, hd, nq, nk, f, rows = dims
    nqd, nkd = nq * hd, nk * hd
    ready = start_loads(((act_hbm, act), (dy_hbm, dyf), (h1_hbm, h1), (dqkv_hbm, dqkv)), in_sem)
    stream_grads(
        outer_jobs(ready(0, 1), act, dyf, lambda at: [(dw2.at[at], 0, d)], f, TILE)
        + outer_jobs(ready(2, 3), h1, dqkv, lambda at: [(dwq.at[at], 0, nqd), (dwk.at[at], nqd, nkd), (dwv.at[at], nqd + nkd, nkd)], d),
        stage, sem)


def grads_second_kernel(dims, order, h2_hbm, du_hbm, hkeep_hbm, recv_hbm, x_hbm, dmid_hbm, g1_hbm, dg2_hbm, db2_hbm, ykeep_hbm, mid_hbm, y_hbm,
                        y_out, dx_out, lng_out, dg2_out, db2_out, dw1,
                        h2, du, hkeep, recv, x, dmid, g1, ykeep, mid, y, lng, dg2, db2, stage, in_sem, end_sem, sem):
    seq, d, hd, nq, nk, f, rows = dims
    half = rows // 2
    top, low = pl.ds(0, half), pl.ds(half, half)
    ready = start_loads(((h2_hbm, h2), (du_hbm, du), (hkeep_hbm, hkeep), (recv_hbm, recv), (x_hbm, x), (dmid_hbm, dmid), (g1_hbm, g1),
                         (dg2_hbm, dg2), (db2_hbm, db2), (ykeep_hbm, ykeep), (mid_hbm, mid), (y_hbm, y.at[top])), in_sem)
    ends = [pltpu.make_async_copy(src, dst, end_sem.at[i]) for i, (src, dst) in enumerate(((y, y_out), (dmid, dx_out), (lng, lng_out), (dg2, dg2_out), (db2, db2_out)))]

    def first_norm_back():
        ready(2, 3, 4, 5, 6, 7, 8, 9, 10, 11)()
        dh1 = (hkeep[...] + recv[pl.ds(0, rows), :]).astype(BF16).astype(F32)
        grad_rows, grad_gain, grad_bias = norm_rows_back(x[...].astype(F32), dh1, g1[...])
        dmid[...] = (dmid[...].astype(F32) + grad_rows).astype(BF16)
        lanes = lng.shape[1]
        for i, total in enumerate((grad_gain, grad_bias)):
            for j in range(d // lanes):
                at = i * (d // lanes) + j
                lng[at:at + 1, :] = total[:, j * lanes:(j + 1) * lanes]
        mlp = (ykeep[...] + recv[pl.ds(rows, half), :]).astype(BF16)
        y[low, :] = (mid[...].astype(F32) + mlp.astype(F32)).astype(BF16)
        for copy in ends:
            copy.start()

    def dw1_jobs(after, first, total):
        at = functools.partial(tile_at, tile=TILE, first=first)
        return [(after, TILE, total // TILE, f, lambda i: mm_at(h2[:, at(i)], du[...]), lambda i: [(dw1.at[at(i)], 0, f)])]

    lead = SLOTS * TILE
    stream_grads(
        dw1_jobs(ready(0, 1), 0, lead) + dw1_jobs(first_norm_back, lead, d - lead),
        stage, sem)
    for copy in ends:
        copy.wait()


def grads_third_kernel(order, ctx_hbm, dx1_hbm, dwo, ctx, dx1, stage, in_sem, sem):
    ready = start_loads(((ctx_hbm, ctx), (dx1_hbm, dx1)), in_sem)
    stream_grads(outer_jobs(ready(0, 1), ctx, dx1, lambda at: [(dwo.at[at], 0, dx1.shape[1])], ctx.shape[1], TILE), stage, sem)


def cost(flops, nbytes):
    return pl.CostEstimate(flops=flops, bytes_accessed=nbytes, transcendentals=0)


def arr(shape, dtype=F32):
    return jax.ShapeDtypeStruct(shape, dtype)


def grads_first(dims, act, dyf, h1, dqkv):
    seq, d, hd, nq, nk, f, rows = dims
    nqd, nkd = nq * hd, nk * hd
    n_all = nqd + 2 * nkd
    return pl.pallas_call(
        functools.partial(grads_first_kernel, dims),
        out_shape=[arr((f, d)), arr((d, nqd)), arr((d, nkd)), arr((d, nkd))],
        in_specs=[ANY] * 4, out_specs=[ANY] * 4,
        scratch_shapes=[pltpu.VMEM((seq, f), BF16), pltpu.VMEM((seq, d), BF16), pltpu.VMEM((seq, d), BF16), pltpu.VMEM((seq, n_all), BF16),
                        pltpu.VMEM((SLOTS, TILE, d), F32), pltpu.SemaphoreType.DMA((4,)), pltpu.SemaphoreType.DMA((SLOTS, 3))],
        compiler_params=pltpu.CompilerParams(vmem_limit_bytes=VMEM_LIMIT),
        cost_estimate=cost(2 * seq * d * (f + n_all), 4 * d * (f + n_all)),
        name="grads_first",
    )(act, dyf, h1, dqkv)


def grads_second(dims, order, h2, du, hkeep, recv, x, dmid, g1, dg2, db2, ykeep, mid, y):
    seq, d, hd, nq, nk, f, rows = dims
    half = rows // 2

    def vb(*shape):
        return pltpu.VMEM(shape, BF16)

    def vf(*shape):
        return pltpu.VMEM(shape, F32)

    return pl.pallas_call(
        functools.partial(grads_second_kernel, dims),
        out_shape=[arr((rows, d), BF16), arr((rows, d), BF16), arr((2 * d // 128, 128)), arr((1, d)), arr((1, d)), arr((d, f))],
        in_specs=[ANY] * 13, out_specs=[ANY] * 6,
        scratch_shapes=[vb(seq, d), vb(seq, f), vf(rows, d), vf(rows + half, d), vb(rows, d), vb(rows, d), vf(1, d),
                        vf(half, d), vb(half, d), vb(rows, d), vf(2 * d // 128, 128), vf(1, d), vf(1, d),
                        vf(SLOTS, TILE, f), pltpu.SemaphoreType.DMA((12,)), pltpu.SemaphoreType.DMA((5,)), pltpu.SemaphoreType.DMA((SLOTS, 3))],
        compiler_params=pltpu.CompilerParams(vmem_limit_bytes=VMEM_LIMIT),
        cost_estimate=cost(2 * seq * d * f, 4 * d * f),
        name="grads_second",
    )(order, h2, du, hkeep, recv, x, dmid, g1, dg2, db2, ykeep, mid, y)


def grads_third(dims, order, ctx, dx1):
    seq, d, hd, nq, nk, f, rows = dims
    nqd = nq * hd
    return pl.pallas_call(
        grads_third_kernel,
        out_shape=arr((nqd, d)),
        in_specs=[ANY] * 3, out_specs=ANY,
        scratch_shapes=[pltpu.VMEM((seq, nqd), BF16), pltpu.VMEM((seq, d), BF16), pltpu.VMEM((SLOTS, TILE, d), F32),
                        pltpu.SemaphoreType.DMA((2,)), pltpu.SemaphoreType.DMA((SLOTS, 3))],
        compiler_params=pltpu.CompilerParams(vmem_limit_bytes=VMEM_LIMIT),
        cost_estimate=cost(2 * seq * d * nqd, 4 * d * nqd),
        name="grads_third",
    )(order, ctx, dx1)


def layer_step(x, dy, positions, g1, b1, g2, b2, wq, wk, wv, wo, w1, w2, head_dim, n_tp):
    rows, batch, d = x.shape
    seq = positions.shape[0]
    nq, nk, f = wq.shape[1] // head_dim, wk.shape[1] // head_dim, w1.shape[1]
    dims = (seq, d, head_dim, nq, nk, f, rows)
    rot = head_dim // 4
    freq = np.zeros((1, head_dim), np.float32)
    freq[0, :2 * rot] = np.tile(ROPE_BASE ** (-np.arange(rot) / rot), 2)
    x2, dy2 = x.reshape(rows, d), dy.reshape(rows, d)
    g1, b1, g2, b2 = (v.reshape(1, d) for v in (g1, b1, g2, b2))
    (h1, h2, dyf, dx1, act, du, ctx, dqkv, y, mid, dmid, send, hkeep, ykeep, dg2, db2) = chain(
        dims, x2, dy2, positions.reshape(1, seq), jnp.asarray(freq), g1, b1, g2, b2, wq, wk, wv, wo, w1, w2)

    def swap(v, bit):
        return lax.ppermute(v, 'tp', [(i, i ^ bit) for i in range(n_tp)])

    recv = swap(send, 3)
    dw2, dwq, dwk, dwv = grads_first(dims, act, dyf, h1, dqkv)
    y, dx, lng, dg2, db2, dw1 = grads_second(dims, dw2, h2, du, hkeep, recv, x2, dmid, g1, dg2, db2, ykeep, mid, y)
    others = [swap(lng, bit) for bit in (1, 2, 3)]
    dwo = grads_third(dims, lng, ctx, dx1)
    half = lng.shape[0] // 2
    sums = [((lng[at] + others[0][at]) + (others[1][at] + others[2][at])).reshape(d) for at in (slice(0, half), slice(half, None))]
    return (y.reshape(x.shape), dx.reshape(x.shape), sums[0], sums[1], dg2.reshape(d), db2.reshape(d), dwq, dwk, dwv, dwo, dw1, dw2)


def solution(mesh):
    seq_spec = P(('dp', 'tp'))
    col_spec = P(None, 'tp')
    row_spec = P('tp', None)
    grad_col_spec = P('dp', 'tp')
    grad_row_spec = P(('dp', 'tp'), None)
    in_specs = (seq_spec, seq_spec, P('dp'), P(), P(), P(), P(), col_spec, col_spec, col_spec, row_spec, col_spec, row_spec)
    out_specs = (seq_spec, seq_spec, P('dp'), P('dp'), P('dp'), P('dp'), grad_col_spec, grad_col_spec, grad_col_spec, grad_row_spec, grad_col_spec, grad_row_spec)

    def run_layer(resid_in, grad_out, positions, ln1_gain, ln1_bias, ln2_gain, ln2_bias, w_query, w_key, w_value, w_out, w_up, w_down):
        step_fn = functools.partial(layer_step, head_dim=w_key.shape[1] // KV_HEADS, n_tp=mesh.shape['tp'])
        sharded = jax.shard_map(step_fn, mesh=mesh, in_specs=in_specs, out_specs=out_specs, check_vma=False)
        return sharded(resid_in, grad_out, positions, ln1_gain, ln1_bias, ln2_gain, ln2_bias, w_query, w_key, w_value, w_out, w_up, w_down)

    return run_layer
```

```python
import functools
import math
import numpy as np
import jax
import jax.numpy as jnp
from jax import lax
from jax.experimental import pallas as pl
from jax.experimental.pallas import tpu as pltpu
from jax.sharding import PartitionSpec as P

KV_HEADS = 8
LN_EPS = 1e-5
ROPE_BASE = 10000.0
F32 = jnp.float32
BF16 = jnp.bfloat16
ANY = pl.BlockSpec(memory_space=pl.ANY)
VMEM = pl.BlockSpec(memory_space=pltpu.VMEM)
VMEM_LIMIT = 67_043_328


def mm(a, b):
    return jnp.dot(a, b, preferred_element_type=F32)


def mm_bt(a, b):
    return lax.dot_general(a, b, (((1,), (1,)), ((), ())), preferred_element_type=F32)


def mm_at(a, b):
    return lax.dot_general(a, b, (((0,), (0,)), ((), ())), preferred_element_type=F32)


def centre(rows):
    centred = rows - jnp.mean(rows, axis=-1, keepdims=True)
    scale = lax.rsqrt(jnp.mean(centred * centred, axis=-1, keepdims=True) + LN_EPS)
    return centred * scale, scale


def norm_rows(rows, gain, bias):
    normed, _ = centre(rows)
    return normed * (1.0 + gain) + bias


def norm_rows_back(rows, grad, gain):
    return norm_back(*centre(rows), grad, gain)


def norm_back(normed, scale, grad, gain):
    weighted = grad * (1.0 + gain)
    inner = jnp.mean(weighted * normed, axis=-1, keepdims=True)
    grad_rows = scale * (weighted - jnp.mean(weighted, axis=-1, keepdims=True) - normed * inner)
    return grad_rows, jnp.sum(grad * normed, axis=0, keepdims=True), jnp.sum(grad, axis=0, keepdims=True)


class Sems:
    def __init__(self):
        self.next = 0

    def take(self, count):
        base = self.next
        self.next += count
        return base


def chain_kernel(dims, x_hbm, dy_hbm, pos_hbm, freq_hbm, g1_hbm, b1_hbm, g2_hbm, b2_hbm, wq_hbm, wk_hbm, wv_hbm, wo_hbm, w1_hbm, w2_hbm,
                 h1_out, h2_out, dy_out, dx1_out, act_out, du_out, ctx_out, dqkv_out, y_out, mid_out, dmid_out, send_out, hkeep_out, ykeep_out, dg2_out, db2_out,
                 pos_ref, freq_ref, g1_ref, b1_ref, g2_ref, b2_ref,
                 wqkv, wo, w1, w2, h1, h2, dyf, dx1, x_own, mid, y_own, tmat, act, du, qs, kv, ctx, prob, cosb, sinb, gcs, dqkv, lng,
                 part_a, part_b, part_c, dr_a, dr_b, dr_c, dr_d, snd_a, snd_b, snd_c, lnk_a, lnk_b, lnk_c, send, hkeep, ykeep, lng_in, lng_chip, dg2, db2,
                 local_sem, out_sem, send_sem, recv_sem):
    seq, d, hd, nq, nk, f, rows = dims
    grp = nq // nk
    half = rows // 2
    me = lax.axis_index("tp")
    part, peer, diag = me ^ 1, me ^ 3, me ^ 2
    sems = Sems()

    def block(idx, sub=None):
        if sub is None:
            return pl.ds(pl.multiple_of(idx * rows, rows), rows)
        return pl.ds(pl.multiple_of(idx * rows + sub * half, half), half)

    def remote(src, dst, sem, dev):
        return pltpu.make_async_remote_copy(src, dst, send_sem.at[sem], recv_sem.at[sem], device_id={"tp": dev})

    def local(src, dst, idx):
        return pltpu.make_async_copy(src, dst, local_sem.at[idx])

    x_in = local(x_hbm, x_own, 0)
    dy_in = local(dy_hbm, dyf.at[block(me)], 1)
    nqd, nkd = nq * hd, nk * hd
    weight_in = [
        local(wq_hbm, wqkv.at[:, pl.ds(0, nqd)], 2),
        local(wk_hbm, wqkv.at[:, pl.ds(nqd, nkd)], 3),
        local(wv_hbm, wqkv.at[:, pl.ds(nqd + nkd, nkd)], 4),
        local(wo_hbm, wo, 5),
        local(w2_hbm, w2, 6),
        local(w1_hbm, w1, 7),
    ]
    small_in = [local(src, dst, 8 + i) for i, (src, dst) in enumerate((
        (g1_hbm, g1_ref), (b1_hbm, b1_ref), (pos_hbm, pos_ref), (freq_hbm, freq_ref), (g2_hbm, g2_ref), (b2_hbm, b2_ref)))]
    x_in.start()
    for copy in small_in:
        copy.start()
    dy_in.start()
    barrier = pltpu.get_barrier_semaphore()
    for dev in (part, peer):
        pl.semaphore_signal(barrier, inc=1, device_id={"tp": dev})
    for copy in weight_in:
        copy.start()

    outs = []

    def put(src, dst):
        copy = pltpu.make_async_copy(src, dst, out_sem.at[len(outs)])
        copy.start()
        outs.append(copy)

    class Gather:
        def __init__(self, buf, pieces):
            self.buf, self.pieces, self.base = buf, pieces, sems.take(3 * len(pieces))

        def copy(self, kind, i):
            owner = (me, me, peer)[kind]
            dev = (peer, part, part)[kind]
            row, n_rows, col, n_cols = self.pieces[i]
            at = self.buf.at[pl.ds(pl.multiple_of(owner * rows + row, half), n_rows), pl.ds(col, n_cols)]
            return remote(at, at, self.base + len(self.pieces) * kind + i, dev)

        def send(self, i):
            self.copy(0, i).start()
            self.copy(1, i).start()

        def forward(self, i):
            self.copy(0, i).wait_recv()
            self.copy(2, i).start()

        def finish(self, i):
            self.copy(1, i).wait_recv()
            self.copy(2, i).wait_recv()

        def feed(self, first, use):
            count = len(self.pieces)
            for i in range(first):
                self.forward(i)
            self.forward(first)
            for i in range(first):
                self.finish(i)
            for i in range(first, count):
                if i + 1 < count:
                    self.forward(i + 1)
                self.finish(i)
                use(i - first, pl.ds(self.pieces[i][2], self.pieces[i][3]))

    class Scatter:
        def __init__(self, chunks, partial, from_part, summed, from_peer=None, link_rows=0, early=0):
            self.chunks, self.cw, self.link_rows, self.early = chunks, d // chunks, link_rows, early
            self.partial, self.from_part, self.summed, self.from_peer = partial, from_part, summed, from_peer
            self.base = sems.take(2 * chunks)
            self.link = sems.take(chunks + 1 + early) if link_rows else None

        def cols(self, i):
            return pl.ds(pl.multiple_of(i * self.cw, self.cw), self.cw)

        def pair(self, i, kind):
            owner = (diag, part)[kind]
            return remote(self.partial.at[block(owner), self.cols(i)], self.from_part.at[kind, :, self.cols(i)], self.base + self.chunks * kind + i, part)

        def first(self, i):
            top = pl.ds(0, half)
            return remote(self.summed.at[top, self.cols(i)], self.from_peer.at[top, self.cols(i)], self.link + i, peer)

        def second(self):
            at = (pl.ds(half, half), pl.ds(self.early * self.cw, d - self.early * self.cw))
            return remote(self.summed.at[at], self.from_peer.at[at], self.link + self.chunks, peer)

        def ahead(self, i):
            at = (pl.ds(half, half), self.cols(i))
            return remote(self.summed.at[at], self.from_peer.at[at], self.link + self.chunks + 1 + i, peer)

        def chip_sum(self, i):
            self.pair(i, 0).wait_recv()
            cols = self.cols(i)
            self.summed[:, cols] = self.partial[block(peer), cols] + self.from_part[0, :, cols]
            if self.link_rows:
                self.first(i).start()
            if self.early:
                @pl.when(i < self.early)
                def _():
                    self.ahead(i).start()

        def run(self, chunk, lag=0):
            def step(i, carry):
                self.partial[:, self.cols(i)] = chunk(self.cols(i))
                self.pair(i, 0).start()
                self.pair(i, 1).start()
                if lag:
                    @pl.when(i >= lag)
                    def _():
                        self.chip_sum(i - lag)
                return carry

            lax.fori_loop(0, self.chunks, step, 0)
            if lag:
                self.drain(self.chunks - lag)

        def drain(self, start=0):
            for i in range(start, self.chunks):
                self.chip_sum(i)
            if self.link_rows == rows:
                self.second().start()

        def kept(self):
            for i in range(self.chunks):
                self.pair(i, 1).wait_recv()

        def kept_rows(self, sub):
            return self.partial[block(me, sub), :] + self.from_part[1, pl.ds(sub * half, half), :]

        def rows_sum(self, sub):
            if sub == 0:
                for i in range(self.chunks):
                    self.first(i).wait_recv()
            else:
                for i in range(self.early):
                    self.ahead(i).wait_recv()
                self.second().wait_recv()
            return self.kept_rows(sub) + self.from_peer[pl.ds(sub * half, half), :]

        def pair_sent(self):
            for i in range(self.chunks):
                self.pair(i, 0).wait_send()
                self.pair(i, 1).wait_send()

        def link_sent(self):
            if self.link_rows:
                for i in range(self.chunks):
                    self.first(i).wait_send()
            if self.link_rows == rows:
                self.second().wait_send()
            for i in range(self.early):
                self.ahead(i).wait_send()

    x_in.wait()
    small_in[0].wait()
    small_in[1].wait()
    h1[block(me), :] = norm_rows(x_own[...].astype(F32), g1_ref[...], b1_ref[...]).astype(BF16)
    pl.semaphore_wait(barrier, 2)
    gather_h1 = Gather(h1, [(0, rows) + cut for cut in cuts(d, (4, 3, 3, 2))])
    gather_dy = Gather(dyf, [(0, rows, 0, d)])
    late = [(0, half, 0, d)] + [(half, half) + cut for cut in cuts(d, (1, 1))]
    for i in range(len(gather_h1.pieces)):
        gather_h1.send(i)
    dy_in.wait()
    gather_dy.send(0)

    small_in[2].wait()
    small_in[3].wait()
    pos_rows = jnp.broadcast_to(pos_ref[...].astype(F32), (hd, seq)).T
    angles = pos_rows * freq_ref[...]
    lane = lax.broadcasted_iota(jnp.int32, (seq, hd), 1)
    rot = hd // 4
    cosb[...] = jnp.cos(angles)
    sinb[...] = jnp.where(lane < rot, -1.0, 1.0) * jnp.sin(angles)

    def turn(v, sign):
        other = jnp.where(lane < rot, pltpu.roll(v, hd - rot, 1), pltpu.roll(v, rot, 1))
        other = jnp.where(lane < 2 * rot, other, 0.0)
        return v * cosb[...] + (sign * sinb[...]) * other

    for copy in weight_in[:3]:
        copy.wait()
    n_all = nqd + 2 * nkd

    def add(total, j, piece):
        total[...] = piece if j == 0 else total[...] + piece

    qkv_sum = part_c.at[:, pl.ds(0, n_all)]
    gather_h1.feed(0, lambda j, cols: add(qkv_sum, j, mm(h1[:, cols], wqkv[cols, :])))

    qkv = qkv_sum
    for k in range(nk):
        for g in range(grp):
            lo = (k * grp + g) * hd
            head = qkv[:, lo:lo + hd].astype(BF16).astype(F32)
            qs[k, g * seq:(g + 1) * seq, :] = turn(head, 1.0).astype(BF16)
        lo = nqd + k * hd
        kv[0, k] = turn(qkv[:, lo:lo + hd].astype(BF16).astype(F32), 1.0).astype(BF16)
        lo = nqd + nkd + k * hd
        kv[1, k] = qkv[:, lo:lo + hd].astype(BF16)
    put(h1, h1_out)
    query = lax.rem(lax.broadcasted_iota(jnp.int32, (grp * seq, seq), 0), seq)
    causal = query >= lax.broadcasted_iota(jnp.int32, (grp * seq, seq), 1)
    for k in range(nk):
        scores = jnp.where(causal, mm_bt(qs[k], kv[0, k]) * hd ** -0.5, -1e30)
        exped = jnp.exp(scores - jnp.max(scores, axis=-1, keepdims=True))
        prob[k] = exped / jnp.sum(exped, axis=-1, keepdims=True)
        head_ctx = mm(prob[k].astype(BF16), kv[1, k]).astype(BF16)
        for g in range(grp):
            lo = (k * grp + g) * hd
            ctx[:, lo:lo + hd] = head_ctx[g * seq:(g + 1) * seq, :]
    put(ctx, ctx_out)
    weight_in[3].wait()
    sum_attn = Scatter(6, part_a, dr_a, snd_a, lnk_a, rows)
    sum_attn.run(lambda cols: mm(ctx[...], wo[:, cols]), lag=2)

    gather_dy.forward(0)
    gather_dy.finish(0)
    weight_in[4].wait()
    put(dyf, dy_out)
    nb = f // 2

    def down_back(j, carry):
        cols = pl.ds(pl.multiple_of(j * nb, nb), nb)
        tmat[:, cols] = mm_bt(dyf[...], w2[cols, :])
        return carry

    lax.fori_loop(0, f // nb, down_back, 0)

    gather_h2 = Gather(h2, late)
    small_in[4].wait()
    small_in[5].wait()
    for sub in (0, 1):
        if sub == 0:
            sum_attn.kept()
        own = pl.ds(sub * half, half)
        attn_rows = sum_attn.rows_sum(sub).astype(BF16)
        mid_rows = (x_own[own, :].astype(F32) + attn_rows.astype(F32)).astype(BF16)
        mid[own, :] = mid_rows
        h2[block(me, sub), :] = norm_rows(mid_rows.astype(F32), g2_ref[...], b2_ref[...]).astype(BF16)
        for i in ((0,) if sub == 0 else range(1, len(late))):
            gather_h2.send(i)
    weight_in[5].wait()

    def up(j, depth):
        cols = pl.ds(0, f)
        piece = mm(h2[:, depth], w1[depth, :])
        if j == 0:
            part_c[:, cols] = piece
        elif j < len(late) - 2:
            part_c[:, cols] += piece
        else:
            relu_up = jnp.maximum((part_c[:, cols] + piece).astype(BF16).astype(F32), 0.0)
            act[...] = (relu_up * relu_up).astype(BF16)
            du[...] = (tmat[...] * (2.0 * relu_up)).astype(BF16)

    gather_h2.feed(1, up)
    put(h2, h2_out)
    put(act, act_out)
    put(du, du_out)
    sum_dh2 = Scatter(8, part_b, dr_b, snd_b, lnk_b, rows, 3)
    sum_dh2.run(lambda cols: mm_bt(du[...], w1[cols, :]), lag=2)

    sum_mlp = Scatter(4, part_c, dr_c, snd_c, lnk_c, half)
    sum_mlp.run(lambda cols: mm(act[...], w2[:, cols]))

    gather_dx1 = Gather(dx1, late)
    normed2, scale2 = centre(mid[...].astype(F32))
    for sub in (0, 1):
        if sub == 0:
            sum_dh2.kept()
        dh2_rows = sum_dh2.rows_sum(sub).astype(BF16).astype(F32)
        own = slice(sub * half, (sub + 1) * half)
        grad_rows, grad_gain, grad_bias = norm_back(normed2[own], scale2[own], dh2_rows, g2_ref[...])
        dx1[block(me, sub), :] = (dyf[block(me, sub), :].astype(F32) + grad_rows).astype(BF16)
        for i in ((0,) if sub == 0 else range(1, len(late))):
            gather_dx1.send(i)
        if sub == 0:
            lng[0:1, :] = grad_gain
            lng[1:2, :] = grad_bias
        else:
            lng[0:1, :] += grad_gain
            lng[1:2, :] += grad_bias
    put(dx1.at[block(me)], dmid_out)
    lng_base = sems.take(2)
    lng_pair = remote(lng, lng_in.at[0], lng_base, part)
    lng_pair.start()
    sum_mlp.drain()
    low = pl.ds(half, half)
    send[pl.ds(rows, half), :] = snd_c[low, :]
    sum_mlp.kept()
    ykeep[...] = sum_mlp.kept_rows(1)
    put(ykeep, ykeep_out)
    put(mid.at[low], mid_out)
    lng_pair.wait_recv()
    lng_chip[...] = lng[...] + lng_in[0]
    lng_link = remote(lng_chip, lng_in.at[1], lng_base + 1, peer)
    lng_link.start()
    dctx_sum = tmat.at[:, pl.ds(0, nqd)]
    gather_dx1.feed(1, lambda j, cols: add(dctx_sum, j, mm_bt(dx1[:, cols], wo[:, cols])))
    put(dx1, dx1_out)

    dctx = dctx_sum[...].astype(BF16)
    for k in range(nk):
        for g in range(grp):
            lo = (k * grp + g) * hd
            gcs[k, g * seq:(g + 1) * seq, :] = dctx[:, lo:lo + hd]
    for k in range(nk):
        grad_v = mm_at(prob[k].astype(BF16), gcs[k]).astype(BF16)
        grad_p = mm_bt(gcs[k], kv[1, k])
        grad_s = (prob[k] * (grad_p - jnp.sum(grad_p * prob[k], axis=-1, keepdims=True)) * hd ** -0.5).astype(BF16)
        grad_q = mm(grad_s, kv[0, k])
        for g in range(grp):
            lo = (k * grp + g) * hd
            dqkv[:, lo:lo + hd] = turn(grad_q[g * seq:(g + 1) * seq, :], -1.0).astype(BF16)
        lo = nqd + k * hd
        dqkv[:, lo:lo + hd] = turn(mm_at(grad_s, qs[k]), -1.0).astype(BF16)
        lo = nqd + nkd + k * hd
        dqkv[:, lo:lo + hd] = grad_v
    put(dqkv, dqkv_out)
    sum_dh1 = Scatter(2, part_a, dr_d, send.at[pl.ds(0, rows)])
    sum_attn.pair_sent()
    sum_dh1.run(lambda cols: mm_bt(dqkv[...], wqkv[cols, :]))
    sum_dh1.drain()
    put(send, send_out)
    sum_dh1.kept()
    for sub in (0, 1):
        hkeep[pl.ds(sub * half, half), :] = sum_dh1.kept_rows(sub)
    put(hkeep, hkeep_out)
    top = pl.ds(0, half)
    y_own[...] = (mid[top, :].astype(F32) + sum_mlp.rows_sum(0).astype(BF16).astype(F32)).astype(BF16)
    put(y_own, y_out)
    lng_link.wait_recv()
    dg2[...] = lng_chip[0:1, :] + lng_in[1, 0:1, :]
    db2[...] = lng_chip[1:2, :] + lng_in[1, 1:2, :]
    put(dg2, dg2_out)
    put(db2, db2_out)

    for gather in (gather_h1, gather_dy, gather_h2, gather_dx1):
        for kind in (0, 1, 2):
            for i in range(len(gather.pieces)):
                gather.copy(kind, i).wait_send()
    for scatter in (sum_dh2, sum_mlp, sum_dh1):
        scatter.pair_sent()
    for scatter in (sum_attn, sum_dh2, sum_mlp):
        scatter.link_sent()
    lng_pair.wait_send()
    lng_link.wait_send()
    for copy in outs:
        copy.wait()


def cuts(d, parts):
    unit, first, out = d // sum(parts), 0, []
    for n in parts:
        out.append((first, n * unit))
        first += n * unit
    return out


def chain(dims, x, dy, pos, freq, g1, b1, g2, b2, wq, wk, wv, wo, w1, w2):
    seq, d, hd, nq, nk, f, rows = dims
    grp = nq // nk
    nqd, nkd = nq * hd, nk * hd
    n_all = nqd + 2 * nkd
    half = rows // 2

    def arr(shape, dtype):
        return jax.ShapeDtypeStruct(shape, dtype)

    def vm(*shape, dtype=BF16):
        return pltpu.VMEM(shape, dtype)

    def vf(*shape):
        return pltpu.VMEM(shape, F32)

    out_shape = [arr((seq, d), BF16)] * 4 + [arr((seq, f), BF16)] * 2 + [arr((seq, nqd), BF16), arr((seq, n_all), BF16)] + [arr((half, d), BF16)] * 2 + [arr((rows, d), BF16), arr((rows + half, d), F32), arr((rows, d), F32), arr((half, d), F32)] + [arr((1, d), F32)] * 2
    n_sems = 3 * (4 + 1 + 3 + 3) + 2 * (6 + 8 + 4 + 2) + (7 + 12 + 5) + 2
    scratch = [
        pltpu.VMEM((1, seq), jnp.int32), vf(1, hd), vf(1, d), vf(1, d), vf(1, d), vf(1, d),
        vm(d, n_all), vm(nqd, d), vm(d, f), vm(f, d),
        vm(seq, d), vm(seq, d), vm(seq, d), vm(seq, d),
        vm(rows, d), vm(rows, d), vm(half, d), vf(seq, f), vm(seq, f), vm(seq, f),
        vm(nk, grp * seq, hd), vm(2, nk, seq, hd), vm(seq, nqd), vf(nk, grp * seq, seq),
        vf(seq, hd), vf(seq, hd), vm(nk, grp * seq, hd), vm(seq, n_all), vf(2, d),
        vf(seq, d), vf(seq, d), vf(seq, d),
        vf(2, rows, d), vf(2, rows, d), vf(2, rows, d), vf(2, rows, d),
        vf(rows, d), vf(rows, d), vf(rows, d), vf(rows, d), vf(rows, d), vf(half, d),
        vf(rows + half, d), vf(rows, d), vf(half, d), vf(2, 2, d), vf(2, d), vf(1, d), vf(1, d),
        pltpu.SemaphoreType.DMA((14,)), pltpu.SemaphoreType.DMA((len(out_shape),)),
        pltpu.SemaphoreType.DMA((n_sems,)), pltpu.SemaphoreType.DMA((n_sems,)),
    ]
    return pl.pallas_call(
        functools.partial(chain_kernel, dims),
        out_shape=out_shape,
        in_specs=[ANY] * 14,
        out_specs=[ANY] * len(out_shape),
        scratch_shapes=scratch,
        compiler_params=pltpu.CompilerParams(collective_id=0, has_side_effects=True, vmem_limit_bytes=VMEM_LIMIT),
        name="chain",
    )(x, dy, pos, freq, g1, b1, g2, b2, wq, wk, wv, wo, w1, w2)


SLOTS = 4
TILE = 256


def stream_grads(jobs, stage, sem):
    def copies(job, i, slot):
        return [pltpu.make_async_copy(stage.at[slot, pl.ds(0, job[1]), pl.ds(lo, n)], dst, sem.at[slot, c]) for c, (dst, lo, n) in enumerate(job[5](i))]

    done, pending = 0, []
    for job in jobs:
        ready, tile, tiles, width, compute, targets = job
        ready()

        def fill(i, slot):
            stage[slot, :tile, :width] = compute(i)
            for copy in copies(job, i, slot):
                copy.start()

        lead = min(SLOTS, tiles)
        for i in range(lead):
            slot = (done + i) % SLOTS
            if len(pending) == SLOTS:
                for copy in pending.pop(0):
                    copy.wait()
            fill(i, slot)
            pending.append(copies(job, i, slot))

        def step(i, carry, base=done):
            slot = lax.rem(base + i, SLOTS)
            for copy in copies(job, i - SLOTS, slot):
                copy.wait()
            fill(i, slot)
            return carry

        lax.fori_loop(lead, tiles, step, 0)
        if tiles > SLOTS:
            pending = [copies(job, i, (done + i) % SLOTS) for i in range(tiles - SLOTS, tiles)]
        done += tiles
    for group in pending:
        for copy in group:
            copy.wait()


def tile_at(i, tile, first=0):
    return pl.ds(pl.multiple_of(first + i * tile, tile), tile)


def outer_jobs(ready, left, right, targets, total, lead=0):
    jobs = []
    width = right.shape[1]
    if lead:
        small = TILE // 2
        jobs.append((ready, small, lead // small, width, lambda i: mm_at(left[:, tile_at(i, small)], right[...]), lambda i: targets(tile_at(i, small))))
        ready = lambda: None
    jobs.append((ready, TILE, (total - lead) // TILE, width, lambda i: mm_at(left[:, tile_at(i, TILE, lead)], right[...]), lambda i: targets(tile_at(i, TILE, lead))))
    return jobs


def start_loads(pairs, sem):
    loads = [pltpu.make_async_copy(src, dst, sem.at[i]) for i, (src, dst) in enumerate(pairs)]
    for copy in loads:
        copy.start()

    def ready(*which):
        def wait():
            for i in which:
                loads[i].wait()

        return wait

    return ready


def grads_first_kernel(dims, act_hbm, dy_hbm, h1_hbm, dqkv_hbm, dw2, dwq, dwk, dwv, act, dyf, h1, dqkv, stage, in_sem, sem):
    seq, d, hd, nq, nk, f, rows = dims
    nqd, nkd = nq * hd, nk * hd
    ready = start_loads(((act_hbm, act), (dy_hbm, dyf), (h1_hbm, h1), (dqkv_hbm, dqkv)), in_sem)
    stream_grads(
        outer_jobs(ready(0, 1), act, dyf, lambda at: [(dw2.at[at], 0, d)], f, TILE)
        + outer_jobs(ready(2, 3), h1, dqkv, lambda at: [(dwq.at[at], 0, nqd), (dwk.at[at], nqd, nkd), (dwv.at[at], nqd + nkd, nkd)], d),
        stage, sem)


def grads_second_kernel(dims, order, h2_hbm, du_hbm, hkeep_hbm, recv_hbm, x_hbm, dmid_hbm, g1_hbm, dg2_hbm, db2_hbm, ykeep_hbm, mid_hbm, y_hbm,
                        y_out, dx_out, lng_out, dg2_out, db2_out, dw1,
                        h2, du, hkeep, recv, x, dmid, g1, ykeep, mid, y, lng, dg2, db2, stage, in_sem, end_sem, sem):
    seq, d, hd, nq, nk, f, rows = dims
    half = rows // 2
    top, low = pl.ds(0, half), pl.ds(half, half)
    ready = start_loads(((h2_hbm, h2), (du_hbm, du), (hkeep_hbm, hkeep), (recv_hbm, recv), (x_hbm, x), (dmid_hbm, dmid), (g1_hbm, g1),
                         (dg2_hbm, dg2), (db2_hbm, db2), (ykeep_hbm, ykeep), (mid_hbm, mid), (y_hbm, y.at[top])), in_sem)
    ends = [pltpu.make_async_copy(src, dst, end_sem.at[i]) for i, (src, dst) in enumerate(((y, y_out), (dmid, dx_out), (lng, lng_out), (dg2, dg2_out), (db2, db2_out)))]

    def first_norm_back():
        ready(2, 3, 4, 5, 6, 7, 8, 9, 10, 11)()
        dh1 = (hkeep[...] + recv[pl.ds(0, rows), :]).astype(BF16).astype(F32)
        grad_rows, grad_gain, grad_bias = norm_rows_back(x[...].astype(F32), dh1, g1[...])
        dmid[...] = (dmid[...].astype(F32) + grad_rows).astype(BF16)
        lanes = lng.shape[1]
        for i, total in enumerate((grad_gain, grad_bias)):
            for j in range(d // lanes):
                at = i * (d // lanes) + j
                lng[at:at + 1, :] = total[:, j * lanes:(j + 1) * lanes]
        mlp = (ykeep[...] + recv[pl.ds(rows, half), :]).astype(BF16)
        y[low, :] = (mid[...].astype(F32) + mlp.astype(F32)).astype(BF16)
        for copy in ends:
            copy.start()

    def dw1_jobs(after, first, total):
        at = functools.partial(tile_at, tile=TILE, first=first)
        return [(after, TILE, total // TILE, f, lambda i: mm_at(h2[:, at(i)], du[...]), lambda i: [(dw1.at[at(i)], 0, f)])]

    lead = SLOTS * TILE
    stream_grads(
        dw1_jobs(ready(0, 1), 0, lead) + dw1_jobs(first_norm_back, lead, d - lead),
        stage, sem)
    for copy in ends:
        copy.wait()


def grads_third_kernel(order, ctx_hbm, dx1_hbm, dwo, ctx, dx1, stage, in_sem, sem):
    ready = start_loads(((ctx_hbm, ctx), (dx1_hbm, dx1)), in_sem)
    stream_grads(outer_jobs(ready(0, 1), ctx, dx1, lambda at: [(dwo.at[at], 0, dx1.shape[1])], ctx.shape[1], TILE), stage, sem)


def cost(flops, nbytes):
    return pl.CostEstimate(flops=flops, bytes_accessed=nbytes, transcendentals=0)


def arr(shape, dtype=F32):
    return jax.ShapeDtypeStruct(shape, dtype)


def grads_first(dims, act, dyf, h1, dqkv):
    seq, d, hd, nq, nk, f, rows = dims
    nqd, nkd = nq * hd, nk * hd
    n_all = nqd + 2 * nkd
    return pl.pallas_call(
        functools.partial(grads_first_kernel, dims),
        out_shape=[arr((f, d)), arr((d, nqd)), arr((d, nkd)), arr((d, nkd))],
        in_specs=[ANY] * 4, out_specs=[ANY] * 4,
        scratch_shapes=[pltpu.VMEM((seq, f), BF16), pltpu.VMEM((seq, d), BF16), pltpu.VMEM((seq, d), BF16), pltpu.VMEM((seq, n_all), BF16),
                        pltpu.VMEM((SLOTS, TILE, d), F32), pltpu.SemaphoreType.DMA((4,)), pltpu.SemaphoreType.DMA((SLOTS, 3))],
        compiler_params=pltpu.CompilerParams(vmem_limit_bytes=VMEM_LIMIT),
        cost_estimate=cost(2 * seq * d * (f + n_all), 4 * d * (f + n_all)),
        name="grads_first",
    )(act, dyf, h1, dqkv)


def grads_second(dims, order, h2, du, hkeep, recv, x, dmid, g1, dg2, db2, ykeep, mid, y):
    seq, d, hd, nq, nk, f, rows = dims
    half = rows // 2

    def vb(*shape):
        return pltpu.VMEM(shape, BF16)

    def vf(*shape):
        return pltpu.VMEM(shape, F32)

    return pl.pallas_call(
        functools.partial(grads_second_kernel, dims),
        out_shape=[arr((rows, d), BF16), arr((rows, d), BF16), arr((2 * d // 128, 128)), arr((1, d)), arr((1, d)), arr((d, f))],
        in_specs=[ANY] * 13, out_specs=[ANY] * 6,
        scratch_shapes=[vb(seq, d), vb(seq, f), vf(rows, d), vf(rows + half, d), vb(rows, d), vb(rows, d), vf(1, d),
                        vf(half, d), vb(half, d), vb(rows, d), vf(2 * d // 128, 128), vf(1, d), vf(1, d),
                        vf(SLOTS, TILE, f), pltpu.SemaphoreType.DMA((12,)), pltpu.SemaphoreType.DMA((5,)), pltpu.SemaphoreType.DMA((SLOTS, 3))],
        compiler_params=pltpu.CompilerParams(vmem_limit_bytes=VMEM_LIMIT),
        cost_estimate=cost(2 * seq * d * f, 4 * d * f),
        name="grads_second",
    )(order, h2, du, hkeep, recv, x, dmid, g1, dg2, db2, ykeep, mid, y)


def grads_third(dims, order, ctx, dx1):
    seq, d, hd, nq, nk, f, rows = dims
    nqd = nq * hd
    return pl.pallas_call(
        grads_third_kernel,
        out_shape=arr((nqd, d)),
        in_specs=[ANY] * 3, out_specs=ANY,
        scratch_shapes=[pltpu.VMEM((seq, nqd), BF16), pltpu.VMEM((seq, d), BF16), pltpu.VMEM((SLOTS, TILE, d), F32),
                        pltpu.SemaphoreType.DMA((2,)), pltpu.SemaphoreType.DMA((SLOTS, 3))],
        compiler_params=pltpu.CompilerParams(vmem_limit_bytes=VMEM_LIMIT),
        cost_estimate=cost(2 * seq * d * nqd, 4 * d * nqd),
        name="grads_third",
    )(order, ctx, dx1)


def layer_step(x, dy, positions, g1, b1, g2, b2, wq, wk, wv, wo, w1, w2, head_dim, n_tp):
    rows, batch, d = x.shape
    seq = positions.shape[0]
    nq, nk, f = wq.shape[1] // head_dim, wk.shape[1] // head_dim, w1.shape[1]
    dims = (seq, d, head_dim, nq, nk, f, rows)
    rot = head_dim // 4
    freq = np.zeros((1, head_dim), np.float32)
    freq[0, :2 * rot] = np.tile(ROPE_BASE ** (-np.arange(rot) / rot), 2)
    x2, dy2 = x.reshape(rows, d), dy.reshape(rows, d)
    g1, b1, g2, b2 = (v.reshape(1, d) for v in (g1, b1, g2, b2))
    (h1, h2, dyf, dx1, act, du, ctx, dqkv, y, mid, dmid, send, hkeep, ykeep, dg2, db2) = chain(
        dims, x2, dy2, positions.reshape(1, seq), jnp.asarray(freq), g1, b1, g2, b2, wq, wk, wv, wo, w1, w2)

    def swap(v, bit):
        return lax.ppermute(v, 'tp', [(i, i ^ bit) for i in range(n_tp)])

    recv = swap(send, 3)
    dw2, dwq, dwk, dwv = grads_first(dims, act, dyf, h1, dqkv)
    y, dx, lng, dg2, db2, dw1 = grads_second(dims, dw2, h2, du, hkeep, recv, x2, dmid, g1, dg2, db2, ykeep, mid, y)
    others = [swap(lng, bit) for bit in (1, 2, 3)]
    dwo = grads_third(dims, lng, ctx, dx1)
    half = lng.shape[0] // 2
    sums = [((lng[at] + others[0][at]) + (others[1][at] + others[2][at])).reshape(d) for at in (slice(0, half), slice(half, None))]
    return (y.reshape(x.shape), dx.reshape(x.shape), sums[0], sums[1], dg2.reshape(d), db2.reshape(d), dwq, dwk, dwv, dwo, dw1, dw2)


def solution(mesh):
    seq_spec = P(('dp', 'tp'))
    col_spec = P(None, 'tp')
    row_spec = P('tp', None)
    grad_col_spec = P('dp', 'tp')
    grad_row_spec = P(('dp', 'tp'), None)
    in_specs = (seq_spec, seq_spec, P('dp'), P(), P(), P(), P(), col_spec, col_spec, col_spec, row_spec, col_spec, row_spec)
    out_specs = (seq_spec, seq_spec, P('dp'), P('dp'), P('dp'), P('dp'), grad_col_spec, grad_col_spec, grad_col_spec, grad_row_spec, grad_col_spec, grad_row_spec)

    def run_layer(resid_in, grad_out, positions, ln1_gain, ln1_bias, ln2_gain, ln2_bias, w_query, w_key, w_value, w_out, w_up, w_down):
        step_fn = functools.partial(layer_step, head_dim=w_key.shape[1] // KV_HEADS, n_tp=mesh.shape['tp'])
        sharded = jax.shard_map(step_fn, mesh=mesh, in_specs=in_specs, out_specs=out_specs, check_vma=False)
        return sharded(resid_in, grad_out, positions, ln1_gain, ln1_bias, ln2_gain, ln2_bias, w_query, w_key, w_value, w_out, w_up, w_down)

    return run_layer
```

```python
import functools
import math
import numpy as np
import jax
import jax.numpy as jnp
from jax import lax
from jax.experimental import pallas as pl
from jax.experimental.pallas import tpu as pltpu
from jax.sharding import PartitionSpec as P

KV_HEADS = 8
LN_EPS = 1e-5
ROPE_BASE = 10000.0
F32 = jnp.float32
BF16 = jnp.bfloat16
ANY = pl.BlockSpec(memory_space=pl.ANY)
VMEM = pl.BlockSpec(memory_space=pltpu.VMEM)
VMEM_LIMIT = 67_043_328


def mm(a, b):
    return jnp.dot(a, b, preferred_element_type=F32)


def mm_bt(a, b):
    return lax.dot_general(a, b, (((1,), (1,)), ((), ())), preferred_element_type=F32)


def mm_at(a, b):
    return lax.dot_general(a, b, (((0,), (0,)), ((), ())), preferred_element_type=F32)


def centre(rows):
    centred = rows - jnp.mean(rows, axis=-1, keepdims=True)
    scale = lax.rsqrt(jnp.mean(centred * centred, axis=-1, keepdims=True) + LN_EPS)
    return centred * scale, scale


def norm_rows(rows, gain, bias):
    normed, _ = centre(rows)
    return normed * (1.0 + gain) + bias


def norm_rows_back(rows, grad, gain):
    return norm_back(*centre(rows), grad, gain)


def norm_back(normed, scale, grad, gain):
    weighted = grad * (1.0 + gain)
    inner = jnp.mean(weighted * normed, axis=-1, keepdims=True)
    grad_rows = scale * (weighted - jnp.mean(weighted, axis=-1, keepdims=True) - normed * inner)
    return grad_rows, jnp.sum(grad * normed, axis=0, keepdims=True), jnp.sum(grad, axis=0, keepdims=True)


class Sems:
    def __init__(self):
        self.next = 0

    def take(self, count):
        base = self.next
        self.next += count
        return base


def chain_kernel(dims, x_hbm, dy_hbm, pos_hbm, freq_hbm, g1_hbm, b1_hbm, g2_hbm, b2_hbm, wq_hbm, wk_hbm, wv_hbm, wo_hbm, w1_hbm, w2_hbm,
                 h1_out, h2_out, dy_out, dx1_out, act_out, du_out, ctx_out, dqkv_out, y_out, mid_out, dmid_out, send_out, hkeep_out, ykeep_out, dg2_out, db2_out,
                 pos_ref, freq_ref, g1_ref, b1_ref, g2_ref, b2_ref,
                 wqkv, wo, w1, w2, h1, h2, dyf, dx1, x_own, mid, y_own, tmat, act, du, qs, kv, ctx, prob, cosb, sinb, gcs, dqkv, lng,
                 part_a, part_b, part_c, dr_a, dr_b, dr_c, dr_d, snd_a, snd_b, snd_c, lnk_a, lnk_b, lnk_c, send, hkeep, ykeep, lng_in, lng_chip, dg2, db2,
                 local_sem, out_sem, send_sem, recv_sem):
    seq, d, hd, nq, nk, f, rows = dims
    grp = nq // nk
    half = rows // 2
    me = lax.axis_index("tp")
    part, peer, diag = me ^ 1, me ^ 3, me ^ 2
    sems = Sems()

    def block(idx, sub=None):
        if sub is None:
            return pl.ds(pl.multiple_of(idx * rows, rows), rows)
        return pl.ds(pl.multiple_of(idx * rows + sub * half, half), half)

    def remote(src, dst, sem, dev):
        return pltpu.make_async_remote_copy(src, dst, send_sem.at[sem], recv_sem.at[sem], device_id={"tp": dev})

    def local(src, dst, idx):
        return pltpu.make_async_copy(src, dst, local_sem.at[idx])

    x_in = local(x_hbm, x_own, 0)
    dy_in = local(dy_hbm, dyf.at[block(me)], 1)
    nqd, nkd = nq * hd, nk * hd
    weight_in = [
        local(wq_hbm, wqkv.at[:, pl.ds(0, nqd)], 2),
        local(wk_hbm, wqkv.at[:, pl.ds(nqd, nkd)], 3),
        local(wv_hbm, wqkv.at[:, pl.ds(nqd + nkd, nkd)], 4),
        local(wo_hbm, wo, 5),
        local(w2_hbm, w2, 6),
        local(w1_hbm, w1, 7),
    ]
    small_in = [local(src, dst, 8 + i) for i, (src, dst) in enumerate((
        (g1_hbm, g1_ref), (b1_hbm, b1_ref), (pos_hbm, pos_ref), (freq_hbm, freq_ref), (g2_hbm, g2_ref), (b2_hbm, b2_ref)))]
    x_in.start()
    for copy in small_in:
        copy.start()
    dy_in.start()
    barrier = pltpu.get_barrier_semaphore()
    for dev in (part, peer):
        pl.semaphore_signal(barrier, inc=1, device_id={"tp": dev})
    for copy in weight_in:
        copy.start()

    outs = []

    def put(src, dst):
        copy = pltpu.make_async_copy(src, dst, out_sem.at[len(outs)])
        copy.start()
        outs.append(copy)

    class Gather:
        def __init__(self, buf, pieces):
            self.buf, self.pieces, self.base = buf, pieces, sems.take(3 * len(pieces))

        def copy(self, kind, i):
            owner = (me, me, peer)[kind]
            dev = (peer, part, part)[kind]
            row, n_rows, col, n_cols = self.pieces[i]
            at = self.buf.at[pl.ds(pl.multiple_of(owner * rows + row, half), n_rows), pl.ds(col, n_cols)]
            return remote(at, at, self.base + len(self.pieces) * kind + i, dev)

        def send(self, i):
            self.copy(0, i).start()
            self.copy(1, i).start()

        def forward(self, i):
            self.copy(0, i).wait_recv()
            self.copy(2, i).start()

        def finish(self, i):
            self.copy(1, i).wait_recv()
            self.copy(2, i).wait_recv()

        def feed(self, first, use):
            count = len(self.pieces)
            for i in range(first):
                self.forward(i)
            self.forward(first)
            for i in range(first):
                self.finish(i)
            for i in range(first, count):
                if i + 1 < count:
                    self.forward(i + 1)
                self.finish(i)
                use(i - first, pl.ds(self.pieces[i][2], self.pieces[i][3]))

    class Scatter:
        def __init__(self, chunks, partial, from_part, summed, from_peer=None, link_rows=0, early=0):
            self.chunks, self.cw, self.link_rows, self.early = chunks, d // chunks, link_rows, early
            self.partial, self.from_part, self.summed, self.from_peer = partial, from_part, summed, from_peer
            self.base = sems.take(2 * chunks)
            self.link = sems.take(chunks + 1 + early) if link_rows else None

        def cols(self, i):
            return pl.ds(pl.multiple_of(i * self.cw, self.cw), self.cw)

        def pair(self, i, kind):
            owner = (diag, part)[kind]
            return remote(self.partial.at[block(owner), self.cols(i)], self.from_part.at[kind, :, self.cols(i)], self.base + self.chunks * kind + i, part)

        def first(self, i):
            top = pl.ds(0, half)
            return remote(self.summed.at[top, self.cols(i)], self.from_peer.at[top, self.cols(i)], self.link + i, peer)

        def second(self):
            at = (pl.ds(half, half), pl.ds(self.early * self.cw, d - self.early * self.cw))
            return remote(self.summed.at[at], self.from_peer.at[at], self.link + self.chunks, peer)

        def ahead(self, i):
            at = (pl.ds(half, half), self.cols(i))
            return remote(self.summed.at[at], self.from_peer.at[at], self.link + self.chunks + 1 + i, peer)

        def chip_sum(self, i):
            self.pair(i, 0).wait_recv()
            cols = self.cols(i)
            self.summed[:, cols] = self.partial[block(peer), cols] + self.from_part[0, :, cols]
            if self.link_rows:
                self.first(i).start()
            if self.early:
                @pl.when(i < self.early)
                def _():
                    self.ahead(i).start()

        def run(self, chunk, lag=0):
            def step(i, carry):
                self.partial[:, self.cols(i)] = chunk(self.cols(i))
                self.pair(i, 0).start()
                self.pair(i, 1).start()
                if lag:
                    @pl.when(i >= lag)
                    def _():
                        self.chip_sum(i - lag)
                return carry

            lax.fori_loop(0, self.chunks, step, 0)
            if lag:
                self.drain(self.chunks - lag)

        def drain(self, start=0):
            for i in range(start, self.chunks):
                self.chip_sum(i)
            if self.link_rows == rows:
                self.second().start()

        def kept(self):
            for i in range(self.chunks):
                self.pair(i, 1).wait_recv()

        def kept_rows(self, sub):
            return self.partial[block(me, sub), :] + self.from_part[1, pl.ds(sub * half, half), :]

        def rows_sum(self, sub):
            if sub == 0:
                for i in range(self.chunks):
                    self.first(i).wait_recv()
            else:
                for i in range(self.early):
                    self.ahead(i).wait_recv()
                self.second().wait_recv()
            return self.kept_rows(sub) + self.from_peer[pl.ds(sub * half, half), :]

        def pair_sent(self):
            for i in range(self.chunks):
                self.pair(i, 0).wait_send()
                self.pair(i, 1).wait_send()

        def link_sent(self):
            if self.link_rows:
                for i in range(self.chunks):
                    self.first(i).wait_send()
            if self.link_rows == rows:
                self.second().wait_send()
            for i in range(self.early):
                self.ahead(i).wait_send()

    x_in.wait()
    small_in[0].wait()
    small_in[1].wait()
    h1[block(me), :] = norm_rows(x_own[...].astype(F32), g1_ref[...], b1_ref[...]).astype(BF16)
    pl.semaphore_wait(barrier, 2)
    gather_h1 = Gather(h1, [(0, rows) + cut for cut in cuts(d, (4, 3, 3, 2))])
    gather_dy = Gather(dyf, [(0, rows, 0, d)])
    late = [(0, half, 0, d)] + [(half, half) + cut for cut in cuts(d, (1, 1))]
    for i in range(len(gather_h1.pieces)):
        gather_h1.send(i)
    dy_in.wait()
    gather_dy.send(0)

    small_in[2].wait()
    small_in[3].wait()
    pos_rows = jnp.broadcast_to(pos_ref[...].astype(F32), (hd, seq)).T
    angles = pos_rows * freq_ref[...]
    lane = lax.broadcasted_iota(jnp.int32, (seq, hd), 1)
    rot = hd // 4
    cosb[...] = jnp.cos(angles)
    sinb[...] = jnp.where(lane < rot, -1.0, 1.0) * jnp.sin(angles)

    def turn(v, sign):
        other = jnp.where(lane < rot, pltpu.roll(v, hd - rot, 1), pltpu.roll(v, rot, 1))
        other = jnp.where(lane < 2 * rot, other, 0.0)
        return v * cosb[...] + (sign * sinb[...]) * other

    for copy in weight_in[:3]:
        copy.wait()
    n_all = nqd + 2 * nkd

    def add(total, j, piece):
        total[...] = piece if j == 0 else total[...] + piece

    qkv_sum = part_c.at[:, pl.ds(0, n_all)]
    gather_h1.feed(0, lambda j, cols: add(qkv_sum, j, mm(h1[:, cols], wqkv[cols, :])))

    qkv = qkv_sum
    for k in range(nk):
        for g in range(grp):
            lo = (k * grp + g) * hd
            head = qkv[:, lo:lo + hd].astype(BF16).astype(F32)
            qs[k, g * seq:(g + 1) * seq, :] = turn(head, 1.0).astype(BF16)
        lo = nqd + k * hd
        kv[0, k] = turn(qkv[:, lo:lo + hd].astype(BF16).astype(F32), 1.0).astype(BF16)
        lo = nqd + nkd + k * hd
        kv[1, k] = qkv[:, lo:lo + hd].astype(BF16)
    put(h1, h1_out)
    query = lax.rem(lax.broadcasted_iota(jnp.int32, (grp * seq, seq), 0), seq)
    causal = query >= lax.broadcasted_iota(jnp.int32, (grp * seq, seq), 1)
    for k in range(nk):
        scores = jnp.where(causal, mm_bt(qs[k], kv[0, k]) * hd ** -0.5, -1e30)
        exped = jnp.exp(scores - jnp.max(scores, axis=-1, keepdims=True))
        prob[k] = exped / jnp.sum(exped, axis=-1, keepdims=True)
        head_ctx = mm(prob[k].astype(BF16), kv[1, k]).astype(BF16)
        for g in range(grp):
            lo = (k * grp + g) * hd
            ctx[:, lo:lo + hd] = head_ctx[g * seq:(g + 1) * seq, :]
    put(ctx, ctx_out)
    weight_in[3].wait()
    sum_attn = Scatter(6, part_a, dr_a, snd_a, lnk_a, rows)
    sum_attn.run(lambda cols: mm(ctx[...], wo[:, cols]), lag=2)

    gather_dy.forward(0)
    gather_dy.finish(0)
    weight_in[4].wait()
    put(dyf, dy_out)
    nb = f // 2

    def down_back(j, carry):
        cols = pl.ds(pl.multiple_of(j * nb, nb), nb)
        tmat[:, cols] = mm_bt(dyf[...], w2[cols, :])
        return carry

    lax.fori_loop(0, f // nb, down_back, 0)

    gather_h2 = Gather(h2, late)
    small_in[4].wait()
    small_in[5].wait()
    for sub in (0, 1):
        if sub == 0:
            sum_attn.kept()
        own = pl.ds(sub * half, half)
        attn_rows = sum_attn.rows_sum(sub).astype(BF16)
        mid_rows = (x_own[own, :].astype(F32) + attn_rows.astype(F32)).astype(BF16)
        mid[own, :] = mid_rows
        h2[block(me, sub), :] = norm_rows(mid_rows.astype(F32), g2_ref[...], b2_ref[...]).astype(BF16)
        for i in ((0,) if sub == 0 else range(1, len(late))):
            gather_h2.send(i)
    weight_in[5].wait()

    def up(j, depth):
        cols = pl.ds(0, f)
        piece = mm(h2[:, depth], w1[depth, :])
        if j == 0:
            part_c[:, cols] = piece
        elif j < len(late) - 2:
            part_c[:, cols] += piece
        else:
            relu_up = jnp.maximum((part_c[:, cols] + piece).astype(BF16).astype(F32), 0.0)
            act[...] = (relu_up * relu_up).astype(BF16)
            du[...] = (tmat[...] * (2.0 * relu_up)).astype(BF16)

    gather_h2.feed(1, up)
    put(h2, h2_out)
    put(act, act_out)
    put(du, du_out)
    sum_dh2 = Scatter(8, part_b, dr_b, snd_b, lnk_b, rows, 3)
    sum_dh2.run(lambda cols: mm_bt(du[...], w1[cols, :]), lag=2)

    sum_mlp = Scatter(4, part_c, dr_c, snd_c, lnk_c, half)
    sum_mlp.run(lambda cols: mm(act[...], w2[:, cols]))

    gather_dx1 = Gather(dx1, late)
    normed2, scale2 = centre(mid[...].astype(F32))
    for sub in (0, 1):
        if sub == 0:
            sum_dh2.kept()
        dh2_rows = sum_dh2.rows_sum(sub).astype(BF16).astype(F32)
        own = slice(sub * half, (sub + 1) * half)
        grad_rows, grad_gain, grad_bias = norm_back(normed2[own], scale2[own], dh2_rows, g2_ref[...])
        dx1[block(me, sub), :] = (dyf[block(me, sub), :].astype(F32) + grad_rows).astype(BF16)
        for i in ((0,) if sub == 0 else range(1, len(late))):
            gather_dx1.send(i)
        if sub == 0:
            lng[0:1, :] = grad_gain
            lng[1:2, :] = grad_bias
        else:
            lng[0:1, :] += grad_gain
            lng[1:2, :] += grad_bias
    put(dx1.at[block(me)], dmid_out)
    lng_base = sems.take(2)
    lng_pair = remote(lng, lng_in.at[0], lng_base, part)
    lng_pair.start()
    sum_mlp.drain()
    low = pl.ds(half, half)
    send[pl.ds(rows, half), :] = snd_c[low, :]
    sum_mlp.kept()
    ykeep[...] = sum_mlp.kept_rows(1)
    put(ykeep, ykeep_out)
    put(mid.at[low], mid_out)
    lng_pair.wait_recv()
    lng_chip[...] = lng[...] + lng_in[0]
    lng_link = remote(lng_chip, lng_in.at[1], lng_base + 1, peer)
    lng_link.start()
    dctx_sum = tmat.at[:, pl.ds(0, nqd)]
    gather_dx1.feed(1, lambda j, cols: add(dctx_sum, j, mm_bt(dx1[:, cols], wo[:, cols])))
    put(dx1, dx1_out)

    dctx = dctx_sum[...].astype(BF16)
    for k in range(nk):
        for g in range(grp):
            lo = (k * grp + g) * hd
            gcs[k, g * seq:(g + 1) * seq, :] = dctx[:, lo:lo + hd]
    for k in range(nk):
        grad_v = mm_at(prob[k].astype(BF16), gcs[k]).astype(BF16)
        grad_p = mm_bt(gcs[k], kv[1, k])
        grad_s = (prob[k] * (grad_p - jnp.sum(grad_p * prob[k], axis=-1, keepdims=True)) * hd ** -0.5).astype(BF16)
        grad_q = mm(grad_s, kv[0, k])
        for g in range(grp):
            lo = (k * grp + g) * hd
            dqkv[:, lo:lo + hd] = turn(grad_q[g * seq:(g + 1) * seq, :], -1.0).astype(BF16)
        lo = nqd + k * hd
        dqkv[:, lo:lo + hd] = turn(mm_at(grad_s, qs[k]), -1.0).astype(BF16)
        lo = nqd + nkd + k * hd
        dqkv[:, lo:lo + hd] = grad_v
    put(dqkv, dqkv_out)
    sum_dh1 = Scatter(3, part_a, dr_d, send.at[pl.ds(0, rows)])
    sum_attn.pair_sent()
    sum_dh1.run(lambda cols: mm_bt(dqkv[...], wqkv[cols, :]))
    sum_dh1.drain()
    put(send, send_out)
    sum_dh1.kept()
    for sub in (0, 1):
        hkeep[pl.ds(sub * half, half), :] = sum_dh1.kept_rows(sub)
    put(hkeep, hkeep_out)
    top = pl.ds(0, half)
    y_own[...] = (mid[top, :].astype(F32) + sum_mlp.rows_sum(0).astype(BF16).astype(F32)).astype(BF16)
    put(y_own, y_out)
    lng_link.wait_recv()
    dg2[...] = lng_chip[0:1, :] + lng_in[1, 0:1, :]
    db2[...] = lng_chip[1:2, :] + lng_in[1, 1:2, :]
    put(dg2, dg2_out)
    put(db2, db2_out)

    for gather in (gather_h1, gather_dy, gather_h2, gather_dx1):
        for kind in (0, 1, 2):
            for i in range(len(gather.pieces)):
                gather.copy(kind, i).wait_send()
    for scatter in (sum_dh2, sum_mlp, sum_dh1):
        scatter.pair_sent()
    for scatter in (sum_attn, sum_dh2, sum_mlp):
        scatter.link_sent()
    lng_pair.wait_send()
    lng_link.wait_send()
    for copy in outs:
        copy.wait()


def cuts(d, parts):
    unit, first, out = d // sum(parts), 0, []
    for n in parts:
        out.append((first, n * unit))
        first += n * unit
    return out


def chain(dims, x, dy, pos, freq, g1, b1, g2, b2, wq, wk, wv, wo, w1, w2):
    seq, d, hd, nq, nk, f, rows = dims
    grp = nq // nk
    nqd, nkd = nq * hd, nk * hd
    n_all = nqd + 2 * nkd
    half = rows // 2

    def arr(shape, dtype):
        return jax.ShapeDtypeStruct(shape, dtype)

    def vm(*shape, dtype=BF16):
        return pltpu.VMEM(shape, dtype)

    def vf(*shape):
        return pltpu.VMEM(shape, F32)

    out_shape = [arr((seq, d), BF16)] * 4 + [arr((seq, f), BF16)] * 2 + [arr((seq, nqd), BF16), arr((seq, n_all), BF16)] + [arr((half, d), BF16)] * 2 + [arr((rows, d), BF16), arr((rows + half, d), F32), arr((rows, d), F32), arr((half, d), F32)] + [arr((1, d), F32)] * 2
    n_sems = 3 * (4 + 1 + 3 + 3) + 2 * (6 + 8 + 4 + 3) + (7 + 12 + 5) + 2
    scratch = [
        pltpu.VMEM((1, seq), jnp.int32), vf(1, hd), vf(1, d), vf(1, d), vf(1, d), vf(1, d),
        vm(d, n_all), vm(nqd, d), vm(d, f), vm(f, d),
        vm(seq, d), vm(seq, d), vm(seq, d), vm(seq, d),
        vm(rows, d), vm(rows, d), vm(half, d), vf(seq, f), vm(seq, f), vm(seq, f),
        vm(nk, grp * seq, hd), vm(2, nk, seq, hd), vm(seq, nqd), vf(nk, grp * seq, seq),
        vf(seq, hd), vf(seq, hd), vm(nk, grp * seq, hd), vm(seq, n_all), vf(2, d),
        vf(seq, d), vf(seq, d), vf(seq, d),
        vf(2, rows, d), vf(2, rows, d), vf(2, rows, d), vf(2, rows, d),
        vf(rows, d), vf(rows, d), vf(rows, d), vf(rows, d), vf(rows, d), vf(half, d),
        vf(rows + half, d), vf(rows, d), vf(half, d), vf(2, 2, d), vf(2, d), vf(1, d), vf(1, d),
        pltpu.SemaphoreType.DMA((14,)), pltpu.SemaphoreType.DMA((len(out_shape),)),
        pltpu.SemaphoreType.DMA((n_sems,)), pltpu.SemaphoreType.DMA((n_sems,)),
    ]
    return pl.pallas_call(
        functools.partial(chain_kernel, dims),
        out_shape=out_shape,
        in_specs=[ANY] * 14,
        out_specs=[ANY] * len(out_shape),
        scratch_shapes=scratch,
        compiler_params=pltpu.CompilerParams(collective_id=0, has_side_effects=True, vmem_limit_bytes=VMEM_LIMIT),
        name="chain",
    )(x, dy, pos, freq, g1, b1, g2, b2, wq, wk, wv, wo, w1, w2)


SLOTS = 4
TILE = 256


def stream_grads(jobs, stage, sem):
    def copies(job, i, slot):
        return [pltpu.make_async_copy(stage.at[slot, pl.ds(0, job[1]), pl.ds(lo, n)], dst, sem.at[slot, c]) for c, (dst, lo, n) in enumerate(job[5](i))]

    done, pending = 0, []
    for job in jobs:
        ready, tile, tiles, width, compute, targets = job
        ready()

        def fill(i, slot):
            stage[slot, :tile, :width] = compute(i)
            for copy in copies(job, i, slot):
                copy.start()

        lead = min(SLOTS, tiles)
        for i in range(lead):
            slot = (done + i) % SLOTS
            if len(pending) == SLOTS:
                for copy in pending.pop(0):
                    copy.wait()
            fill(i, slot)
            pending.append(copies(job, i, slot))

        def step(i, carry, base=done):
            slot = lax.rem(base + i, SLOTS)
            for copy in copies(job, i - SLOTS, slot):
                copy.wait()
            fill(i, slot)
            return carry

        lax.fori_loop(lead, tiles, step, 0)
        if tiles > SLOTS:
            pending = [copies(job, i, (done + i) % SLOTS) for i in range(tiles - SLOTS, tiles)]
        done += tiles
    for group in pending:
        for copy in group:
            copy.wait()


def tile_at(i, tile, first=0):
    return pl.ds(pl.multiple_of(first + i * tile, tile), tile)


def outer_jobs(ready, left, right, targets, total, lead=0):
    jobs = []
    width = right.shape[1]
    if lead:
        small = TILE // 2
        jobs.append((ready, small, lead // small, width, lambda i: mm_at(left[:, tile_at(i, small)], right[...]), lambda i: targets(tile_at(i, small))))
        ready = lambda: None
    jobs.append((ready, TILE, (total - lead) // TILE, width, lambda i: mm_at(left[:, tile_at(i, TILE, lead)], right[...]), lambda i: targets(tile_at(i, TILE, lead))))
    return jobs


def start_loads(pairs, sem):
    loads = [pltpu.make_async_copy(src, dst, sem.at[i]) for i, (src, dst) in enumerate(pairs)]
    for copy in loads:
        copy.start()

    def ready(*which):
        def wait():
            for i in which:
                loads[i].wait()

        return wait

    return ready


def grads_first_kernel(dims, act_hbm, dy_hbm, h1_hbm, dqkv_hbm, dw2, dwq, dwk, dwv, act, dyf, h1, dqkv, stage, in_sem, sem):
    seq, d, hd, nq, nk, f, rows = dims
    nqd, nkd = nq * hd, nk * hd
    ready = start_loads(((act_hbm, act), (dy_hbm, dyf), (h1_hbm, h1), (dqkv_hbm, dqkv)), in_sem)
    stream_grads(
        outer_jobs(ready(0, 1), act, dyf, lambda at: [(dw2.at[at], 0, d)], f, TILE)
        + outer_jobs(ready(2, 3), h1, dqkv, lambda at: [(dwq.at[at], 0, nqd), (dwk.at[at], nqd, nkd), (dwv.at[at], nqd + nkd, nkd)], d),
        stage, sem)


def grads_second_kernel(dims, order, h2_hbm, du_hbm, hkeep_hbm, recv_hbm, x_hbm, dmid_hbm, g1_hbm, dg2_hbm, db2_hbm, ykeep_hbm, mid_hbm, y_hbm,
                        y_out, dx_out, lng_out, dg2_out, db2_out, dw1,
                        h2, du, hkeep, recv, x, dmid, g1, ykeep, mid, y, lng, dg2, db2, stage, in_sem, end_sem, sem):
    seq, d, hd, nq, nk, f, rows = dims
    half = rows // 2
    top, low = pl.ds(0, half), pl.ds(half, half)
    ready = start_loads(((h2_hbm, h2), (du_hbm, du), (hkeep_hbm, hkeep), (recv_hbm, recv), (x_hbm, x), (dmid_hbm, dmid), (g1_hbm, g1),
                         (dg2_hbm, dg2), (db2_hbm, db2), (ykeep_hbm, ykeep), (mid_hbm, mid), (y_hbm, y.at[top])), in_sem)
    ends = [pltpu.make_async_copy(src, dst, end_sem.at[i]) for i, (src, dst) in enumerate(((y, y_out), (dmid, dx_out), (lng, lng_out), (dg2, dg2_out), (db2, db2_out)))]

    def first_norm_back():
        ready(2, 3, 4, 5, 6, 7, 8, 9, 10, 11)()
        dh1 = (hkeep[...] + recv[pl.ds(0, rows), :]).astype(BF16).astype(F32)
        grad_rows, grad_gain, grad_bias = norm_rows_back(x[...].astype(F32), dh1, g1[...])
        dmid[...] = (dmid[...].astype(F32) + grad_rows).astype(BF16)
        lanes = lng.shape[1]
        for i, total in enumerate((grad_gain, grad_bias)):
            for j in range(d // lanes):
                at = i * (d // lanes) + j
                lng[at:at + 1, :] = total[:, j * lanes:(j + 1) * lanes]
        mlp = (ykeep[...] + recv[pl.ds(rows, half), :]).astype(BF16)
        y[low, :] = (mid[...].astype(F32) + mlp.astype(F32)).astype(BF16)
        for copy in ends:
            copy.start()

    def dw1_jobs(after, first, total):
        at = functools.partial(tile_at, tile=TILE, first=first)
        return [(after, TILE, total // TILE, f, lambda i: mm_at(h2[:, at(i)], du[...]), lambda i: [(dw1.at[at(i)], 0, f)])]

    lead = SLOTS * TILE
    stream_grads(
        dw1_jobs(ready(0, 1), 0, lead) + dw1_jobs(first_norm_back, lead, d - lead),
        stage, sem)
    for copy in ends:
        copy.wait()


def grads_third_kernel(order, ctx_hbm, dx1_hbm, dwo, ctx, dx1, stage, in_sem, sem):
    ready = start_loads(((ctx_hbm, ctx), (dx1_hbm, dx1)), in_sem)
    stream_grads(outer_jobs(ready(0, 1), ctx, dx1, lambda at: [(dwo.at[at], 0, dx1.shape[1])], ctx.shape[1], TILE), stage, sem)


def cost(flops, nbytes):
    return pl.CostEstimate(flops=flops, bytes_accessed=nbytes, transcendentals=0)


def arr(shape, dtype=F32):
    return jax.ShapeDtypeStruct(shape, dtype)


def grads_first(dims, act, dyf, h1, dqkv):
    seq, d, hd, nq, nk, f, rows = dims
    nqd, nkd = nq * hd, nk * hd
    n_all = nqd + 2 * nkd
    return pl.pallas_call(
        functools.partial(grads_first_kernel, dims),
        out_shape=[arr((f, d)), arr((d, nqd)), arr((d, nkd)), arr((d, nkd))],
        in_specs=[ANY] * 4, out_specs=[ANY] * 4,
        scratch_shapes=[pltpu.VMEM((seq, f), BF16), pltpu.VMEM((seq, d), BF16), pltpu.VMEM((seq, d), BF16), pltpu.VMEM((seq, n_all), BF16),
                        pltpu.VMEM((SLOTS, TILE, d), F32), pltpu.SemaphoreType.DMA((4,)), pltpu.SemaphoreType.DMA((SLOTS, 3))],
        compiler_params=pltpu.CompilerParams(vmem_limit_bytes=VMEM_LIMIT),
        cost_estimate=cost(2 * seq * d * (f + n_all), 4 * d * (f + n_all)),
        name="grads_first",
    )(act, dyf, h1, dqkv)


def grads_second(dims, order, h2, du, hkeep, recv, x, dmid, g1, dg2, db2, ykeep, mid, y):
    seq, d, hd, nq, nk, f, rows = dims
    half = rows // 2

    def vb(*shape):
        return pltpu.VMEM(shape, BF16)

    def vf(*shape):
        return pltpu.VMEM(shape, F32)

    return pl.pallas_call(
        functools.partial(grads_second_kernel, dims),
        out_shape=[arr((rows, d), BF16), arr((rows, d), BF16), arr((2 * d // 128, 128)), arr((1, d)), arr((1, d)), arr((d, f))],
        in_specs=[ANY] * 13, out_specs=[ANY] * 6,
        scratch_shapes=[vb(seq, d), vb(seq, f), vf(rows, d), vf(rows + half, d), vb(rows, d), vb(rows, d), vf(1, d),
                        vf(half, d), vb(half, d), vb(rows, d), vf(2 * d // 128, 128), vf(1, d), vf(1, d),
                        vf(SLOTS, TILE, f), pltpu.SemaphoreType.DMA((12,)), pltpu.SemaphoreType.DMA((5,)), pltpu.SemaphoreType.DMA((SLOTS, 3))],
        compiler_params=pltpu.CompilerParams(vmem_limit_bytes=VMEM_LIMIT),
        cost_estimate=cost(2 * seq * d * f, 4 * d * f),
        name="grads_second",
    )(order, h2, du, hkeep, recv, x, dmid, g1, dg2, db2, ykeep, mid, y)


def grads_third(dims, order, ctx, dx1):
    seq, d, hd, nq, nk, f, rows = dims
    nqd = nq * hd
    return pl.pallas_call(
        grads_third_kernel,
        out_shape=arr((nqd, d)),
        in_specs=[ANY] * 3, out_specs=ANY,
        scratch_shapes=[pltpu.VMEM((seq, nqd), BF16), pltpu.VMEM((seq, d), BF16), pltpu.VMEM((SLOTS, TILE, d), F32),
                        pltpu.SemaphoreType.DMA((2,)), pltpu.SemaphoreType.DMA((SLOTS, 3))],
        compiler_params=pltpu.CompilerParams(vmem_limit_bytes=VMEM_LIMIT),
        cost_estimate=cost(2 * seq * d * nqd, 4 * d * nqd),
        name="grads_third",
    )(order, ctx, dx1)


def layer_step(x, dy, positions, g1, b1, g2, b2, wq, wk, wv, wo, w1, w2, head_dim, n_tp):
    rows, batch, d = x.shape
    seq = positions.shape[0]
    nq, nk, f = wq.shape[1] // head_dim, wk.shape[1] // head_dim, w1.shape[1]
    dims = (seq, d, head_dim, nq, nk, f, rows)
    rot = head_dim // 4
    freq = np.zeros((1, head_dim), np.float32)
    freq[0, :2 * rot] = np.tile(ROPE_BASE ** (-np.arange(rot) / rot), 2)
    x2, dy2 = x.reshape(rows, d), dy.reshape(rows, d)
    g1, b1, g2, b2 = (v.reshape(1, d) for v in (g1, b1, g2, b2))
    (h1, h2, dyf, dx1, act, du, ctx, dqkv, y, mid, dmid, send, hkeep, ykeep, dg2, db2) = chain(
        dims, x2, dy2, positions.reshape(1, seq), jnp.asarray(freq), g1, b1, g2, b2, wq, wk, wv, wo, w1, w2)

    def swap(v, bit):
        return lax.ppermute(v, 'tp', [(i, i ^ bit) for i in range(n_tp)])

    recv = swap(send, 3)
    dw2, dwq, dwk, dwv = grads_first(dims, act, dyf, h1, dqkv)
    y, dx, lng, dg2, db2, dw1 = grads_second(dims, dw2, h2, du, hkeep, recv, x2, dmid, g1, dg2, db2, ykeep, mid, y)
    others = [swap(lng, bit) for bit in (1, 2, 3)]
    dwo = grads_third(dims, lng, ctx, dx1)
    half = lng.shape[0] // 2
    sums = [((lng[at] + others[0][at]) + (others[1][at] + others[2][at])).reshape(d) for at in (slice(0, half), slice(half, None))]
    return (y.reshape(x.shape), dx.reshape(x.shape), sums[0], sums[1], dg2.reshape(d), db2.reshape(d), dwq, dwk, dwv, dwo, dw1, dw2)


def solution(mesh):
    seq_spec = P(('dp', 'tp'))
    col_spec = P(None, 'tp')
    row_spec = P('tp', None)
    grad_col_spec = P('dp', 'tp')
    grad_row_spec = P(('dp', 'tp'), None)
    in_specs = (seq_spec, seq_spec, P('dp'), P(), P(), P(), P(), col_spec, col_spec, col_spec, row_spec, col_spec, row_spec)
    out_specs = (seq_spec, seq_spec, P('dp'), P('dp'), P('dp'), P('dp'), grad_col_spec, grad_col_spec, grad_col_spec, grad_row_spec, grad_col_spec, grad_row_spec)

    def run_layer(resid_in, grad_out, positions, ln1_gain, ln1_bias, ln2_gain, ln2_bias, w_query, w_key, w_value, w_out, w_up, w_down):
        step_fn = functools.partial(layer_step, head_dim=w_key.shape[1] // KV_HEADS, n_tp=mesh.shape['tp'])
        sharded = jax.shard_map(step_fn, mesh=mesh, in_specs=in_specs, out_specs=out_specs, check_vma=False)
        return sharded(resid_in, grad_out, positions, ln1_gain, ln1_bias, ln2_gain, ln2_bias, w_query, w_key, w_value, w_out, w_up, w_down)

    return run_layer
```
